32 devices in a mesh: batch: 8 (over y, x, core), tensor: 4 (over z).
Axes of the slice: x: 2, y: 2, z: 4, core: 2. Of those that a mesh axis runs over, the one named last changes fastest.
Arguments:
- hidden_in: bfloat16 [32, 512, 768], P(('batch', 'tensor')), may hold values from -6 to 6
- segment_ids: int32 [32, 512], P('batch'), may hold values from 0 to 7, never falling along the last dimension, each value on 1 to 128 neighbouring positions
- query_weight: bfloat16 [768, 768], P(None, 'tensor'), may hold values from -0.21875 to 0.21875
- query_bias: float32 [768], P('tensor'), may hold values from -3 to 3
- key_weight: bfloat16 [768, 768], P(None, 'tensor'), may hold values from -0.21875 to 0.21875
- value_weight: bfloat16 [768, 768], P(None, 'tensor'), may hold values from -0.21875 to 0.21875
- value_bias: float32 [768], P('tensor'), may hold values from -3 to 3
- out_weight: bfloat16 [768, 768], P('tensor'), may hold values from -1.25 to 1.25
- out_bias: float32 [768], replicated, may hold values from -3 to 3
- attn_gain: float32 [768], replicated, may hold values from 0.5 to 1.5
- attn_shift: float32 [768], replicated, may hold values from -3 to 3
- up_weight: bfloat16 [768, 3072], P(None, 'tensor'), may hold values from -0.21875 to 0.21875
- up_bias: float32 [3072], P('tensor'), may hold values from -3 to 3
- down_weight: bfloat16 [3072, 768], P('tensor'), may hold values from -0.109375 to 0.109375
- down_bias: float32 [768], replicated, may hold values from -3 to 3
- ffn_gain: float32 [768], replicated, may hold values from 0.5 to 1.5
- ffn_shift: float32 [768], replicated, may hold values from -3 to 3
- cotangent: bfloat16 [32, 512, 768], P(('batch', 'tensor')), may hold values from -6 to 6
Outputs:
- layer_out: bfloat16 [32, 512, 768], P(('batch', 'tensor'))
- pooled: float32 [32, 8, 768], P(('batch', 'tensor'))
- grad_input: float32 [32, 512, 768], P(('batch', 'tensor'))
- grad_query_weight: float32 [768, 768], P(None, 'tensor')
- grad_query_bias: float32 [768], P('tensor')
- grad_key_weight: float32 [768, 768], P(None, 'tensor')
- grad_value_weight: float32 [768, 768], P(None, 'tensor')
- grad_value_bias: float32 [768], P('tensor')
- grad_out_weight: float32 [768, 768], P('tensor')
- grad_out_bias: float32 [768], P('tensor')
- grad_attn_gain: float32 [768], P('tensor')
- grad_attn_shift: float32 [768], P('tensor')
- grad_up_weight: float32 [768, 3072], P(None, 'tensor')
- grad_up_bias: float32 [3072], P('tensor')
- grad_down_weight: float32 [3072, 768], P('tensor')
- grad_down_bias: float32 [768], P('tensor')
- grad_ffn_gain: float32 [768], P('tensor')
- grad_ffn_shift: float32 [768], P('tensor')
The draws below stay inside these ranges and needn't reach their ends.
Inputs may be any that keep to these rules, and one draw needn't show every extreme that they name: `segment_ids`: in each row the text numbers never fall, every text 0 to 7 occurs, each has 1 to 128 positions, and some text has exactly 128.
All inputs are finite; a program needn't handle non-finite values.
Results may differ from the reference program's by a relative error of at most 0.015.
Values may be sent and summed in bfloat16 or wider, within the bound.
A program may use at most 128 MiB of HBM per device.

```python
import math
import jax
import jax.numpy as jnp
import numpy as np
from jax import lax

D = 768
HEADS = 12
HEAD_DIM = 64
FF = 3072
SEQ = 512
TEXTS = 8
TEXT_MOST = 128
ROWS_DEV = 4
ROWS = 32
N_BATCH = 8


def block_levels(rng, shape, shards, smallest, top_value):
    def one(axis_at, parts):
        steps = jax.random.uniform(jax.random.fold_in(jax.random.fold_in(rng, 6), axis_at), (parts,), jnp.float32, smallest / len(shards), top_value / len(shards))
        return jnp.repeat(jnp.exp(steps), shape[axis_at] // parts).reshape((-1,) + (1,) * (len(shape) - axis_at - 1))

    level = one(*shards[0])
    for cut in shards[1:]:
        level = level * one(*cut)
    return level


def split_up(count, total, bound, lean):
    weights = [(1 << 20) // math.isqrt(standing ** lean) + 1 for standing in range(2, count + 1)]
    rest, given = total - bound - (count - 1), [1] * (count - 1)
    while rest > 0:
        candidates = [i for i in range(count - 1) if given[i] < bound]
        whole, remaining = sum([weights[i] for i in candidates]), rest
        for i in candidates:
            addition = min(bound - given[i], max(1, remaining * weights[i] // whole), rest)
            given[i] = given[i] + addition
            rest = rest - addition
    return np.array([bound] + given)


def ragged_sizes(stream_key, count, total, bound, lean):
    if count == 2:
        one = jax.random.randint(stream_key, (), max(1, total - bound), min(bound, total - 1) + 1)
        return jnp.stack([one, total - one])
    sizes = jnp.asarray(split_up(count, total, bound, lean), jnp.int32)
    twos = (count - 1) // 2
    giver, receiver = sizes[1:1 + 2 * twos:2], sizes[2:2 + 2 * twos:2]
    slack = jnp.minimum(giver - 1, bound - receiver)
    moved = jax.random.randint(jax.random.fold_in(stream_key, 1), (twos,), 0, 1 << 20) % (slack + 1)
    sizes = sizes.at[1:1 + 2 * twos:2].set(giver - moved).at[2:2 + 2 * twos:2].set(receiver + moved)
    return sizes[jax.random.permutation(jax.random.fold_in(stream_key, 2), count)]


def bell_draw(own_key, dims, scale, limit, pieces=(), held_as=jnp.bfloat16):
    values = scale * jax.random.normal(own_key, dims, jnp.float32)
    if pieces:
        values = values * block_levels(own_key, dims, pieces, -0.22, 0.18)
    return jnp.clip(values, -limit, limit).astype(held_as)


def setup_inputs(seed: int = 0) -> dict:
    key_of = jax.random.split(jax.random.key(seed), 19)
    hidden_in = bell_draw(key_of[0], (ROWS, SEQ, D), 1.0, 6.0, ((0, 32),))
    segment_ids = jax.vmap(lambda own: jnp.searchsorted(jnp.cumsum(ragged_sizes(own, TEXTS, SEQ, TEXT_MOST, 1)), jnp.arange(SEQ), side="right"))(jax.random.split(key_of[1], ROWS)).reshape((ROWS, SEQ)).astype(jnp.int32)
    query_weight = bell_draw(key_of[2], (D, D), D ** -0.5, 0.21875, ((1, 4),))
    query_bias = bell_draw(key_of[3], (D,), 0.5, 3.0, ((0, 4),), jnp.float32)
    key_weight = bell_draw(key_of[4], (D, D), D ** -0.5, 0.21875, ((1, 4),))
    value_weight = bell_draw(key_of[5], (D, D), D ** -0.5, 0.21875, ((1, 4),))
    value_bias = bell_draw(key_of[6], (D,), 0.5, 3.0, ((0, 4),), jnp.float32)
    out_weight = bell_draw(key_of[7], (D, D), (D // 32) ** -0.5, 1.25, ((0, 4),))
    out_bias = bell_draw(key_of[8], (D,), 0.5, 3.0, (), jnp.float32)
    attn_gain = jnp.clip(1.0 + 0.1 * jax.random.normal(key_of[9], (D,), jnp.float32), 0.5, 1.5)
    attn_shift = bell_draw(key_of[10], (D,), 0.5, 3.0, (), jnp.float32)
    up_weight = bell_draw(key_of[11], (D, FF), D ** -0.5, 0.21875, ((1, 4),))
    up_bias = bell_draw(key_of[12], (FF,), 0.5, 3.0, ((0, 4),), jnp.float32)
    down_weight = bell_draw(key_of[13], (FF, D), FF ** -0.5, 0.109375, ((0, 4),))
    down_bias = bell_draw(key_of[14], (D,), 0.5, 3.0, (), jnp.float32)
    ffn_gain = jnp.clip(1.0 + 0.1 * jax.random.normal(key_of[15], (D,), jnp.float32), 0.5, 1.5)
    ffn_shift = bell_draw(key_of[16], (D,), 0.5, 3.0, (), jnp.float32)
    cotangent = bell_draw(key_of[17], (ROWS, SEQ, D), 1.0, 6.0, ((0, 32),))
    return dict(hidden_in=hidden_in, segment_ids=segment_ids, query_weight=query_weight, query_bias=query_bias, key_weight=key_weight, value_weight=value_weight, value_bias=value_bias, out_weight=out_weight, out_bias=out_bias, attn_gain=attn_gain, attn_shift=attn_shift, up_weight=up_weight, up_bias=up_bias, down_weight=down_weight, down_bias=down_bias, ffn_gain=ffn_gain, ffn_shift=ffn_shift, cotangent=cotangent)


@jax.custom_vjp
def low(v):
    return lax.optimization_barrier(v.astype(jnp.bfloat16)).astype(jnp.float32)

@jax.custom_vjp
def low_back(v):
    return v

def low_keep(v):
    return (low(v), None)

def low_pass(kept, grad):
    return (grad,)

def back_keep(v):
    return (v, None)

def back_low(kept, grad):
    return (low(grad),)
low.defvjp(low_keep, low_pass)
low_back.defvjp(back_keep, back_low)

def matmul(left, right):
    return jnp.einsum('...d,de->...e', left, right, precision=lax.Precision.HIGHEST)

def normalize(resid, gain, shift):
    center = resid - lax.optimization_barrier(jnp.mean(resid, axis=-1, keepdims=True))
    spread = lax.optimization_barrier(jnp.mean(center * center, axis=-1, keepdims=True))
    return center * lax.rsqrt(spread + 1e-12) * gain + shift

def layer(weights, rows_in, segment_rows):
    query_weight, query_bias, key_weight, value_weight, value_bias, out_weight, out_bias, attn_gain, attn_shift, up_weight, up_bias, down_weight, down_bias, ffn_gain, ffn_shift = weights
    groups, length, width = rows_in.shape
    query = low_back(low(matmul(rows_in, query_weight) + query_bias))
    keyset = low_back(low(matmul(rows_in, key_weight)))
    valueset = low_back(low(matmul(rows_in, value_weight) + value_bias))

    def by_heads(tensor):
        return tensor.reshape(groups, length, HEADS, HEAD_DIM)
    raw = jnp.einsum('gqhd,gkhd->ghqk', by_heads(query), by_heads(keyset), precision=lax.Precision.HIGHEST)
    scores = low_back(raw * (1.0 / math.sqrt(HEAD_DIM)))
    same_text = segment_rows[:, :, None] == segment_rows[:, None, :]
    scores = jnp.where(same_text[:, None], scores, -1000000000.0)
    probs = low(jax.nn.softmax(scores, axis=-1))
    context = jnp.einsum('ghqk,gkhd->gqhd', probs, by_heads(valueset), precision=lax.Precision.HIGHEST)
    context = low_back(low(context.reshape(groups, length, width)))
    attn = low_back(matmul(context, out_weight))
    hidden1 = normalize(attn + out_bias + rows_in, attn_gain, attn_shift)
    preact = low_back(matmul(low(hidden1), up_weight) + up_bias)
    activated = low(jax.nn.gelu(preact, approximate=False))
    ffn = low_back(matmul(activated, down_weight))
    final = normalize(ffn + down_bias + hidden1, ffn_gain, ffn_shift)
    labels = jnp.arange(TEXTS, dtype=jnp.int32)
    member = (segment_rows[:, None, :] == labels[None, :, None]).astype(jnp.float32)
    counts = lax.optimization_barrier(jnp.sum(member, axis=-1))
    pooled = jnp.einsum('rts,rsd->rtd', member, final, precision=lax.Precision.HIGHEST) / counts[:, :, None]
    return (final, pooled)

def reference(hidden_in, segment_ids, query_weight, query_bias, key_weight, value_weight, value_bias, out_weight, out_bias, attn_gain, attn_shift, up_weight, up_bias, down_weight, down_bias, ffn_gain, ffn_shift, cotangent):
    weights = tuple((item.astype(jnp.float32) for item in (query_weight, query_bias, key_weight, value_weight, value_bias, out_weight, out_bias, attn_gain, attn_shift, up_weight, up_bias, down_weight, down_bias, ffn_gain, ffn_shift)))
    inputs_float = hidden_in.astype(jnp.float32).reshape(N_BATCH, ROWS_DEV, SEQ, D)
    segment_groups = segment_ids.reshape(N_BATCH, ROWS_DEV, SEQ)

    def run(weight_set, inputs_all):

        def advance(carry, items):
            return (carry, jax.checkpoint(layer)(weight_set, items[0], items[1]))
        _, results = lax.scan(advance, None, (inputs_all, segment_groups))
        return (results[0], results[1])
    outputs, pullback, pooled_groups = jax.vjp(run, weights, inputs_float, has_aux=True)
    grad_weights, grad_inputs = pullback(cotangent.astype(jnp.float32).reshape(outputs.shape))
    final = outputs.reshape(ROWS, SEQ, D)
    pooled = pooled_groups.reshape(ROWS, TEXTS, D)
    return (final.astype(jnp.bfloat16), pooled, grad_inputs.reshape(ROWS, SEQ, D), grad_weights[0], grad_weights[1], grad_weights[2], grad_weights[3], grad_weights[4], grad_weights[5], grad_weights[6], grad_weights[7], grad_weights[8], grad_weights[9], grad_weights[10], grad_weights[11], grad_weights[12], grad_weights[13], grad_weights[14])
```

```python
import functools
import math

import jax
import jax.numpy as jnp
from jax import lax
from jax.experimental import pallas as pl
from jax.experimental.pallas import tpu as pltpu
from jax.sharding import PartitionSpec as P

HEAD_DIM = 64
TEXTS = 8
PLANE = 8
CHIPS = 4
MESH = pl.DeviceIdType.MESH
F32 = jnp.float32
BF16 = jnp.bfloat16


class Place:
    def __init__(self, n_t):
        bi = lax.axis_index("batch")
        self.t = lax.axis_index("tensor")
        self.n_t = n_t
        self.r = lax.rem(bi, PLANE)
        self.base = bi - self.r
        self.c = lax.rem(self.r, 2)
        self.q = self.r // 2

    def z(self, step):
        return {"batch": self.base + self.r, "tensor": lax.rem(self.t + step, self.n_t)}

    def chip(self, j):
        other = self.xor_q(j)
        return {"batch": self.base + other * 2 + self.c, "tensor": self.t}

    def xor_q(self, j):
        x, y = lax.rem(self.q, 2), self.q // 2
        if j & 1:
            x = 1 - x
        if j & 2:
            y = 1 - y
        return y * 2 + x

    def sibling(self):
        return {"batch": self.base + self.q * 2 + 1 - self.c, "tensor": self.t}

    def greet(self):
        barrier = pltpu.get_barrier_semaphore()
        peers = [self.z(s) for s in range(1, self.n_t)]
        peers += [self.chip(j) for j in range(1, CHIPS)] + [self.sibling()]
        for peer in peers:
            pl.semaphore_signal(barrier, inc=1, device_id=peer, device_id_type=MESH)
        pl.semaphore_wait(barrier, len(peers))


def remote(src, dst, send, recv, dev):
    return pltpu.make_async_remote_copy(
        src_ref=src, dst_ref=dst, send_sem=send, recv_sem=recv, device_id=dev, device_id_type=MESH
    )


def gather_kernel(n_t, wl, w, zs, zr, xs, xr, ss, sr, ls):
    me = Place(n_t)
    groups, rows = wl.shape[0], wl.shape[1]
    ch = rows // PLANE
    half = rows // 2
    mine = pl.ds(pl.multiple_of((me.c * CHIPS + me.q) * ch, ch), ch)
    my_half = pl.ds(pl.multiple_of(me.c * half, half), half)
    me.greet()

    def zcopy(g, s):
        return remote(wl.at[g, mine], w.at[g, me.t, mine], zs.at[g, s], zr.at[g, s], me.z(s + 1))

    def came(s):
        return lax.rem(me.t + n_t - 1 - s, n_t)

    def xcopy(g, s, j):
        place = w.at[g, came(s), mine]
        return remote(place, place, xs.at[g, s, j], xr.at[g, s, j], me.chip(j + 1))

    def scopy(g, s):
        place = w.at[g, came(s), my_half]
        return remote(place, place, ss.at[g, s], sr.at[g, s], me.sibling())

    for g in range(groups):
        for s in range(n_t - 1):
            zcopy(g, s).start()
    for g in range(groups):
        pltpu.make_async_copy(wl.at[g], w.at[g, me.t], ls.at[g]).start()
    for g in range(groups):
        for s in range(n_t - 1):
            zcopy(g, s).wait_recv()
            for j in range(CHIPS - 1):
                xcopy(g, s, j).start()
    for g in range(groups):
        for s in range(n_t - 1):
            for j in range(CHIPS - 1):
                xcopy(g, s, j).wait_recv()
            scopy(g, s).start()
    for g in range(groups):
        for s in range(n_t - 1):
            scopy(g, s).wait_recv()
    for g in range(groups):
        pltpu.make_async_copy(wl.at[g], w.at[g, me.t], ls.at[g]).wait()
        for s in range(n_t - 1):
            zcopy(g, s).wait_send()
            scopy(g, s).wait_send()
            for j in range(CHIPS - 1):
                xcopy(g, s, j).wait_send()


def gather_weights(wl, n_t):
    groups, rows, cols = wl.shape
    dma = pltpu.SemaphoreType.DMA
    return pl.pallas_call(
        functools.partial(gather_kernel, n_t),
        out_shape=jax.ShapeDtypeStruct((groups, n_t, rows, cols), wl.dtype),
        in_specs=[pl.BlockSpec(memory_space=pltpu.VMEM)],
        out_specs=pl.BlockSpec(memory_space=pltpu.VMEM),
        scratch_shapes=[
            dma((groups, n_t - 1)),
            dma((groups, n_t - 1)),
            dma((groups, n_t - 1, CHIPS - 1)),
            dma((groups, n_t - 1, CHIPS - 1)),
            dma((groups, n_t - 1)),
            dma((groups, n_t - 1)),
            dma((groups,)),
        ],
        compiler_params=pltpu.CompilerParams(
            collective_id=1, has_side_effects=True, vmem_limit_bytes=60 << 20
        ),
    )(wl)


def reduce_kernel(
    n_t, gin, vin, fout, vout, g_ref, a_ref, b_ref, d_ref, va, vb, vd, vsum,
    ls, as_, ar, bs, br, ds_, dr, fs, fr, ss, sr, vs, vr,
):
    me = Place(n_t)
    groups, rows = gin.shape[0], gin.shape[2]
    ch = rows // PLANE
    half = rows // 2
    mine = pl.ds(pl.multiple_of((me.c * CHIPS + me.q) * ch, ch), ch)
    my_half = pl.ds(pl.multiple_of(me.c * half, half), half)
    other_half = pl.ds(pl.multiple_of((1 - me.c) * half, half), half)
    me.greet()
    units = [(g, s) for g in range(groups) for s in range(n_t)]

    def tu(s):
        return lax.rem(me.t + 1 + s, n_t)

    def r1(g, s):
        return remote(
            gin.at[g, tu(s), other_half], a_ref.at[g, s], as_.at[g, s], ar.at[g, s], me.sibling()
        )

    def r2(g, s, j):
        target = pl.ds(pl.multiple_of((me.c * CHIPS + me.xor_q(j + 1)) * ch, ch), ch)
        return remote(
            g_ref.at[g, s, pl.ds(pl.multiple_of(me.xor_q(j + 1) * ch, ch), ch)],
            b_ref.at[g, s, j], bs.at[g, s, j], br.at[g, s, j], me.chip(j + 1),
        )

    own_q = pl.ds(pl.multiple_of(me.q * ch, ch), ch)

    def r3(g, s):
        return remote(
            g_ref.at[g, s, own_q], d_ref.at[g, s], ds_.at[g, s], dr.at[g, s], me.z(s + 1)
        )

    def r4(g, j):
        place = fout.at[g, mine]
        return remote(place, place, fs.at[g, j], fr.at[g, j], me.chip(j + 1))

    def r5(g):
        place = fout.at[g, my_half]
        return remote(place, place, ss.at[g], sr.at[g], me.sibling())

    v1 = remote(vin, va, vs.at[0], vr.at[0], me.sibling())
    v1.start()
    for g, s in units:
        r1(g, s).start()
    v1.wait_recv()
    vsum[...] = vin[...] + va[...]
    v2 = [
        remote(vsum, vb.at[j], vs.at[1 + j], vr.at[1 + j], me.chip(j + 1)) for j in range(CHIPS - 1)
    ]
    for c in v2:
        c.start()

    for g, s in units:
        r1(g, s).wait_recv()

        @pl.loop(0, CHIPS)
        def _(k):
            part = pl.ds(pl.multiple_of(k * ch, ch), ch)
            src = pl.ds(pl.multiple_of(me.c * half + k * ch, ch), ch)
            g_ref[g, s, part] = (
                gin[g, tu(s), src].astype(F32) + a_ref[g, s, part].astype(F32)
            ).astype(BF16)

        for j in range(CHIPS - 1):
            r2(g, s, j).start()
    for c in v2:
        c.wait()
    va[...] = vsum[...] + vb[0] + vb[1] + vb[2]
    v3 = [
        remote(va.at[tu(s)], vd.at[s], vs.at[4 + s], vr.at[4 + s], me.z(s + 1))
        for s in range(n_t - 1)
    ]
    for c in v3:
        c.start()
    for g, s in units:
        for j in range(CHIPS - 1):
            r2(g, s, j).wait_recv()
        total = g_ref[g, s, own_q].astype(F32)
        for j in range(CHIPS - 1):
            total = total + b_ref[g, s, j].astype(F32)
        g_ref[g, s, own_q] = total.astype(BF16)
        if s < n_t - 1:
            r3(g, s).start()
    for c in v3:
        c.wait()
    vout[...] = va[me.t] + vd[0] + vd[1] + vd[2]
    for g in range(groups):
        for s in range(n_t - 1):
            r3(g, s).wait_recv()
        total = g_ref[g, n_t - 1, own_q].astype(F32)
        for s in range(n_t - 1):
            total = total + d_ref[g, s].astype(F32)
        fout[g, mine] = total.astype(BF16)
        for j in range(CHIPS - 1):
            r4(g, j).start()
    for g in range(groups):
        for j in range(CHIPS - 1):
            r4(g, j).wait_recv()
        r5(g).start()
    for g in range(groups):
        r5(g).wait_recv()
    v1.wait_send()
    for g, s in units:
        r1(g, s).wait_send()
        for j in range(CHIPS - 1):
            r2(g, s, j).wait_send()
        if s < n_t - 1:
            r3(g, s).wait_send()
    for g in range(groups):
        for j in range(CHIPS - 1):
            r4(g, j).wait_send()
        r5(g).wait_send()


def reduce_grads(gin, vin, n_t):
    groups, _, rows, cols = gin.shape
    dma = pltpu.SemaphoreType.DMA
    vmem = pltpu.VMEM
    ch, half = rows // PLANE, rows // 2
    vshape = vin.shape
    return pl.pallas_call(
        functools.partial(reduce_kernel, n_t),
        out_shape=(
            jax.ShapeDtypeStruct((groups, rows, cols), BF16),
            jax.ShapeDtypeStruct(vshape[1:], F32),
        ),
        in_specs=[pl.BlockSpec(memory_space=vmem)] * 2,
        out_specs=[pl.BlockSpec(memory_space=vmem)] * 2,
        scratch_shapes=[
            vmem((groups, n_t, half, cols), BF16),
            vmem((groups, n_t, half, cols), BF16),
            vmem((groups, n_t, CHIPS - 1, ch, cols), BF16),
            vmem((groups, n_t - 1, ch, cols), BF16),
            vmem(vshape, F32),
            vmem((CHIPS - 1,) + vshape, F32),
            vmem((n_t - 1,) + vshape[1:], F32),
            vmem(vshape, F32),
            dma((1,)),
            dma((groups, n_t)),
            dma((groups, n_t)),
            dma((groups, n_t, CHIPS - 1)),
            dma((groups, n_t, CHIPS - 1)),
            dma((groups, n_t - 1)),
            dma((groups, n_t - 1)),
            dma((groups, CHIPS - 1)),
            dma((groups, CHIPS - 1)),
            dma((groups,)),
            dma((groups,)),
            dma((4 + n_t,)),
            dma((4 + n_t,)),
        ],
        compiler_params=pltpu.CompilerParams(
            collective_id=2, has_side_effects=True, vmem_limit_bytes=62 << 20
        ),
    )(gin, vin)


def product(left, right):
    return jnp.dot(left, right, preferred_element_type=F32)


def through_rows(left, right):
    return lax.dot_general(left, right, (((0,), (0,)), ((), ())), preferred_element_type=F32)


def against_cols(left, right):
    return lax.dot_general(left, right, (((1,), (1,)), ((), ())), preferred_element_type=F32)


def normalize(resid, gain, shift):
    center = resid - jnp.mean(resid, axis=-1, keepdims=True)
    spread = jnp.mean(center * center, axis=-1, keepdims=True)
    return center * lax.rsqrt(spread + 1e-12) * gain + shift


def gelu_exact(value):
    return jax.nn.gelu(value, approximate=False)


def per_device(
    n_t, n_b,
    hidden_in, segment_ids, query_weight, query_bias, key_weight, value_weight, value_bias,
    out_weight, out_bias, attn_gain, attn_shift, up_weight, up_bias, down_weight, down_bias,
    ffn_gain, ffn_shift, cotangent,
):
    x = hidden_in[0]
    inner = query_weight.shape[1]
    heads = inner // HEAD_DIM
    scale = 1.0 / math.sqrt(HEAD_DIM)
    t = lax.axis_index("tensor")
    qkvo = jnp.concatenate([query_weight, key_weight, value_weight, out_weight.T], axis=1)
    w = gather_weights(jnp.stack([qkvo, up_weight, down_weight]), n_t)
    biases = lax.all_gather(
        jnp.concatenate([query_bias, value_bias, up_bias]), "tensor", axis=0, tiled=False
    )
    bq, bv, bu = biases[:, :inner], biases[:, inner : 2 * inner], biases[:, 2 * inner :]
    seg = lax.dynamic_slice_in_dim(segment_ids, t, 1, 0)[0]
    same = seg[:, None] == seg[None, :]

    def heads_of(v):
        return v.reshape(v.shape[0], n_t * heads, HEAD_DIM)

    def cat(f):
        return jnp.concatenate([f(i) for i in range(n_t)], axis=1)

    q = cat(lambda i: product(x, w[0, i, :, :inner]) + bq[i]).astype(BF16)
    k = cat(lambda i: product(x, w[0, i, :, inner : 2 * inner])).astype(BF16)
    v = cat(lambda i: product(x, w[0, i, :, 2 * inner : 3 * inner]) + bv[i]).astype(BF16)
    qh, kh, vh = heads_of(q), heads_of(k), heads_of(v)
    scores = jnp.einsum("qhd,khd->hqk", qh, kh, preferred_element_type=F32) * scale
    scores = jnp.where(same[None], scores, -1000000000.0)
    ex = jnp.exp(scores - jnp.max(scores, axis=-1, keepdims=True))
    prob = ex / jnp.sum(ex, axis=-1, keepdims=True)
    plow = prob.astype(BF16)
    ctx = jnp.einsum("hqk,khd->qhd", plow, vh, preferred_element_type=F32).astype(BF16)
    ctx = ctx.reshape(x.shape)
    xf = x.astype(F32)
    wot = jnp.concatenate([w[0, i, :, 3 * inner :] for i in range(n_t)], axis=1)
    attn = against_cols(ctx, wot)
    hidden1, pull1 = jax.vjp(normalize, attn + out_bias + xf, attn_gain, attn_shift)
    h1 = hidden1.astype(BF16)
    ffn = 0.0
    acts, pulls = [], []
    for i in range(n_t):
        pre = product(h1, w[1, i]) + bu[i]
        act, pull = jax.vjp(gelu_exact, pre)
        acts.append(act.astype(BF16))
        pulls.append(pull)
        ffn = ffn + product(acts[-1], w[2, i])
    final, pull2 = jax.vjp(normalize, ffn + down_bias + hidden1, ffn_gain, ffn_shift)
    labels = jnp.arange(TEXTS, dtype=jnp.int32)
    member = (seg[None, :] == labels[:, None]).astype(F32)
    pooled = (
        jnp.dot(member, final, precision=lax.Precision.HIGHEST)
        / jnp.sum(member, axis=-1)[:, None]
    )
    dres2, ffn_gain_part, ffn_shift_part = pull2(cotangent[0].astype(F32))
    dffn = dres2.astype(BF16)
    gdown, gup, gub = [], [], []
    dh = dres2
    for i in range(n_t):
        gdown.append(through_rows(acts[i], dffn).astype(BF16))
        dpre = pulls[i](against_cols(dffn, w[2, i]))[0].astype(BF16)
        gub.append(jnp.sum(dpre.astype(F32), axis=0))
        gup.append(through_rows(h1, dpre).astype(BF16))
        dh = dh + against_cols(dpre, w[1, i])
    dres1, attn_gain_part, attn_shift_part = pull1(dh)
    dattn = dres1.astype(BF16)
    gout = through_rows(dattn, ctx).astype(BF16)
    dctx = product(dattn, wot).astype(BF16)
    dctxh = heads_of(dctx)
    dv = jnp.einsum("hqk,qhd->khd", plow, dctxh, preferred_element_type=F32).astype(BF16)
    dprob = jnp.einsum("qhd,khd->hqk", dctxh, vh, preferred_element_type=F32)
    ds = (prob * (dprob - jnp.sum(dprob * prob, axis=-1, keepdims=True))).astype(BF16)
    dq = (jnp.einsum("hqk,khd->qhd", ds, kh, preferred_element_type=F32) * scale).astype(BF16)
    dk = (jnp.einsum("hqk,qhd->khd", ds, qh, preferred_element_type=F32) * scale).astype(BF16)
    dq, dk, dv = (z.reshape(x.shape) for z in (dq, dk, dv))
    grads = [through_rows(x, z).astype(BF16) for z in (dq, dk, dv)] + [gout]
    cols = lambda z, i: z[..., i * inner : (i + 1) * inner]
    gqkvo = [jnp.concatenate([cols(z, i) for z in grads], axis=1) for i in range(n_t)]
    dx = dres1
    for i in range(n_t):
        dqkv = jnp.concatenate([cols(dq, i), cols(dk, i), cols(dv, i)], axis=1)
        dx = dx + against_cols(dqkv, w[0, i, :, : 3 * inner])
    vecs = [
        jnp.sum(dres1, axis=0), attn_gain_part, attn_shift_part,
        jnp.sum(dres2, axis=0), ffn_gain_part, ffn_shift_part,
        jnp.sum(dq.astype(F32), axis=0), jnp.sum(dv.astype(F32), axis=0),
    ]
    vrow = [jnp.concatenate([cols(z, i) for z in vecs] + [gub[i]]) for i in range(n_t)]
    used = vrow[0].shape[0]
    lanes = 384
    vin = jnp.pad(jnp.stack(vrow), ((0, 0), (0, 8 * lanes - used))).reshape(n_t, 8, lanes)
    gin = jnp.stack([jnp.stack(gdown), jnp.stack(gup), jnp.stack(gqkvo)])
    fout, vout = reduce_grads(gin, vin, n_t)
    if n_b > PLANE:
        apart = [[i + PLANE * j for j in range(n_b // PLANE)] for i in range(PLANE)]
        fout, vout = lax.psum((fout.astype(F32), vout), "batch", axis_index_groups=apart)
    fout = fout.astype(F32)
    vec = vout.reshape(-1)
    vc = lambda i: vec[i * inner : (i + 1) * inner]
    return (
        final.astype(BF16)[None],
        pooled[None],
        dx[None],
        fout[2, :, :inner],
        vc(6),
        fout[2, :, inner : 2 * inner],
        fout[2, :, 2 * inner : 3 * inner],
        vc(7),
        fout[2, :, 3 * inner :].T,
        vc(0),
        vc(1),
        vc(2),
        fout[1],
        vec[8 * inner : 8 * inner + up_bias.shape[0]],
        fout[0],
        vc(3),
        vc(4),
        vc(5),
    )


def solution(mesh):
    rows, tens = P(("batch", "tensor"), None, None), P("tensor")
    col, row = P(None, "tensor"), P("tensor", None)
    in_specs = (
        rows, P("batch", None), col, tens, col, col, tens, row, P(), P(), P(), col, tens, row,
        P(), P(), P(), rows,
    )
    out_specs = (
        rows, rows, rows, col, tens, col, col, tens, row, tens, tens, tens, col, tens, row, tens,
        tens, tens,
    )
    body = functools.partial(per_device, mesh.shape["tensor"], mesh.shape["batch"])
    return jax.shard_map(
        body, mesh=mesh, in_specs=in_specs, out_specs=out_specs, check_vma=False
    )
```

```python
import functools
import math

import jax
import jax.numpy as jnp
from jax import lax
from jax.experimental import pallas as pl
from jax.experimental.pallas import tpu as pltpu
from jax.sharding import PartitionSpec as P

HEAD_DIM = 64
TEXTS = 8
TEXT_MOST = 128
PLANE = 8
CHIPS = 4
LANES = 128
TILE = 256
MESH = pl.DeviceIdType.MESH
F32 = jnp.float32
BF16 = jnp.bfloat16
QKVO, UP, DOWN = 0, 1, 2
ERFC_STEP = 0.43
ERFC_POLY = (
    0.24251981500369507,
    0.24429385145717694,
    0.2054723295686731,
    0.24508130662046312,
    -0.0823056340674522,
    0.3798888788682746,
    -0.3080966384375393,
    0.07314607841870144,
)


class Place:
    def __init__(self, n_t):
        bi = lax.axis_index("batch")
        self.t = lax.axis_index("tensor")
        self.n_t = n_t
        self.r = lax.rem(bi, PLANE)
        self.base = bi - self.r
        self.c = lax.rem(self.r, 2)
        self.q = self.r // 2
        self.x = lax.rem(self.q, 2)
        self.y = self.q // 2

    def z(self, step):
        return {"batch": self.base + self.r, "tensor": lax.rem(self.t + step, self.n_t)}

    def other(self, axis):
        if isinstance(axis, int) and axis == 2:
            return (1 - self.y) * 2 + 1 - self.x
        over_x = self.y * 2 + 1 - self.x
        over_y = (1 - self.y) * 2 + self.x
        return over_x * (1 - axis) + over_y * axis

    def chip(self, axis):
        return {"batch": self.base + self.other(axis) * 2 + self.c, "tensor": self.t}

    def sibling(self):
        return {"batch": self.base + self.q * 2 + 1 - self.c, "tensor": self.t}

    def greet(self):
        barrier = pltpu.get_barrier_semaphore()
        peers = [self.z(s) for s in range(1, self.n_t)]
        peers += [self.chip(j) for j in range(3)] + [self.sibling()]
        for peer in peers:
            pl.semaphore_signal(barrier, inc=1, device_id=peer, device_id_type=MESH)
        pl.semaphore_wait(barrier, len(peers))


def remote(src, dst, send, recv, dev):
    return pltpu.make_async_remote_copy(
        src_ref=src, dst_ref=dst, send_sem=send, recv_sem=recv, device_id=dev, device_id_type=MESH
    )


def span(start, size):
    return pl.ds(start if isinstance(start, int) else pl.multiple_of(start, size), size)


def nn(left, right):
    return jnp.dot(left, right, preferred_element_type=F32)


def nt(left, right):
    return lax.dot_general(left, right, (((1,), (1,)), ((), ())), preferred_element_type=F32)


def tn(left, right):
    return lax.dot_general(left, right, (((0,), (0,)), ((), ())), preferred_element_type=F32)


def gelu_both(x):
    t = 1.0 / (1.0 + (ERFC_STEP * math.sqrt(0.5)) * jnp.abs(x))
    poly = jnp.full_like(x, ERFC_POLY[-1])
    for c in ERFC_POLY[-2::-1]:
        poly = poly * t + c
    bell = jnp.exp(x * x * -0.5)
    tail = 0.5 * (poly * t) * bell
    cdf = jnp.where(x > 0, 1.0 - tail, tail)
    return x * cdf, cdf + x * (bell * (1.0 / math.sqrt(2.0 * math.pi)))


def layer_kernel(
    n_t,
    wl, x, dy, segc, segr, vecs, bloc,
    layer_out, pooled, acc, fout, vout,
    w, g, a, b, d, qkv, ctx, dctx, prob, act, dg, h1, dlow, work, tr, dsc, n1, near, bias, rstd,
    sums, vsum, va, vb, vd,
    ls, zs, zr, xs, xr, rs, rr, ss, sr, cs, cr,
    r1s, r1r, r2s, r2r, r3s, r3r, r4s, r4r, r5s, r5r, vs, vr,
):
    me = Place(n_t)
    length, width = x.shape
    rows = w.shape[2]
    heads = 3
    ch, half = rows // PLANE, rows // 2
    mine = span((me.c * CHIPS + me.q) * ch, ch)
    my_half = span(me.c * half, half)
    blocks = length // LANES
    far = n_t - 1

    def came(s):
        return lax.rem(me.t + far - s, n_t)

    def goes(s):
        return lax.rem(me.t + 1 + s, n_t)

    def local(k):
        return pltpu.make_async_copy(wl.at[k], w.at[k, me.t], ls.at[k])

    def zcopy(k, s):
        place = w.at[k, me.t, mine]
        return remote(place, place, zs.at[k, s], zr.at[k, s], me.z(s + 1))

    def xcopy(k, s, j):
        place = w.at[k, came(s), mine]
        return remote(place, place, xs.at[k, s, j], xr.at[k, s, j], me.chip(j))

    def relay(k, s, j):
        start = (me.c * CHIPS + me.other(j)) * ch + j * (ch // 2)
        place = w.at[k, came(s), span(start, ch // 2)]
        return remote(place, place, rs.at[k, s, j], rr.at[k, s, j], me.chip(1 - j))

    def scopy(k, s):
        place = w.at[k, came(s), my_half]
        return remote(place, place, ss.at[k, s], sr.at[k, s], me.sibling())

    def bcopy(s):
        return remote(bloc, near.at[me.t], cs.at[s], cr.at[s], me.z(s + 1))

    def on_z(k, s):
        zcopy(k, s).wait_recv()
        for j in range(2):
            xcopy(k, s, j).start()

    def on_xy(k, s):
        for j in range(2):
            xcopy(k, s, j).wait_recv()
            relay(k, s, j).start()

    def on_relay(k, s):
        for j in range(2):
            relay(k, s, j).wait_recv()
        scopy(k, s).start()

    def slot(k):
        return 1 if k == 1 else 0

    def inbox(k):
        return act if k == 2 else a.at[k]

    def r1(k, s):
        return remote(
            g.at[slot(k), s, span((1 - me.c) * half, half)],
            inbox(k).at[s, span(0, half)], r1s.at[k, s], r1r.at[k, s], me.sibling(),
        )

    def quarter(q):
        return span(me.c * half + q * ch, ch)

    def turn(s):
        return lax.rem(jnp.int32(s), 2)

    def r2(k, s, j):
        first = turn(s)
        if j == 0:
            return remote(
                g.at[slot(k), s, quarter(me.other(first))], b.at[slot(k), s, 0],
                r2s.at[k, s, 0], r2r.at[k, s, 0], me.chip(first),
            )
        if j == 1:
            return remote(
                g.at[slot(k), s, quarter(me.other(2))], b.at[slot(k), s, 1],
                r2s.at[k, s, 1], r2r.at[k, s, 1], me.chip(first),
            )
        return remote(
            g.at[slot(k), s, quarter(me.other(1 - first))], b.at[slot(k), s, 2],
            r2s.at[k, s, 2], r2r.at[k, s, 2], me.chip(1 - first),
        )

    def r3(k, s):
        return remote(b.at[slot(k), s, 0], d.at[k, s], r3s.at[k, s], r3r.at[k, s], me.z(s + 1))

    def r4(k, j):
        place = fout.at[k, mine]
        return remote(place, place, r4s.at[k, j], r4r.at[k, j], me.chip(j))

    def r5(k):
        place = fout.at[k, my_half]
        return remote(place, place, r5s.at[k], r5r.at[k], me.sibling())

    def on_r1(k, s):
        r1(k, s).wait_recv()

        @pl.loop(0, half // 64)
        def _(m):
            src = span(me.c * half + m * 64, 64)
            got = inbox(k)[s, span(m * 64, 64)].astype(F32)
            g[slot(k), s, src] = (g[slot(k), s, src].astype(F32) + got).astype(BF16)

        r2(k, s, 0).start()
        r2(k, s, 1).start()

    def on_r2(k, s):
        first = turn(s)
        r2(k, s, 0).wait_recv()
        r2(k, s, 1).wait_recv()
        away = quarter(me.other(1 - first))
        keep = quarter(me.q)
        g[slot(k), s, away] = (
            g[slot(k), s, away].astype(F32) + b[slot(k), s, 1].astype(F32)
        ).astype(BF16)
        r2(k, s, 2).start()
        g[slot(k), s, keep] = (
            g[slot(k), s, keep].astype(F32) + b[slot(k), s, 0].astype(F32)
        ).astype(BF16)

    def on_r2b(k, s, last):
        r2(k, s, 2).wait_recv()
        b[slot(k), s, 0] = (
            g[slot(k), s, quarter(me.q)].astype(F32) + b[slot(k), s, 2].astype(F32)
        ).astype(BF16)
        if last is None:

            @pl.when(s < far)
            def _():
                r3(k, s).start()

        elif not last:
            r3(k, s).start()

    def on_r3(k):
        total = b[slot(k), far, 0].astype(F32)
        for s in range(far):
            r3(k, s).wait_recv()
            total = total + d[k, s].astype(F32)
        for s in range(far):
            r3(k, s).wait_send()
        fout[k, mine] = total.astype(BF16)
        for j in range(3):
            r4(k, j).start()

    def on_r4(k):
        for j in range(3):
            r4(k, j).wait_recv()
        r5(k).start()

    low_lanes = lax.broadcasted_iota(jnp.int32, (1, LANES), 1) < HEAD_DIM
    low = jnp.where(low_lanes, 1.0, 0.0).astype(BF16)
    high = jnp.where(low_lanes, 0.0, 1.0).astype(BF16)
    low32 = jnp.where(low_lanes, 1.0, 0.0)
    high32 = jnp.where(low_lanes, 0.0, 1.0)

    def band(i):
        lo = max(0, i * LANES - TEXT_MOST)
        return lo, min(length, (i + 1) * LANES + TEXT_MOST)

    def project(tt):
        @pl.loop(0, length // TILE)
        def _(m):
            r = span(m * TILE, TILE)
            xm = x[r, :]
            for lo, hi in ((0, 256), (256, 512), (512, 640)):
                piece = nn(xm, w[QKVO, tt, :, lo:hi])
                qkv[tt, r, lo:hi] = (
                    (piece + near[tt, 1:2, lo:hi]) * near[tt, 2:3, lo:hi]
                ).astype(BF16)

    def attend(tt):
        for i in range(blocks):
            lo, hi = band(i)
            r = slice(i * LANES, (i + 1) * LANES)
            heads_in = (
                (qkv[tt, r, 0:128] * low, 128, 256),
                (qkv[tt, r, 0:128] * high, 128, 256),
                (qkv[tt, r, 384:512] * low, 512, 384),
            )
            outs = []
            for h, (q, kc, vc) in enumerate(heads_in):
                s = nt(q, qkv[tt, lo:hi, kc : kc + LANES]) + bias[r, 0 : hi - lo]
                e = jnp.exp(s - jnp.max(s, axis=-1, keepdims=True))
                p = (e * (1.0 / jnp.sum(e, axis=-1, keepdims=True))).astype(BF16)
                prob[tt, h, r, 0 : hi - lo] = p
                outs.append(nn(p, qkv[tt, lo:hi, vc : vc + LANES]))
            ctx[tt, r, 0:128] = (outs[2] * high32).astype(BF16)
            ctx[tt, r, 128:256] = (outs[0] * low32 + outs[1] * high32).astype(BF16)

    def attend_back(tt):
        for group in range(2):
            if group == 0:
                qc, kc, vc, dc = 0, 128, 256, 128
                hs = ((0, low, low, low32), (1, high, high, high32))
            else:
                qc, kc, vc, dc = 384, 512, 384, 0
                hs = ((2, low, high, low32),)
            dq = [None] * blocks
            for i in range(blocks):
                lo, hi = band(i)
                r = slice(i * LANES, (i + 1) * LANES)
                for n, (h, qm, vm, out_mask) in enumerate(hs):
                    dp = nt(dctx[r, dc : dc + LANES] * vm, qkv[tt, lo:hi, vc : vc + LANES])
                    p = prob[tt, h, r, 0 : hi - lo].astype(F32)
                    pd = p * dp
                    ds = (pd - p * jnp.sum(pd, axis=-1, keepdims=True)).astype(BF16)
                    dsc[n, r, 0 : hi - lo] = ds
                    part = nn(ds, qkv[tt, lo:hi, kc : kc + LANES]) * (
                        out_mask * (1.0 / math.sqrt(HEAD_DIM))
                    )
                    dq[i] = part if dq[i] is None else dq[i] + part
                if group == 0:
                    work[r, 0:128] = dq[i].astype(BF16)
            for j in range(blocks):
                rj = slice(j * LANES, (j + 1) * LANES)
                dk = dv = None
                for i in range(blocks):
                    lo, hi = band(i)
                    if not lo <= j * LANES < hi:
                        continue
                    r = slice(i * LANES, (i + 1) * LANES)
                    at = slice(j * LANES - lo, (j + 1) * LANES - lo)
                    for n, (h, qm, vm, _) in enumerate(hs):
                        more = tn(dsc[n, r, at], qkv[tt, r, qc : qc + LANES] * qm)
                        dk = more if dk is None else dk + more
                        more = tn(prob[tt, h, r, at], dctx[r, dc : dc + LANES] * vm)
                        dv = more if dv is None else dv + more
                if group == 0:
                    work[rj, 128:256] = dk.astype(BF16)
                    work[rj, 256:384] = dv.astype(BF16)
                else:
                    work[rj, 384:512] = (dq[j] + dv).astype(BF16)
                    work[rj, 512:640] = dk.astype(BF16)

    def add_sum(k, tile):
        n = tile.shape[0] // 8
        sums[k] += jnp.sum(tile.reshape(n, 8, tile.shape[1]), axis=0)

    def transpose_to(src):
        @pl.loop(0, rows // TILE)
        def _(m):
            cols = span(m * TILE, TILE)
            tr[cols, :] = src[:, cols].T

    for k in range(3):
        local(k).start()
    dy_in = pltpu.make_async_copy(dy, work, ls.at[3])
    dy_in.start()
    me.greet()
    for s in range(far):
        bcopy(s).start()
    for k in range(3):
        local(k).wait()
        for s in range(far):
            zcopy(k, s).start()
    near[me.t] = bloc[...]
    sums[...] = jnp.zeros_like(sums)
    for i in range(blocks):
        lo, hi = band(i)
        r = slice(i * LANES, (i + 1) * LANES)
        bias[r, 0 : hi - lo] = jnp.where(segc[r, :] == segr[0:1, lo:hi], 0.0, -1000000000.0)
    project(me.t)
    for s in range(far):
        on_z(QKVO, s)
    for s in range(far):
        bcopy(s).wait_recv()
    on_xy(QKVO, 0)
    attend(me.t)
    on_xy(QKVO, 1)
    on_relay(QKVO, 0)
    on_xy(QKVO, 2)

    @pl.loop(0, far)
    def _(s):
        tt = came(s)
        on_z(UP, s)
        scopy(QKVO, s).wait_recv()
        project(tt)

        @pl.when(s < far - 1)
        def _():
            on_relay(QKVO, s + 1)

        attend(tt)

        @pl.when(s > 0)
        def _():
            on_xy(UP, s - 1)

    on_xy(UP, far - 1)
    for s in range(far):
        on_z(DOWN, s)

    @pl.loop(0, length // TILE)
    def _(m):
        r = span(m * TILE, TILE)
        for n in range(width // TILE):
            c = slice(n * TILE, (n + 1) * TILE)
            out = x[r, c].astype(F32) + vecs[0:1, c]
            for t in range(n_t):
                out = out + nt(ctx[t, r, :], w[QKVO, t, c, 512:768])
            acc[r, c] = out

    on_relay(UP, 0)

    @pl.loop(0, length // 32)
    def _(m):
        r = span(m * 32, 32)
        center = acc[r, :]
        center = center - jnp.mean(center, axis=-1, keepdims=True)
        inv = lax.rsqrt(jnp.mean(center * center, axis=-1, keepdims=True) + 1e-12)
        rstd[r, :] = inv
        center = center * inv
        n1[r, :] = center
        h1[r, :] = (center * vecs[1:2, :] + vecs[2:3, :]).astype(BF16)

    def rise(tt):
        @pl.loop(0, length // TILE)
        def _(m):
            r = span(m * TILE, TILE)
            hm = h1[r, :]
            for n in range(rows // TILE):
                c = slice(n * TILE, (n + 1) * TILE)
                up, slope = gelu_both(nn(hm, w[UP, tt, :, c]) + near[tt, 0:1, c])
                act[tt, r, c] = up.astype(BF16)
                dg[tt, r, c] = slope.astype(BF16)

    def fall(tt, first):
        @pl.loop(0, length // TILE)
        def _(m):
            r = span(m * TILE, TILE)
            am = act[tt, r, :]
            for n in range(width // TILE):
                c = slice(n * TILE, (n + 1) * TILE)
                out = nn(am, w[DOWN, tt, :, c])
                acc[r, c] = out if first else acc[r, c] + out

    rise(me.t)
    on_relay(UP, 1)

    @pl.loop(0, far)
    def _(s):
        scopy(UP, s).wait_recv()
        on_xy(DOWN, s)
        rise(came(s))

        @pl.when(s == 0)
        def _():
            on_relay(UP, far - 1)

    on_relay(DOWN, 0)
    fall(me.t, True)

    @pl.loop(0, far)
    def _(s):
        @pl.when(s < far - 1)
        def _():
            on_relay(DOWN, s + 1)

        scopy(DOWN, s).wait_recv()
        fall(came(s), False)

    dy_in.wait()

    @pl.loop(0, length // 32)
    def _(m):
        r = span(m * 32, 32)
        center = acc[r, :] + vecs[3:4, :] + (n1[r, :] * vecs[1:2, :] + vecs[2:3, :])
        center = center - jnp.mean(center, axis=-1, keepdims=True)
        inv = lax.rsqrt(jnp.mean(center * center, axis=-1, keepdims=True) + 1e-12)
        n2 = center * inv
        final = n2 * vecs[4:5, :] + vecs[5:6, :]
        out = final.astype(BF16)
        g[1, 0, r, :] = out
        g[1, 1, r, :] = (final - out.astype(F32)).astype(BF16)
        dyt = work[r, :].astype(F32)
        dn = dyt * vecs[4:5, :]
        dyn = dyt * n2
        add_sum(1, dyn)
        add_sum(2, dyt)
        dr = inv * (
            dn
            - jnp.mean(dn, axis=-1, keepdims=True)
            - n2 * jnp.mean(dn * n2, axis=-1, keepdims=True)
        )
        add_sum(0, dr)
        acc[r, :] = dr
        dlow[r, :] = dr.astype(BF16)

    to_out = pltpu.make_async_copy(g.at[1, 0, span(0, length)], layer_out, ls.at[4])
    to_out.start()
    labels = lax.broadcasted_iota(jnp.int32, (TEXTS, length), 0)
    member = jnp.where(segr[0:1, :] == labels, 1.0, 0.0)
    counts = jnp.sum(member, axis=-1, keepdims=True)
    member = member.astype(BF16)
    pooled[...] = (nn(member, g[1, 0, 0:length, :]) + nn(member, g[1, 1, 0:length, :])) / counts

    ones = jnp.ones((8, length), BF16)

    def grad_to(k, s, left_t, right):
        @pl.loop(0, rows // TILE)
        def _(m):
            r = span(m * TILE, TILE)
            lt = left_t(r)
            for n in range(width // TILE):
                c = slice(n * TILE, (n + 1) * TILE)
                g[k, s, r, c] = nn(lt, right[:, c]).astype(BF16)

    @pl.loop(0, n_t)
    def _(s):
        tt = goes(s)
        grad_to(0, s, lambda r: act[tt, :, r].T, dlow)
        r1(0, s).start()

    to_out.wait()
    transpose_to(h1)

    @pl.loop(0, n_t)
    def _(s):
        tt = goes(s)
        on_r1(0, s)

        @pl.loop(0, length // TILE)
        def _(m):
            r = span(m * TILE, TILE)
            dm = dlow[r, :]
            for n in range(rows // TILE):
                c = slice(n * TILE, (n + 1) * TILE)
                work[r, c] = (nt(dm, w[DOWN, tt, c, :]) * dg[tt, r, c].astype(F32)).astype(BF16)

        @pl.when(s > 0)
        def _():
            on_r2(0, s - 1)

        grad_to(1, s, lambda r: tr[r, :], work)
        r1(1, s).start()

        @pl.loop(0, length // TILE)
        def _(m):
            r = span(m * TILE, TILE)
            dm = work[r, :]
            for n in range(width // TILE):
                c = slice(n * TILE, (n + 1) * TILE)
                acc[r, c] += nt(dm, w[UP, tt, c, :])

        vsum[pl.ds(8 + tt, 1), :] = nn(ones, work[...])[0:1, :]

    on_r2(0, far)

    @pl.loop(0, length // 32)
    def _(m):
        r = span(m * 32, 32)
        dh, nt1 = acc[r, :], n1[r, :]
        add_sum(4, dh * nt1)
        add_sum(5, dh)
        dn = dh * vecs[1:2, :]
        dr = rstd[r, :] * (
            dn
            - jnp.mean(dn, axis=-1, keepdims=True)
            - nt1 * jnp.mean(dn * nt1, axis=-1, keepdims=True)
        )
        add_sum(3, dr)
        acc[r, :] = dr
        dlow[r, :] = dr.astype(BF16)

    for s in range(n_t):
        on_r2b(0, s, s == far)
    transpose_to(dlow)
    for k, row in ((3, 0), (4, 1), (5, 2), (0, 3), (1, 4), (2, 5)):
        vsum[row : row + 1, :] = jnp.sum(sums[k], axis=0, keepdims=True)
    vsum[6:8, :] = jnp.zeros((2, width), F32)
    work[:, 640:768] = jnp.zeros((length, LANES), BF16)

    @pl.loop(0, n_t)
    def _(s):
        tt = goes(s)
        on_r1(1, s)

        @pl.loop(0, length // TILE)
        def _(m):
            r = span(m * TILE, TILE)
            out = nn(dlow[r, :], w[QKVO, tt, :, 512:768])
            dctx[r, 0:128] = (out[:, 0:128] * high32).astype(BF16)
            dctx[r, 128:256] = out[:, 128:256].astype(BF16)

        @pl.when(s == 1)
        def _():
            on_r3(0)

        @pl.when(s == 2)
        def _():
            on_r4(0)

        attend_back(tt)

        @pl.when(s > 0)
        def _():
            on_r2(1, s - 1)

        r1(0, s).wait_send()
        for j in range(3):
            r2(0, s, j).wait_send()

        @pl.loop(0, rows // TILE)
        def _(m):
            r = span(m * TILE, TILE)
            lt = x[:, r].T
            g[0, s, r, 0:256] = nn(lt, work[:, 0:256]).astype(BF16)
            g[0, s, r, 256:512] = nn(lt, work[:, 256:512]).astype(BF16)
            g[0, s, r, 512:768] = (nn(lt, work[:, 512:768]) + nn(tr[r, :], ctx[tt])).astype(BF16)

        r1(2, s).start()

        @pl.loop(0, length // TILE)
        def _(m):
            r = span(m * TILE, TILE)
            dm = work[r, 0:640]
            for n in range(width // TILE):
                c = slice(n * TILE, (n + 1) * TILE)
                acc[r, c] += nt(dm, w[QKVO, tt, c, 0:640])

        vsum[pl.ds(12 + tt, 1), :] = nn(ones, work[...])[0:1, :]

    v1 = remote(vsum, va, vs.at[0], vr.at[0], me.sibling())
    v1.start()
    on_r2(1, far)
    for s in range(n_t):
        on_r1(2, s)
    v1.wait()
    vsum[...] = vsum[...] + va[...]
    v2 = [remote(vsum, vb.at[j], vs.at[1 + j], vr.at[1 + j], me.chip(j)) for j in range(3)]
    for c in v2:
        c.start()
    for s in range(n_t):
        on_r2b(1, s, s == far)
    for s in range(n_t):
        on_r2(2, s)
    for c in v2:
        c.wait()
    va[...] = vsum[...] + vb[0] + vb[1] + vb[2]
    v3 = [remote(va, vd.at[s], vs.at[4 + s], vr.at[4 + s], me.z(s + 1)) for s in range(far)]
    for c in v3:
        c.start()
    on_r3(1)
    for s in range(n_t):
        on_r2b(2, s, s == far)
    on_r4(1)
    on_r3(2)
    for c in v3:
        c.wait()
    total = va[...]
    for s in range(far):
        total = total + vd[s]
    vout[...] = total
    on_r4(2)
    for k in range(3):
        r5(k).wait_recv()

    for s in range(far):
        bcopy(s).wait_send()
    for k in range(3):
        for s in range(far):
            zcopy(k, s).wait_send()
            scopy(k, s).wait_send()
            for j in range(2):
                xcopy(k, s, j).wait_send()
                relay(k, s, j).wait_send()
        for s in range(n_t):
            if k > 0:
                r1(k, s).wait_send()
                for j in range(3):
                    r2(k, s, j).wait_send()
        for j in range(3):
            r4(k, j).wait_send()
        r5(k).wait_send()


def run_layer(wl, x, dy, segc, segr, vecs, bloc, n_t):
    groups, rows, cols = wl.shape
    length, width = x.shape
    ch, half, far = rows // PLANE, rows // 2, n_t - 1
    dma, vmem = pltpu.SemaphoreType.DMA, pltpu.VMEM
    here, there = pl.BlockSpec(memory_space=vmem), pl.BlockSpec(memory_space=pl.ANY)
    shape = jax.ShapeDtypeStruct
    pair = lambda *dims: [dma(dims), dma(dims)]
    return pl.pallas_call(
        functools.partial(layer_kernel, n_t),
        out_shape=(
            shape((length, width), BF16),
            shape((TEXTS, width), F32),
            shape((length, width), F32),
            shape((groups, rows, cols), BF16),
            shape((16, width), F32),
        ),
        in_specs=[there, here, there, here, here, here, here],
        out_specs=[there, here, here, here, here],
        scratch_shapes=[
            vmem((groups, n_t, rows, cols), BF16),
            vmem((2, n_t, rows, cols), BF16),
            vmem((2, n_t, half, cols), BF16),
            vmem((2, n_t, 3, ch, cols), BF16),
            vmem((groups, far, ch, cols), BF16),
            vmem((n_t, length, 640), BF16),
            vmem((n_t, length, 256), BF16),
            vmem((length, 256), BF16),
            vmem((n_t, 3, length, 384), BF16),
            vmem((n_t, length, rows), BF16),
            vmem((n_t, length, rows), BF16),
            vmem((length, width), BF16),
            vmem((length, width), BF16),
            vmem((length, width), BF16),
            vmem((width, length), BF16),
            vmem((2, length, 384), BF16),
            vmem((length, width), F32),
            vmem((n_t, 8, width), F32),
            vmem((length, 384), F32),
            vmem((length, 1), F32),
            vmem((6, 8, width), F32),
            vmem((16, width), F32),
            vmem((16, width), F32),
            vmem((3, 16, width), F32),
            vmem((far, 16, width), F32),
            dma((5,)),
            *pair(groups, far),
            *pair(groups, far, 2),
            *pair(groups, far, 2),
            *pair(groups, far),
            *pair(far),
            *pair(groups, n_t),
            *pair(groups, n_t, 3),
            *pair(groups, far),
            *pair(groups, 3),
            *pair(groups),
            *pair(4 + far),
        ],
        compiler_params=pltpu.CompilerParams(
            collective_id=1, has_side_effects=True, vmem_limit_bytes=67043328
        ),
    )(wl, x, dy, segc, segr, vecs, bloc)


def per_device(
    n_t, n_b,
    hidden_in, segment_ids, query_weight, query_bias, key_weight, value_weight, value_bias,
    out_weight, out_bias, attn_gain, attn_shift, up_weight, up_bias, down_weight, down_bias,
    ffn_gain, ffn_shift, cotangent,
):
    x = hidden_in[0]
    width, inner = query_weight.shape
    two = 2 * HEAD_DIM
    t = lax.axis_index("tensor")
    wo = out_weight.T
    qkvo = jnp.concatenate(
        [
            query_weight[:, :two], key_weight[:, :two], value_weight[:, :two],
            query_weight[:, two:], value_weight[:, two:], key_weight[:, two:],
            wo[:, two:], wo[:, :two],
        ],
        axis=1,
    )
    wl = jnp.stack([qkvo, up_weight, down_weight])
    none = jnp.zeros((two,), F32)
    scale = 1.0 / math.sqrt(HEAD_DIM)
    bias_row = jnp.concatenate(
        [query_bias[:two], none, value_bias[:two], query_bias[two:], value_bias[two:], none, none]
    )
    full = jnp.ones((HEAD_DIM,), F32)
    down = full * scale
    scale_row = jnp.concatenate([down, down] + [full] * 4 + [down] + [full] * 5)
    bloc = jnp.concatenate(
        [jnp.stack([up_bias, bias_row, scale_row]), jnp.zeros((5, width), F32)], axis=0
    )
    vecs = jnp.stack(
        [out_bias, attn_gain, attn_shift, down_bias, ffn_gain, ffn_shift, out_bias, out_bias]
    )
    seg = lax.dynamic_slice_in_dim(segment_ids, t, 1, 0)[0]
    segr = jnp.broadcast_to(seg[None, :], (8, seg.shape[0]))
    final, pooled, dx, fout, vout = run_layer(
        wl, x, cotangent[0], seg[:, None], segr, vecs, bloc, n_t
    )
    if n_b > PLANE:
        apart = [[i + PLANE * j for j in range(n_b // PLANE)] for i in range(PLANE)]
        fout, vout = lax.psum((fout.astype(F32), vout), "batch", axis_index_groups=apart)
    gq = fout[2].astype(F32)
    here = lax.dynamic_slice_in_dim(vout, t * inner, inner, 1)
    dub = lax.dynamic_slice_in_dim(vout, 8 + t, 1, 0)[0]
    dqb = lax.dynamic_slice_in_dim(vout, 12 + t, 1, 0)[0]
    h = HEAD_DIM
    return (
        final[None],
        pooled[None],
        dx[None],
        jnp.concatenate([gq[:, :two], gq[:, 6 * h : 7 * h]], axis=1),
        jnp.concatenate([dqb[:two], dqb[6 * h : 7 * h]]),
        jnp.concatenate([gq[:, two : 2 * two], gq[:, 8 * h : 9 * h]], axis=1),
        jnp.concatenate([gq[:, 2 * two : 3 * two], gq[:, 7 * h : 8 * h]], axis=1),
        jnp.concatenate([dqb[2 * two : 3 * two], dqb[7 * h : 8 * h]]),
        jnp.concatenate([gq[:, 10 * h :], gq[:, 9 * h : 10 * h]], axis=1).T,
        here[0],
        here[1],
        here[2],
        fout[1].astype(F32),
        dub,
        fout[0].astype(F32),
        here[3],
        here[4],
        here[5],
    )


def solution(mesh):
    rows, tens = P(("batch", "tensor"), None, None), P("tensor")
    col, row = P(None, "tensor"), P("tensor", None)
    in_specs = (
        rows, P("batch", None), col, tens, col, col, tens, row, P(), P(), P(), col, tens, row,
        P(), P(), P(), rows,
    )
    out_specs = (
        rows, rows, rows, col, tens, col, col, tens, row, tens, tens, tens, col, tens, row, tens,
        tens, tens,
    )
    body = functools.partial(per_device, mesh.shape["tensor"], mesh.shape["batch"])
    return jax.shard_map(
        body, mesh=mesh, in_specs=in_specs, out_specs=out_specs, check_vma=False
    )
```

```python
import functools
import math

import jax
import jax.numpy as jnp
from jax import lax
from jax.experimental import pallas as pl
from jax.experimental.pallas import tpu as pltpu
from jax.sharding import PartitionSpec as P

HEAD_DIM = 64
TEXTS = 8
TEXT_MOST = 128
PLANE = 8
CHIPS = 4
LANES = 128
TILE = 256
MESH = pl.DeviceIdType.MESH
F32 = jnp.float32
BF16 = jnp.bfloat16
QKVO, UP, DOWN = 0, 1, 2
ERFC_STEP = 0.43
ERFC_POLY = (
    0.24251981500369507,
    0.24429385145717694,
    0.2054723295686731,
    0.24508130662046312,
    -0.0823056340674522,
    0.3798888788682746,
    -0.3080966384375393,
    0.07314607841870144,
)


class Place:
    def __init__(self, n_t):
        bi = lax.axis_index("batch")
        self.t = lax.axis_index("tensor")
        self.n_t = n_t
        self.r = lax.rem(bi, PLANE)
        self.base = bi - self.r
        self.c = lax.rem(self.r, 2)
        self.q = self.r // 2
        self.x = lax.rem(self.q, 2)
        self.y = self.q // 2

    def z(self, step):
        return {"batch": self.base + self.r, "tensor": lax.rem(self.t + step, self.n_t)}

    def other(self, axis):
        y = self.y if axis == 0 else 1 - self.y
        x = self.x if axis == 1 else 1 - self.x
        return y * 2 + x

    def chip(self, axis):
        return {"batch": self.base + self.other(axis) * 2 + self.c, "tensor": self.t}

    def sibling(self):
        return {"batch": self.base + self.q * 2 + 1 - self.c, "tensor": self.t}

    def greet(self):
        barrier = pltpu.get_barrier_semaphore()
        peers = [self.z(s) for s in range(1, self.n_t)]
        peers += [self.chip(j) for j in range(3)] + [self.sibling()]
        for peer in peers:
            pl.semaphore_signal(barrier, inc=1, device_id=peer, device_id_type=MESH)
        pl.semaphore_wait(barrier, len(peers))


def remote(src, dst, send, recv, dev):
    return pltpu.make_async_remote_copy(
        src_ref=src, dst_ref=dst, send_sem=send, recv_sem=recv, device_id=dev, device_id_type=MESH
    )


def span(start, size):
    return pl.ds(start if isinstance(start, int) else pl.multiple_of(start, size), size)


def nn(left, right):
    return jnp.dot(left, right, preferred_element_type=F32)


def nt(left, right):
    return lax.dot_general(left, right, (((1,), (1,)), ((), ())), preferred_element_type=F32)


def tn(left, right):
    return lax.dot_general(left, right, (((0,), (0,)), ((), ())), preferred_element_type=F32)


def gelu_both(x):
    t = 1.0 / (1.0 + (ERFC_STEP * math.sqrt(0.5)) * jnp.abs(x))
    poly = jnp.full_like(x, ERFC_POLY[-1])
    for c in ERFC_POLY[-2::-1]:
        poly = poly * t + c
    bell = jnp.exp(x * x * -0.5)
    tail = 0.5 * (poly * t) * bell
    cdf = jnp.where(x > 0, 1.0 - tail, tail)
    return x * cdf, cdf + x * (bell * (1.0 / math.sqrt(2.0 * math.pi)))


def layer_kernel(
    n_t,
    wq, wk, wv, wo, wup, wdown, x, dy, seg, vecs,
    layer_out, pooled, acc, fout, vout,
    w, g, a, b, d, qkv, ctx, dctx, prob, act, dg, h1, dlow, work, tr, dsc, n1, near, bloc, bias,
    memb, rstd, sums, vsum, va, vb, vd,
    ls, zs, zr, xs, xr, rs, rr, ss, sr, cs, cr,
    r1s, r1r, r2s, r2r, r3s, r3r, r4s, r4r, r5s, r5r, vs, vr,
):
    me = Place(n_t)
    length, width = x.shape
    rows = w.shape[2]
    heads = 3
    ch, half = rows // PLANE, rows // 2
    mine = span((me.c * CHIPS + me.q) * ch, ch)
    my_half = span(me.c * half, half)
    blocks = length // LANES
    far = n_t - 1

    def came(s):
        return lax.rem(me.t + far - s, n_t)

    def goes(s):
        return lax.rem(me.t + 1 + s, n_t)

    pieces = (
        (wq, 0, 128, 0), (wk, 0, 128, 128), (wv, 0, 128, 256), (wq, 128, 64, 384),
        (wv, 128, 64, 448), (wk, 128, 64, 512), (wo, 128, 64, 576), (wo, 0, 128, 640),
    )

    def local(k):
        if k > 0:
            return [pltpu.make_async_copy((wup, wdown)[k - 1], w.at[k, me.t], ls.at[7 + k])]
        return [
            pltpu.make_async_copy(
                src.at[pl.ds(at, size)], w.at[0, me.t, pl.ds(to, size)], ls.at[n]
            )
            for n, (src, at, size, to) in enumerate(pieces)
        ]

    def zcopy(k, s):
        place = w.at[k, me.t, mine]
        return remote(place, place, zs.at[k, s], zr.at[k, s], me.z(s + 1))

    def xcopy(k, s, j):
        place = w.at[k, came(s), mine]
        return remote(place, place, xs.at[k, s, j], xr.at[k, s, j], me.chip(j))

    def relay(k, s, j):
        start = (me.c * CHIPS + me.other(j)) * ch + j * (ch // 2)
        place = w.at[k, came(s), span(start, ch // 2)]
        return remote(place, place, rs.at[k, s, j], rr.at[k, s, j], me.chip(1 - j))

    def scopy(k, s):
        place = w.at[k, came(s), my_half]
        return remote(place, place, ss.at[k, s], sr.at[k, s], me.sibling())

    def bcopy(s):
        return remote(bloc, near.at[me.t], cs.at[s], cr.at[s], me.z(s + 1))

    def on_z(k, s):
        zcopy(k, s).wait_recv()
        for j in range(2):
            xcopy(k, s, j).start()

    def on_xy(k, s):
        for j in range(2):
            xcopy(k, s, j).wait_recv()
            relay(k, s, j).start()

    def on_relay(k, s):
        for j in range(2):
            relay(k, s, j).wait_recv()
        scopy(k, s).start()

    def slot(k):
        return 1 if k == 1 else 0

    def inbox(k):
        return act if k == 2 else a.at[k]

    def r1(k, s):
        return remote(
            g.at[slot(k), s, span((1 - me.c) * half, half)],
            inbox(k).at[s, span(0, half)], r1s.at[k, s], r1r.at[k, s], me.sibling(),
        )

    def quarter(q):
        return span(me.c * half + q * ch, ch)

    cut = ch // 2

    def sub(q, h):
        return span(me.c * half + q * ch + h * cut, cut)

    def r2(k, s, h, j):
        source = (me.other(h), me.other(2), me.other(1 - h))[j]
        return remote(
            g.at[slot(k), s, sub(source, h)], b.at[slot(k), s, j, span(h * cut, cut)],
            r2s.at[k, s, h, j], r2r.at[k, s, h, j], me.chip(1 - h if j == 2 else h),
        )

    def r3(k, s):
        return remote(b.at[slot(k), s, 0], d.at[k, s], r3s.at[k, s], r3r.at[k, s], me.z(s + 1))

    def r4(k, j):
        place = fout.at[k, mine]
        return remote(place, place, r4s.at[k, j], r4r.at[k, j], me.chip(j))

    def r5(k):
        place = fout.at[k, my_half]
        return remote(place, place, r5s.at[k], r5r.at[k], me.sibling())

    def on_r1(k, s):
        r1(k, s).wait_recv()

        @pl.loop(0, CHIPS)
        def _(m):
            src = span(me.c * half + m * ch, ch)
            g[slot(k), s, src] += inbox(k)[s, span(m * ch, ch)]

        for h in range(2):
            for j in range(2):
                r2(k, s, h, j).start()

    def on_r2(k, s):
        for h in range(2):
            rows_h = span(h * cut, cut)
            r2(k, s, h, 1).wait_recv()
            g[slot(k), s, sub(me.other(1 - h), h)] += b[slot(k), s, 1, rows_h]
            r2(k, s, h, 2).start()
            r2(k, s, h, 0).wait_recv()
            g[slot(k), s, sub(me.q, h)] += b[slot(k), s, 0, rows_h]

    def on_r2b(k, s, last):
        for h in range(2):
            r2(k, s, h, 2).wait_recv()
        b[slot(k), s, 0] = g[slot(k), s, quarter(me.q)] + b[slot(k), s, 2]
        if last is None:

            @pl.when(s < far)
            def _():
                r3(k, s).start()

        elif not last:
            r3(k, s).start()

    def on_r3(k):
        total = b[slot(k), far, 0].astype(F32)
        for s in range(far):
            r3(k, s).wait_recv()
            total = total + d[k, s].astype(F32)
        for s in range(far):
            r3(k, s).wait_send()
        fout[k, mine] = total.astype(BF16)
        for j in range(3):
            r4(k, j).start()

    def on_r4(k):
        for j in range(3):
            r4(k, j).wait_recv()
        r5(k).start()

    low_lanes = lax.broadcasted_iota(jnp.int32, (1, LANES), 1) < HEAD_DIM
    low = jnp.where(low_lanes, 1.0, 0.0).astype(BF16)
    high = jnp.where(low_lanes, 0.0, 1.0).astype(BF16)
    low32 = jnp.where(low_lanes, 1.0, 0.0)
    high32 = jnp.where(low_lanes, 0.0, 1.0)

    def band(i):
        lo = max(0, i * LANES - TEXT_MOST)
        return lo, min(length, (i + 1) * LANES + TEXT_MOST)

    def project(tt):
        @pl.loop(0, length // TILE)
        def _(m):
            r = span(m * TILE, TILE)
            xm = x[r, :]
            for lo, hi in ((0, 256), (256, 512), (512, 640)):
                piece = nt(xm, w[QKVO, tt, lo:hi, :])
                qkv[tt, r, lo:hi] = (
                    (piece + near[tt, 1:2, lo:hi]) * scales[:, lo:hi]
                ).astype(BF16)

    def attend(tt, some=None):
        for i in some or range(blocks):
            lo, hi = band(i)
            r = slice(i * LANES, (i + 1) * LANES)
            heads_in = (
                (qkv[tt, r, 0:128] * low, 128, 256),
                (qkv[tt, r, 0:128] * high, 128, 256),
                (qkv[tt, r, 384:512] * low, 512, 384),
            )
            outs = []
            for h, (q, kc, vc) in enumerate(heads_in):
                s = nt(q, qkv[tt, lo:hi, kc : kc + LANES]) + bias[r, 0 : hi - lo]
                e = jnp.exp(s - jnp.max(s, axis=-1, keepdims=True))
                p = (e * (1.0 / jnp.sum(e, axis=-1, keepdims=True))).astype(BF16)
                prob[tt, h, r, 0 : hi - lo] = p
                outs.append(nn(p, qkv[tt, lo:hi, vc : vc + LANES]))
            ctx[tt, r, 0:128] = (outs[2] * high32).astype(BF16)
            ctx[tt, r, 128:256] = (outs[0] * low32 + outs[1] * high32).astype(BF16)

    def attend_back(tt):
        for group in range(2):
            if group == 0:
                qc, kc, vc, dc = 0, 128, 256, 128
                hs = ((0, low, low, low32), (1, high, high, high32))
            else:
                qc, kc, vc, dc = 384, 512, 384, 0
                hs = ((2, low, high, low32),)
            dq = [None] * blocks
            for i in range(blocks):
                lo, hi = band(i)
                r = slice(i * LANES, (i + 1) * LANES)
                for n, (h, qm, vm, out_mask) in enumerate(hs):
                    dp = nt(dctx[r, dc : dc + LANES] * vm, qkv[tt, lo:hi, vc : vc + LANES])
                    p = prob[tt, h, r, 0 : hi - lo].astype(F32)
                    pd = p * dp
                    ds = (pd - p * jnp.sum(pd, axis=-1, keepdims=True)).astype(BF16)
                    dsc[n, r, 0 : hi - lo] = ds
                    part = nn(ds, qkv[tt, lo:hi, kc : kc + LANES]) * (
                        out_mask * (1.0 / math.sqrt(HEAD_DIM))
                    )
                    dq[i] = part if dq[i] is None else dq[i] + part
                if group == 0:
                    work[r, 0:128] = dq[i].astype(BF16)
            for j in range(blocks):
                rj = slice(j * LANES, (j + 1) * LANES)
                dk = dv = None
                for i in range(blocks):
                    lo, hi = band(i)
                    if not lo <= j * LANES < hi:
                        continue
                    r = slice(i * LANES, (i + 1) * LANES)
                    at = slice(j * LANES - lo, (j + 1) * LANES - lo)
                    for n, (h, qm, vm, _) in enumerate(hs):
                        more = tn(dsc[n, r, at], qkv[tt, r, qc : qc + LANES] * qm)
                        dk = more if dk is None else dk + more
                        more = tn(prob[tt, h, r, at], dctx[r, dc : dc + LANES] * vm)
                        dv = more if dv is None else dv + more
                if group == 0:
                    work[rj, 128:256] = dk.astype(BF16)
                    work[rj, 256:384] = dv.astype(BF16)
                else:
                    work[rj, 384:512] = (dq[j] + dv).astype(BF16)
                    work[rj, 512:640] = dk.astype(BF16)

    def add_sum(k, tile):
        n = tile.shape[0] // 8
        sums[k] += jnp.sum(tile.reshape(n, 8, tile.shape[1]), axis=0)

    def by_tiles(body):
        @pl.loop(0, length // 64)
        def _(m):
            for part in range(4):
                body(span(m * 64 + part * 16, 16))

    def transpose_to(src):
        @pl.loop(0, rows // TILE)
        def _(m):
            cols = span(m * TILE, TILE)
            tr[cols, :] = src[:, cols].T

    for k in range(3):
        for copy in local(k):
            copy.start()
    dy_in = pltpu.make_async_copy(dy, work, ls.at[10])
    dy_in.start()
    own = vecs[7:8, :]
    mid, end = own[:, 128:256], own[:, 256:384]
    turned = jnp.where(low_lanes, pltpu.roll(mid, HEAD_DIM, 1), pltpu.roll(end, HEAD_DIM, 1))
    bloc[...] = jnp.zeros_like(bloc)
    bloc[0:1, :] = vecs[6:7, :]
    bloc[1:2, 0:128] = own[:, 0:128]
    bloc[1:2, 256:384] = turned
    bloc[1:2, 384:512] = jnp.where(low_lanes, mid, end)
    near[me.t] = bloc[...]
    me.greet()
    for k in range(3):
        for copy in local(k):
            copy.wait()
        for s in range(far):
            zcopy(k, s).start()
        if k == 0:
            for s in range(far):
                bcopy(s).start()
    lane = lax.broadcasted_iota(jnp.int32, (1, 640), 1)
    is_query = (lane < 128) | ((lane >= 384) & (lane < 448))
    scales = jnp.where(is_query, 1.0 / math.sqrt(HEAD_DIM), 1.0)
    sums[...] = jnp.zeros_like(sums)
    labels = lax.broadcasted_iota(jnp.int32, (TEXTS, length), 0)
    memb[...] = jnp.where(seg[pl.ds(me.t, 1), :] == labels, 1.0, 0.0)
    for i in range(blocks):
        lo, hi = band(i)
        r = slice(i * LANES, (i + 1) * LANES)
        bias[r, 0 : hi - lo] = (tn(memb[:, r], memb[:, lo:hi]) - 1.0) * 1000000000.0
    project(me.t)
    on_z(QKVO, 0)
    attend(me.t, (0, 1))
    on_z(QKVO, 1)
    on_xy(QKVO, 0)
    attend(me.t, (2, 3))
    on_z(QKVO, 2)
    on_xy(QKVO, 1)
    on_relay(QKVO, 0)
    for s in range(far):
        bcopy(s).wait_recv()
    on_xy(QKVO, 2)

    @pl.loop(0, far)
    def _(s):
        tt = came(s)
        scopy(QKVO, s).wait_recv()
        project(tt)

        @pl.when(s < far - 1)
        def _():
            on_relay(QKVO, s + 1)

        attend(tt)
        on_z(UP, s)

        @pl.when(s > 0)
        def _():
            on_xy(UP, s - 1)

    @pl.loop(0, length // TILE)
    def _(m):
        r = span(m * TILE, TILE)
        for n in range(width // TILE):
            c = slice(n * TILE, (n + 1) * TILE)
            out = x[r, c].astype(F32) + vecs[0:1, c]
            for t in range(n_t):
                out = out + nn(ctx[t, r, :], w[QKVO, t, 512:768, c])
            acc[r, c] = out

    on_relay(UP, 0)

    @by_tiles
    def _(r):
        center = acc[r, :]
        center = center - jnp.mean(center, axis=-1, keepdims=True)
        inv = lax.rsqrt(jnp.mean(center * center, axis=-1, keepdims=True) + 1e-12)
        rstd[r, :] = inv
        center = center * inv
        n1[r, :] = center
        h1[r, :] = (center * vecs[1:2, :] + vecs[2:3, :]).astype(BF16)

    def rise(tt):
        @pl.loop(0, length // TILE)
        def _(m):
            r = span(m * TILE, TILE)
            hm = h1[r, :]
            for n in range(rows // TILE):
                c = slice(n * TILE, (n + 1) * TILE)
                up, slope = gelu_both(nn(hm, w[UP, tt, :, c]) + near[tt, 0:1, c])
                act[tt, r, c] = up.astype(BF16)
                dg[tt, r, c] = slope.astype(BF16)

    def fall(tt, first):
        @pl.loop(0, length // TILE)
        def _(m):
            r = span(m * TILE, TILE)
            am = act[tt, r, :]
            for n in range(width // TILE):
                c = slice(n * TILE, (n + 1) * TILE)
                out = nn(am, w[DOWN, tt, :, c])
                acc[r, c] = out if first else acc[r, c] + out

    on_z(DOWN, 0)
    rise(me.t)
    on_xy(UP, 2)
    on_relay(UP, 1)
    on_z(DOWN, 1)

    @pl.loop(0, far)
    def _(s):
        scopy(UP, s).wait_recv()
        rise(came(s))

        @pl.when(s == 0)
        def _():
            on_relay(UP, far - 1)
            on_z(DOWN, far - 1)

        on_xy(DOWN, s)

    on_relay(DOWN, 0)
    fall(me.t, True)

    @pl.loop(0, far)
    def _(s):
        @pl.when(s < far - 1)
        def _():
            on_relay(DOWN, s + 1)

        scopy(DOWN, s).wait_recv()
        fall(came(s), False)

    dy_in.wait()

    @by_tiles
    def _(r):
        center = acc[r, :] + vecs[3:4, :] + (n1[r, :] * vecs[1:2, :] + vecs[2:3, :])
        center = center - jnp.mean(center, axis=-1, keepdims=True)
        inv = lax.rsqrt(jnp.mean(center * center, axis=-1, keepdims=True) + 1e-12)
        n2 = center * inv
        final = n2 * vecs[4:5, :] + vecs[5:6, :]
        out = final.astype(BF16)
        layer_out[r, :] = out
        g[1, 1, r, :] = (final - out.astype(F32)).astype(BF16)
        dyt = work[r, :].astype(F32)
        dn = dyt * vecs[4:5, :]
        dyn = dyt * n2
        add_sum(1, dyn)
        add_sum(2, dyt)
        dr = inv * (
            dn
            - jnp.mean(dn, axis=-1, keepdims=True)
            - n2 * jnp.mean(dn * n2, axis=-1, keepdims=True)
        )
        add_sum(0, dr)
        acc[r, :] = dr
        dlow[r, :] = dr.astype(BF16)

    counts = jnp.sum(memb[...], axis=-1, keepdims=True)
    member = memb[...].astype(BF16)
    pooled[...] = (nn(member, layer_out[...]) + nn(member, g[1, 1, 0:length, :])) / counts

    ones = jnp.ones((8, length), BF16)

    def grad_to(k, s, left_t, right):
        @pl.loop(0, rows // TILE)
        def _(m):
            r = span(m * TILE, TILE)
            lt = left_t(r)
            for n in range(width // TILE):
                c = slice(n * TILE, (n + 1) * TILE)
                g[k, s, r, c] = nn(lt, right[:, c]).astype(BF16)

    @pl.loop(0, n_t)
    def _(s):
        tt = goes(s)
        grad_to(0, s, lambda r: act[tt, :, r].T, dlow)
        r1(0, s).start()

    transpose_to(h1)

    @pl.loop(0, n_t)
    def _(s):
        tt = goes(s)
        on_r1(0, s)

        @pl.loop(0, length // TILE)
        def _(m):
            r = span(m * TILE, TILE)
            dm = dlow[r, :]
            for n in range(rows // TILE):
                c = slice(n * TILE, (n + 1) * TILE)
                work[r, c] = (nt(dm, w[DOWN, tt, c, :]) * dg[tt, r, c].astype(F32)).astype(BF16)

        @pl.when(s > 0)
        def _():
            on_r1(1, s - 1)
            on_r2(0, s - 1)

        grad_to(1, s, lambda r: tr[r, :], work)
        r1(1, s).start()

        @pl.loop(0, length // TILE)
        def _(m):
            r = span(m * TILE, TILE)
            dm = work[r, :]
            for n in range(width // TILE):
                c = slice(n * TILE, (n + 1) * TILE)
                acc[r, c] += nt(dm, w[UP, tt, c, :])

        vsum[pl.ds(8 + tt, 1), :] = nn(ones, work[...])[0:1, :]

    on_r2(0, far)
    on_r1(1, far)

    @by_tiles
    def _(r):
        dh, nt1 = acc[r, :], n1[r, :]
        add_sum(4, dh * nt1)
        add_sum(5, dh)
        dn = dh * vecs[1:2, :]
        dr = rstd[r, :] * (
            dn
            - jnp.mean(dn, axis=-1, keepdims=True)
            - nt1 * jnp.mean(dn * nt1, axis=-1, keepdims=True)
        )
        add_sum(3, dr)
        acc[r, :] = dr
        dlow[r, :] = dr.astype(BF16)

    for s in range(n_t):
        on_r2b(0, s, s == far)
    for k, row in ((3, 0), (4, 1), (5, 2), (0, 3), (1, 4), (2, 5)):
        vsum[row : row + 1, :] = jnp.sum(sums[k], axis=0, keepdims=True)
    vsum[6:8, :] = jnp.zeros((2, width), F32)
    work[:, 640:768] = jnp.zeros((length, LANES), BF16)

    @pl.loop(0, n_t)
    def _(s):
        tt = goes(s)
        on_r2(1, s)

        @pl.loop(0, length // TILE)
        def _(m):
            r = span(m * TILE, TILE)
            out = nt(dlow[r, :], w[QKVO, tt, 512:768, :])
            dctx[r, 0:128] = (out[:, 0:128] * high32).astype(BF16)
            dctx[r, 128:256] = out[:, 128:256].astype(BF16)

        @pl.when(s == 0)
        def _():
            on_r3(0)

        attend_back(tt)
        on_r2b(1, s, None)

        @pl.when(s == 1)
        def _():
            on_r4(0)

        @pl.when(s > 0)
        def _():
            on_r1(2, s - 1)

        @pl.when(s > 1)
        def _():
            on_r2(2, s - 2)

        @pl.when(s == far)
        def _():
            on_r3(1)

        r1(0, s).wait_send()
        for h in range(2):
            for j in range(3):
                r2(0, s, h, j).wait_send()

        for m in range(rows // TILE):
            r = slice(m * TILE, (m + 1) * TILE)
            lt = work[:, r].T
            ct = ctx[tt].T if r.start == 512 else None
            for n in range(width // TILE):
                c = slice(n * TILE, (n + 1) * TILE)
                out = nn(lt, x[:, c])
                if ct is not None:
                    out = out + nn(ct, dlow[:, c])
                g[0, s, r, c] = out.astype(BF16)

        r1(2, s).start()

        @pl.loop(0, length // TILE)
        def _(m):
            r = span(m * TILE, TILE)
            dm = work[r, 0:640]
            for n in range(width // TILE):
                c = slice(n * TILE, (n + 1) * TILE)
                acc[r, c] += nn(dm, w[QKVO, tt, 0:640, c])

        vsum[pl.ds(12 + tt, 1), :] = nn(ones, work[...])[0:1, :]

    v1 = remote(vsum, va, vs.at[0], vr.at[0], me.sibling())
    v1.start()
    on_r1(2, far)
    v1.wait()
    vsum[...] = vsum[...] + va[...]
    v2 = [remote(vsum, vb.at[j], vs.at[1 + j], vr.at[1 + j], me.chip(j)) for j in range(3)]
    for c in v2:
        c.start()
    on_r2(2, far - 1)
    on_r2b(2, 0, False)
    on_r2b(2, 1, False)
    on_r4(1)
    on_r2(2, far)
    on_r2b(2, 2, False)
    for c in v2:
        c.wait()
    va[...] = vsum[...] + vb[0] + vb[1] + vb[2]
    v3 = [remote(va, vd.at[s], vs.at[4 + s], vr.at[4 + s], me.z(s + 1)) for s in range(far)]
    for c in v3:
        c.start()
    on_r2b(2, far, True)
    on_r3(2)
    for c in v3:
        c.wait()
    total = va[...]
    for s in range(far):
        total = total + vd[s]
    vsum[...] = total
    inner = width // n_t
    turns = lax.rem(width - me.t * inner, width)
    vout[...] = pltpu.roll(total[0:8, :], turns, 1)
    vout[6:7, :] = vsum[pl.ds(8 + me.t, 1), :]
    vout[7:8, :] = vsum[pl.ds(12 + me.t, 1), :]
    on_r4(2)
    for k in range(3):
        r5(k).wait_recv()

    for s in range(far):
        bcopy(s).wait_send()
    for k in range(3):
        for s in range(far):
            zcopy(k, s).wait_send()
            scopy(k, s).wait_send()
            for j in range(2):
                xcopy(k, s, j).wait_send()
                relay(k, s, j).wait_send()
        for s in range(n_t):
            if k > 0:
                r1(k, s).wait_send()
                for h in range(2):
                    for j in range(3):
                        r2(k, s, h, j).wait_send()
        for j in range(3):
            r4(k, j).wait_send()
        r5(k).wait_send()


def run_layer(wq, wk, wv, wo, wup, wdown, x, dy, seg, vecs, n_t):
    groups, (rows, cols) = 3, wup.shape
    length, width = x.shape
    ch, half, far = rows // PLANE, rows // 2, n_t - 1
    dma, vmem = pltpu.SemaphoreType.DMA, pltpu.VMEM
    here, there = pl.BlockSpec(memory_space=vmem), pl.BlockSpec(memory_space=pl.ANY)
    shape = jax.ShapeDtypeStruct
    pair = lambda *dims: [dma(dims), dma(dims)]
    return pl.pallas_call(
        functools.partial(layer_kernel, n_t),
        out_shape=(
            shape((length, width), BF16),
            shape((TEXTS, width), F32),
            shape((length, width), F32),
            shape((groups, rows, cols), BF16),
            shape((8, width), F32),
        ),
        in_specs=[there] * 6 + [here, there, here, here],
        out_specs=[here] * 5,
        scratch_shapes=[
            vmem((groups, n_t, rows, cols), BF16),
            vmem((2, n_t, rows, cols), BF16),
            vmem((2, n_t, half, cols), BF16),
            vmem((2, n_t, 3, ch, cols), BF16),
            vmem((groups, far, ch, cols), BF16),
            vmem((n_t, length, 640), BF16),
            vmem((n_t, length, 256), BF16),
            vmem((length, 256), BF16),
            vmem((n_t, 3, length, 384), BF16),
            vmem((n_t, length, rows), BF16),
            vmem((n_t, length, rows), BF16),
            vmem((length, width), BF16),
            vmem((length, width), BF16),
            vmem((length, width), BF16),
            vmem((width, length), BF16),
            vmem((2, length, 384), BF16),
            vmem((length, width), F32),
            vmem((n_t, 8, width), F32),
            vmem((8, width), F32),
            vmem((length, 384), F32),
            vmem((TEXTS, length), F32),
            vmem((length, 1), F32),
            vmem((6, 8, width), F32),
            vmem((16, width), F32),
            vmem((16, width), F32),
            vmem((3, 16, width), F32),
            vmem((far, 16, width), F32),
            dma((11,)),
            *pair(groups, far),
            *pair(groups, far, 2),
            *pair(groups, far, 2),
            *pair(groups, far),
            *pair(far),
            *pair(groups, n_t),
            *pair(groups, n_t, 2, 3),
            *pair(groups, far),
            *pair(groups, 3),
            *pair(groups),
            *pair(4 + far),
        ],
        compiler_params=pltpu.CompilerParams(
            collective_id=1, has_side_effects=True, vmem_limit_bytes=67043328
        ),
    )(wq, wk, wv, wo, wup, wdown, x, dy, seg, vecs)


def per_device(
    n_t, n_b,
    hidden_in, segment_ids, query_weight, query_bias, key_weight, value_weight, value_bias,
    out_weight, out_bias, attn_gain, attn_shift, up_weight, up_bias, down_weight, down_bias,
    ffn_gain, ffn_shift, cotangent,
):
    inner, width = out_weight.shape
    spare = jnp.zeros((width - 2 * inner,), F32)
    vecs = jnp.concatenate(
        [
            out_bias, attn_gain, attn_shift, down_bias, ffn_gain, ffn_shift, up_bias,
            query_bias, value_bias, spare,
        ]
    ).reshape(8, width)
    final, pooled, dx, fout, vout = run_layer(
        query_weight.T, key_weight.T, value_weight.T, out_weight, up_weight, down_weight,
        hidden_in[0], cotangent[0], segment_ids, vecs, n_t,
    )
    if n_b > PLANE:
        apart = [[i + PLANE * j for j in range(n_b // PLANE)] for i in range(PLANE)]
        fout, vout = lax.psum((fout.astype(F32), vout), "batch", axis_index_groups=apart)
    h = HEAD_DIM

    def rows_of(*spans):
        return jnp.concatenate([fout[2, h * lo : h * hi] for lo, hi in spans], axis=0).astype(F32)

    def lanes_of(*spans):
        return jnp.concatenate([vout[7, h * lo : h * hi] for lo, hi in spans])

    return (
        final[None],
        pooled[None],
        dx[None],
        rows_of((0, 2), (6, 7)).T,
        lanes_of((0, 2), (6, 7)),
        rows_of((2, 4), (8, 9)).T,
        rows_of((4, 6), (7, 8)).T,
        lanes_of((4, 6), (7, 8)),
        rows_of((10, 12), (9, 10)),
        vout[0, :inner],
        vout[1, :inner],
        vout[2, :inner],
        fout[1].astype(F32),
        vout[6],
        fout[0].astype(F32),
        vout[3, :inner],
        vout[4, :inner],
        vout[5, :inner],
    )


def solution(mesh):
    rows, tens = P(("batch", "tensor"), None, None), P("tensor")
    col, row = P(None, "tensor"), P("tensor", None)
    in_specs = (
        rows, P("batch", None), col, tens, col, col, tens, row, P(), P(), P(), col, tens, row,
        P(), P(), P(), rows,
    )
    out_specs = (
        rows, rows, rows, col, tens, col, col, tens, row, tens, tens, tens, col, tens, row, tens,
        tens, tens,
    )
    body = functools.partial(per_device, mesh.shape["tensor"], mesh.shape["batch"])
    return jax.shard_map(
        body, mesh=mesh, in_specs=in_specs, out_specs=out_specs, check_vma=False
    )
```

```python
import functools
import math

import jax
import jax.numpy as jnp
from jax import lax
from jax.experimental import pallas as pl
from jax.experimental.pallas import tpu as pltpu
from jax.sharding import PartitionSpec as P

HEAD_DIM = 64
TEXTS = 8
TEXT_MOST = 128
PLANE = 8
CHIPS = 4
LANES = 128
TILE = 256
MESH = pl.DeviceIdType.MESH
F32 = jnp.float32
BF16 = jnp.bfloat16
QKVO, UP, DOWN = 0, 1, 2
ERFC_STEP = 0.43
ERFC_POLY = (
    0.24251981500369507,
    0.24429385145717694,
    0.2054723295686731,
    0.24508130662046312,
    -0.0823056340674522,
    0.3798888788682746,
    -0.3080966384375393,
    0.07314607841870144,
)


class Place:
    def __init__(self, n_t):
        bi = lax.axis_index("batch")
        self.t = lax.axis_index("tensor")
        self.n_t = n_t
        self.r = lax.rem(bi, PLANE)
        self.base = bi - self.r
        self.c = lax.rem(self.r, 2)
        self.q = self.r // 2
        self.x = lax.rem(self.q, 2)
        self.y = self.q // 2

    def z(self, step):
        return {"batch": self.base + self.r, "tensor": lax.rem(self.t + step, self.n_t)}

    def line(self, way):
        step = 1 if way == 0 else self.n_t - 1
        return {"batch": self.base + self.r, "tensor": lax.rem(self.t + step, self.n_t)}

    def other(self, axis):
        y = self.y if axis == 0 else 1 - self.y
        x = self.x if axis == 1 else 1 - self.x
        return y * 2 + x

    def chip(self, axis):
        return {"batch": self.base + self.other(axis) * 2 + self.c, "tensor": self.t}

    def sibling(self):
        return {"batch": self.base + self.q * 2 + 1 - self.c, "tensor": self.t}

    def greet(self):
        barrier = pltpu.get_barrier_semaphore()
        peers = [self.z(s) for s in range(1, self.n_t)]
        peers += [self.chip(j) for j in range(3)] + [self.sibling()]
        for peer in peers:
            pl.semaphore_signal(barrier, inc=1, device_id=peer, device_id_type=MESH)
        pl.semaphore_wait(barrier, len(peers))


def remote(src, dst, send, recv, dev):
    return pltpu.make_async_remote_copy(
        src_ref=src, dst_ref=dst, send_sem=send, recv_sem=recv, device_id=dev, device_id_type=MESH
    )


def span(start, size):
    return pl.ds(start if isinstance(start, int) else pl.multiple_of(start, size), size)


def nn(left, right):
    return jnp.dot(left, right, preferred_element_type=F32)


def nt(left, right):
    return lax.dot_general(left, right, (((1,), (1,)), ((), ())), preferred_element_type=F32)


def tn(left, right):
    return lax.dot_general(left, right, (((0,), (0,)), ((), ())), preferred_element_type=F32)


def gelu_both(x):
    t = 1.0 / (1.0 + (ERFC_STEP * math.sqrt(0.5)) * jnp.abs(x))
    poly = jnp.full_like(x, ERFC_POLY[-1])
    for c in ERFC_POLY[-2::-1]:
        poly = poly * t + c
    bell = jnp.exp(x * x * -0.5)
    tail = 0.5 * (poly * t) * bell
    cdf = jnp.where(x > 0, 1.0 - tail, tail)
    return x * cdf, cdf + x * (bell * (1.0 / math.sqrt(2.0 * math.pi)))


def layer_kernel(
    n_t,
    wq, wk, wv, wo, wup, wdown, x, dy, seg, vecs,
    layer_out, pooled, acc, fout, vout,
    w, g, a, b, d, qkv, ctx, dctx, prob, act, dg, h1, dlow, work, tr, dsc, n1, near, bloc, bias,
    memb, rstd, sums, vsum, va, vb, vd,
    ls, zs, zr, xs, xr, rs, rr, ss, sr, cs, cr,
    r1s, r1r, r2s, r2r, r3s, r3r, r4s, r4r, r5s, r5r, vs, vr,
):
    me = Place(n_t)
    length, width = x.shape
    rows = w.shape[2]
    heads = 3
    ch, half = rows // PLANE, rows // 2
    mine = span((me.c * CHIPS + me.q) * ch, ch)
    my_half = span(me.c * half, half)
    blocks = length // LANES
    far = n_t - 1

    order = [sorted((abs(i - j), j) for j in range(n_t) if j != i) for i in range(n_t)]

    def pick(index, values):
        out = values[-1]
        for i in range(len(values) - 2, -1, -1):
            out = jnp.where(index == i, values[i], out)
        return out

    near_first = [pick(me.t, [jnp.int32(row[e][1]) for row in order]) for e in range(far)]

    def came(s):
        return near_first[s] if isinstance(s, int) else pick(s, near_first)

    def goes(s):
        return lax.rem(me.t + 1 + s, n_t)

    inner = rows // 4

    def local(k):
        if k > 0:
            return [pltpu.make_async_copy((wup, wdown)[k - 1], w.at[k, me.t], ls.at[3 + k])]
        return [
            pltpu.make_async_copy(src, w.at[0, me.t, pl.ds(n * inner, inner)], ls.at[n])
            for n, src in enumerate((wq, wk, wv, wo))
        ]

    def zown(k, way):
        place = w.at[k, me.t, mine]
        return remote(place, place, zs.at[k, far + way], zr.at[k, me.t], me.line(way))

    def zrecv(k, s):
        place = w.at[k, came(s), mine]
        return remote(place, place, zs.at[k, s], zr.at[k, came(s)], me.line(0))

    def zpass(k, s, act_on):
        src = came(s)
        place = w.at[k, src, mine]
        for way in range(2):
            goes_on = (src < me.t) & (me.t < far) if way == 0 else (src > me.t) & (me.t > 0)

            @pl.when(goes_on)
            def _():
                act_on(remote(place, place, zs.at[k, s], zr.at[k, src], me.line(way)))

    def zends(k, act_on):
        @pl.when(me.t < far)
        def _():
            act_on(zown(k, 0))

        @pl.when(me.t > 0)
        def _():
            act_on(zown(k, 1))

    def xcopy(k, s, j):
        place = w.at[k, came(s), mine]
        return remote(place, place, xs.at[k, s, j], xr.at[k, s, j], me.chip(j))

    def relay(k, s, j):
        start = (me.c * CHIPS + me.other(j)) * ch + j * (ch // 2)
        place = w.at[k, came(s), span(start, ch // 2)]
        return remote(place, place, rs.at[k, s, j], rr.at[k, s, j], me.chip(1 - j))

    def scopy(k, s):
        place = w.at[k, came(s), my_half]
        return remote(place, place, ss.at[k, s], sr.at[k, s], me.sibling())

    def bcopy(s):
        return remote(bloc, near.at[me.t], cs.at[s], cr.at[s], me.z(s + 1))

    def on_z(k, s):
        zrecv(k, s).wait_recv()
        zpass(k, s, lambda c: c.start())
        for j in range(2):
            xcopy(k, s, j).start()

    def on_xy(k, s):
        for j in range(2):
            xcopy(k, s, j).wait_recv()
            relay(k, s, j).start()

    def on_relay(k, s):
        for j in range(2):
            relay(k, s, j).wait_recv()
        scopy(k, s).start()

    def slot(k):
        return 1 if k == 1 else 0

    def inbox(k):
        return act if k == 2 else a.at[k]

    def r1(k, s):
        return remote(
            g.at[slot(k), s, span((1 - me.c) * half, half)],
            inbox(k).at[s, span(0, half)], r1s.at[k, s], r1r.at[k, s], me.sibling(),
        )

    def quarter(q):
        return span(me.c * half + q * ch, ch)

    cut = ch // 2

    def sub(q, h):
        return span(me.c * half + q * ch + h * cut, cut)

    def r2(k, s, h, j):
        source = (me.other(h), me.other(2), me.other(1 - h))[j]
        return remote(
            g.at[slot(k), s, sub(source, h)], b.at[k, s, j, span(h * cut, cut)],
            r2s.at[k, s, h, j], r2r.at[k, s, h, j], me.chip(1 - h if j == 2 else h),
        )

    def r3(k, s):
        return remote(b.at[k, s, 0], d.at[k, s], r3s.at[k, s], r3r.at[k, s], me.z(s + 1))

    def r4(k, j):
        place = fout.at[k, mine]
        return remote(place, place, r4s.at[k, j], r4r.at[k, j], me.chip(j))

    def r5(k):
        place = fout.at[k, my_half]
        return remote(place, place, r5s.at[k], r5r.at[k], me.sibling())

    def on_r1(k, s):
        r1(k, s).wait_recv()

        @pl.loop(0, CHIPS)
        def _(m):
            src = span(me.c * half + m * ch, ch)
            g[slot(k), s, src] += inbox(k)[s, span(m * ch, ch)]

        for h in range(2):
            for j in range(2):
                r2(k, s, h, j).start()

    def on_r2(k, s):
        for h in range(2):
            rows_h = span(h * cut, cut)
            r2(k, s, h, 1).wait_recv()
            g[slot(k), s, sub(me.other(1 - h), h)] += b[k, s, 1, rows_h]
            r2(k, s, h, 2).start()
            r2(k, s, h, 0).wait_recv()
            g[slot(k), s, sub(me.q, h)] += b[k, s, 0, rows_h]

    def on_r2b(k, s, last):
        for h in range(2):
            r2(k, s, h, 2).wait_recv()
        b[k, s, 0] = g[slot(k), s, quarter(me.q)] + b[k, s, 2]
        if last is None:

            @pl.when(s < far)
            def _():
                r3(k, s).start()

        elif not last:
            r3(k, s).start()

    def on_r3(k):
        total = b[k, far, 0].astype(F32)
        for s in range(far):
            r3(k, s).wait_recv()
            total = total + d[k, s].astype(F32)
        for s in range(far):
            r3(k, s).wait_send()
        fout[k, mine] = total.astype(BF16)
        for j in range(3):
            r4(k, j).start()

    def on_r4(k):
        for j in range(3):
            r4(k, j).wait_recv()
        r5(k).start()

    def pair_sum(n):
        return remote(vsum.at[n], va.at[n], vs.at[n, 0], vr.at[n, 0], me.sibling())

    def plane_sum(n, j):
        return remote(vsum.at[n], vb.at[n, j], vs.at[n, 1 + j], vr.at[n, 1 + j], me.chip(j))

    def line_sum(n, s):
        return remote(va.at[n], vd.at[n, s], vs.at[n, 4 + s], vr.at[n, 4 + s], me.z(s + 1))

    def on_pair(n):
        pair_sum(n).wait()
        vsum[n] += va[n]
        for j in range(3):
            plane_sum(n, j).start()

    def on_plane(n):
        for j in range(3):
            plane_sum(n, j).wait()
        va[n] = vsum[n] + vb[n, 0] + vb[n, 1] + vb[n, 2]
        for s in range(far):
            line_sum(n, s).start()

    def on_line(n):
        for s in range(far):
            line_sum(n, s).wait()
        total = va[n]
        for s in range(far):
            total = total + vd[n, s]
        return total

    low_lanes = lax.broadcasted_iota(jnp.int32, (1, LANES), 1) < HEAD_DIM
    low = jnp.where(low_lanes, 1.0, 0.0).astype(BF16)
    high = jnp.where(low_lanes, 0.0, 1.0).astype(BF16)
    low32 = jnp.where(low_lanes, 1.0, 0.0)
    high32 = jnp.where(low_lanes, 0.0, 1.0)

    def band(i):
        lo = max(0, i * LANES - TEXT_MOST)
        return lo, min(length, (i + 1) * LANES + TEXT_MOST)

    q01, k01, v01, o01 = (0, 128), (192, 320), (384, 512), (576, 704)
    q2, k2, v2, o2 = (128, 192), (320, 384), (512, 576), (704, 768)

    def picked(tt, spans, cols=slice(None)):
        return jnp.concatenate([w[QKVO, tt, lo:hi, cols] for lo, hi in spans], axis=0)

    def project(tt):
        @pl.loop(0, length // TILE)
        def _(m):
            r = span(m * TILE, TILE)
            xm = x[r, :]
            for lo, hi, spans in (
                (0, 256, (q01, k01)), (256, 512, (v01, q2, v2)), (512, 640, (k2, o2)),
            ):
                piece = nt(xm, picked(tt, spans))
                qkv[tt, r, lo:hi] = (
                    (piece + near[tt, 1:2, lo:hi]) * scales[:, lo:hi]
                ).astype(BF16)

    def attend(tt, some=None):
        for i in some or range(blocks):
            lo, hi = band(i)
            r = slice(i * LANES, (i + 1) * LANES)
            heads_in = (
                (qkv[tt, r, 0:128] * low, 128, 256),
                (qkv[tt, r, 0:128] * high, 128, 256),
                (qkv[tt, r, 384:512] * low, 512, 384),
            )
            sc = [
                nt(q, qkv[tt, lo:hi, kc : kc + LANES]) + bias[r, 0 : hi - lo]
                for q, kc, _ in heads_in
            ]
            ex = [jnp.exp(z - jnp.max(z, axis=-1, keepdims=True)) for z in sc]
            ps = [(e * (1.0 / jnp.sum(e, axis=-1, keepdims=True))).astype(BF16) for e in ex]
            for h, p in enumerate(ps):
                prob[tt, h, r, 0 : hi - lo] = p
            outs = [
                nn(p, qkv[tt, lo:hi, vc : vc + LANES]) for p, (_, _, vc) in zip(ps, heads_in)
            ]
            ctx[tt, r, 0:128] = (outs[2] * high32).astype(BF16)
            ctx[tt, r, 128:256] = (outs[0] * low32 + outs[1] * high32).astype(BF16)

    def attend_back(tt):
        for group in range(2):
            if group == 0:
                qc, kc, vc, dc = 0, 128, 256, 128
                hs = ((0, low, low, low32), (1, high, high, high32))
            else:
                qc, kc, vc, dc = 384, 512, 384, 0
                hs = ((2, low, high, low32),)
            dq = [None] * blocks
            for i in range(blocks):
                lo, hi = band(i)
                r = slice(i * LANES, (i + 1) * LANES)
                for n, (h, qm, vm, out_mask) in enumerate(hs):
                    dp = nt(dctx[r, dc : dc + LANES] * vm, qkv[tt, lo:hi, vc : vc + LANES])
                    p = prob[tt, h, r, 0 : hi - lo].astype(F32)
                    pd = p * dp
                    ds = (pd - p * jnp.sum(pd, axis=-1, keepdims=True)).astype(BF16)
                    dsc[n, r, 0 : hi - lo] = ds
                    part = nn(ds, qkv[tt, lo:hi, kc : kc + LANES]) * (
                        out_mask * (1.0 / math.sqrt(HEAD_DIM))
                    )
                    dq[i] = part if dq[i] is None else dq[i] + part
                if group == 0:
                    work[r, 0:128] = dq[i].astype(BF16)
            for j in range(blocks):
                rj = slice(j * LANES, (j + 1) * LANES)
                dk = dv = None
                for i in range(blocks):
                    lo, hi = band(i)
                    if not lo <= j * LANES < hi:
                        continue
                    r = slice(i * LANES, (i + 1) * LANES)
                    at = slice(j * LANES - lo, (j + 1) * LANES - lo)
                    for n, (h, qm, vm, _) in enumerate(hs):
                        more = tn(dsc[n, r, at], qkv[tt, r, qc : qc + LANES] * qm)
                        dk = more if dk is None else dk + more
                        more = tn(prob[tt, h, r, at], dctx[r, dc : dc + LANES] * vm)
                        dv = more if dv is None else dv + more
                if group == 0:
                    work[rj, 128:256] = dk.astype(BF16)
                    work[rj, 256:384] = dv.astype(BF16)
                else:
                    work[rj, 384:512] = (dq[j] + dv).astype(BF16)
                    work[rj, 512:640] = dk.astype(BF16)

    def add_sum(k, tile):
        n = tile.shape[0] // 8
        sums[k] += jnp.sum(tile.reshape(n, 8, tile.shape[1]), axis=0)

    def by_tiles(body):
        @pl.loop(0, length // 64)
        def _(m):
            body(span(m * 64, 64))

    def transpose_to(src):
        @pl.loop(0, rows // TILE)
        def _(m):
            cols = span(m * TILE, TILE)
            tr[cols, :] = src[:, cols].T

    for k in range(3):
        for copy in local(k):
            copy.start()
    dy_in = pltpu.make_async_copy(dy, work, ls.at[6])
    dy_in.start()
    own = vecs[7:8, :]
    mid, end = own[:, 128:256], own[:, 256:384]
    turned = jnp.where(low_lanes, pltpu.roll(mid, HEAD_DIM, 1), pltpu.roll(end, HEAD_DIM, 1))
    bloc[...] = jnp.zeros_like(bloc)
    bloc[0:1, :] = vecs[6:7, :]
    bloc[1:2, 0:128] = own[:, 0:128]
    bloc[1:2, 256:384] = turned
    bloc[1:2, 384:512] = jnp.where(low_lanes, mid, end)
    near[me.t] = bloc[...]
    me.greet()
    for s in range(far):
        bcopy(s).start()
    for k in range(3):
        for copy in local(k):
            copy.wait()
        zends(k, lambda c: c.start())
    lane = lax.broadcasted_iota(jnp.int32, (1, 640), 1)
    is_query = (lane < 128) | ((lane >= 384) & (lane < 448))
    scales = jnp.where(is_query, 1.0 / math.sqrt(HEAD_DIM), 1.0)
    sums[...] = jnp.zeros_like(sums)
    labels = lax.broadcasted_iota(jnp.int32, (TEXTS, length), 0)
    memb[...] = jnp.where(seg[pl.ds(me.t, 1), :] == labels, 1.0, 0.0)
    for i in range(blocks):
        lo, hi = band(i)
        r = slice(i * LANES, (i + 1) * LANES)
        bias[r, 0 : hi - lo] = (tn(memb[:, r], memb[:, lo:hi]) - 1.0) * 1000000000.0
    project(me.t)
    on_z(QKVO, 0)
    attend(me.t, (0, 1))
    on_z(QKVO, 1)
    on_xy(QKVO, 0)
    attend(me.t, (2, 3))
    on_z(QKVO, 2)
    on_xy(QKVO, 1)
    on_relay(QKVO, 0)
    for s in range(far):
        bcopy(s).wait_recv()
    on_xy(QKVO, 2)

    @pl.loop(0, far)
    def _(s):
        tt = came(s)
        scopy(QKVO, s).wait_recv()
        project(tt)

        @pl.when(s < far - 1)
        def _():
            on_relay(QKVO, s + 1)

        attend(tt)
        on_z(UP, s)

        @pl.when(s > 0)
        def _():
            on_xy(UP, s - 1)

    @pl.loop(0, length // TILE)
    def _(m):
        r = span(m * TILE, TILE)
        for n in range(width // TILE):
            c = slice(n * TILE, (n + 1) * TILE)
            out = x[r, c].astype(F32) + vecs[0:1, c]
            for t in range(n_t):
                out = out + nn(ctx[t, r, :], picked(t, (k2, o2, o01), c))
            acc[r, c] = out

    on_relay(UP, 0)

    @by_tiles
    def _(r):
        center = acc[r, :]
        center = center - jnp.mean(center, axis=-1, keepdims=True)
        inv = lax.rsqrt(jnp.mean(center * center, axis=-1, keepdims=True) + 1e-12)
        rstd[r, :] = inv
        center = center * inv
        n1[r, :] = center
        h1[r, :] = (center * vecs[1:2, :] + vecs[2:3, :]).astype(BF16)

    def rise(tt):
        @pl.loop(0, length // TILE)
        def _(m):
            r = span(m * TILE, TILE)
            hm = h1[r, :]
            for n in range(rows // TILE):
                c = slice(n * TILE, (n + 1) * TILE)
                up, slope = gelu_both(nn(hm, w[UP, tt, :, c]) + near[tt, 0:1, c])
                act[tt, r, c] = up.astype(BF16)
                dg[tt, r, c] = slope.astype(BF16)

    def fall(tt, first):
        @pl.loop(0, length // TILE)
        def _(m):
            r = span(m * TILE, TILE)
            am = act[tt, r, :]
            for n in range(width // TILE):
                c = slice(n * TILE, (n + 1) * TILE)
                out = nn(am, w[DOWN, tt, :, c])
                acc[r, c] = out if first else acc[r, c] + out

    on_z(DOWN, 0)
    rise(me.t)
    on_xy(UP, 2)
    on_relay(UP, 1)
    on_z(DOWN, 1)

    @pl.loop(0, far)
    def _(s):
        scopy(UP, s).wait_recv()
        rise(came(s))

        @pl.when(s == 0)
        def _():
            on_relay(UP, far - 1)
            on_z(DOWN, far - 1)

        on_xy(DOWN, s)

    on_relay(DOWN, 0)
    fall(me.t, True)

    @pl.loop(0, far)
    def _(s):
        @pl.when(s < far - 1)
        def _():
            on_relay(DOWN, s + 1)

        scopy(DOWN, s).wait_recv()
        fall(came(s), False)

    dy_in.wait()

    @by_tiles
    def _(r):
        dyt = work[r, :].astype(F32)
        center = acc[r, :] + vecs[3:4, :] + (n1[r, :] * vecs[1:2, :] + vecs[2:3, :])
        center = center - jnp.mean(center, axis=-1, keepdims=True)
        inv = lax.rsqrt(jnp.mean(center * center, axis=-1, keepdims=True) + 1e-12)
        n2 = center * inv
        final = n2 * vecs[4:5, :] + vecs[5:6, :]
        out = final.astype(BF16)
        dn = dyt * vecs[4:5, :]
        dr = inv * (
            dn
            - jnp.mean(dn, axis=-1, keepdims=True)
            - n2 * jnp.mean(dn * n2, axis=-1, keepdims=True)
        )
        layer_out[r, :] = out
        g[1, 1, r, :] = (final - out.astype(F32)).astype(BF16)
        acc[r, :] = dr
        dlow[r, :] = dr.astype(BF16)
        add_sum(0, dr)
        add_sum(1, dyt * n2)
        add_sum(2, dyt)

    counts = jnp.sum(memb[...], axis=-1, keepdims=True)
    member = memb[...].astype(BF16)
    pooled[...] = (nn(member, layer_out[...]) + nn(member, g[1, 1, 0:length, :])) / counts

    ones = jnp.ones((8, length), BF16)

    def grad_to(k, s, left_t, right):
        @pl.loop(0, rows // TILE)
        def _(m):
            r = span(m * TILE, TILE)
            lt = left_t(r)
            for n in range(width // TILE):
                c = slice(n * TILE, (n + 1) * TILE)
                g[k, s, r, c] = nn(lt, right[:, c]).astype(BF16)

    @pl.loop(0, n_t)
    def _(s):
        tt = goes(s)
        grad_to(0, s, lambda r: act[tt, :, r].T, dlow)
        r1(0, s).start()

        @pl.when(s > 0)
        def _():
            on_r1(0, s - 1)

    transpose_to(h1)
    on_r1(0, far)

    @pl.loop(0, n_t)
    def _(s):
        tt = goes(s)

        @pl.loop(0, length // TILE)
        def _(m):
            r = span(m * TILE, TILE)
            dm = dlow[r, :]
            for n in range(rows // TILE):
                c = slice(n * TILE, (n + 1) * TILE)
                work[r, c] = (nt(dm, w[DOWN, tt, c, :]) * dg[tt, r, c].astype(F32)).astype(BF16)

        @pl.when(s > 0)
        def _():
            on_r1(1, s - 1)

        grad_to(1, s, lambda r: tr[r, :], work)
        r1(1, s).start()

        @pl.loop(0, length // TILE)
        def _(m):
            r = span(m * TILE, TILE)
            dm = work[r, :]
            for n in range(width // TILE):
                c = slice(n * TILE, (n + 1) * TILE)
                acc[r, c] += nt(dm, w[UP, tt, c, :])

        vsum[1, pl.ds(tt, 1), :] = nn(ones, work[...])[0:1, :]
        on_r2(0, s)

    on_r1(1, far)

    @by_tiles
    def _(r):
        dh, nt1 = acc[r, :], n1[r, :]
        dn = dh * vecs[1:2, :]
        dr = rstd[r, :] * (
            dn
            - jnp.mean(dn, axis=-1, keepdims=True)
            - nt1 * jnp.mean(dn * nt1, axis=-1, keepdims=True)
        )
        acc[r, :] = dr
        dlow[r, :] = dr.astype(BF16)
        add_sum(3, dr)
        add_sum(4, dh * nt1)
        add_sum(5, dh)

    on_r2b(0, 0, False)
    on_r2b(0, 1, False)
    vsum[0] = jnp.zeros((8, width), F32)
    for k, row in ((3, 0), (4, 1), (5, 2), (0, 3), (1, 4), (2, 5)):
        vsum[0, row : row + 1, :] = jnp.sum(sums[k], axis=0, keepdims=True)
    pair_sum(0).start()
    work[:, 640:768] = jnp.zeros((length, LANES), BF16)

    @pl.loop(0, n_t)
    def _(s):
        tt = goes(s)

        @pl.loop(0, length // TILE)
        def _(m):
            r = span(m * TILE, TILE)
            out = nt(dlow[r, :], picked(tt, (k2, o2, o01)))
            dctx[r, 0:128] = (out[:, 0:128] * high32).astype(BF16)
            dctx[r, 128:256] = out[:, 128:256].astype(BF16)

        attend_back(tt)

        @pl.when(s == 0)
        def _():
            on_pair(0)
            on_r2b(0, 2, False)
            on_r2(1, 0)
            on_r2(1, 1)

        @pl.when(s == 1)
        def _():
            on_r2b(0, 3, True)
            on_r2(1, 2)
            on_r2(1, 3)

        @pl.when(s == 2)
        def _():
            on_r3(0)
            on_plane(0)
            on_r2b(1, 0, False)

        @pl.when(s == 3)
        def _():
            on_r2b(1, 1, False)
            on_r2b(1, 2, False)

        r1(0, s).wait_send()
        for h in range(2):
            for j in range(3):
                r2(0, s, h, j).wait_send()

        for m in range(rows // TILE):
            r = slice(m * TILE, (m + 1) * TILE)
            lt = work[:, r].T
            ct = ctx[tt].T if r.start == 512 else None
            for n in range(width // TILE):
                c = slice(n * TILE, (n + 1) * TILE)
                out = nn(lt, x[:, c])
                if ct is not None:
                    out = out + nn(ct, dlow[:, c])
                out = out.astype(BF16)
                at = 0
                for lo, hi in ((q01, k01), (v01, q2, v2), (k2, o2, o01))[m]:
                    g[0, s, lo:hi, c] = out[at : at + hi - lo, :]
                    at += hi - lo

        r1(2, s).start()

        @pl.loop(0, length // TILE)
        def _(m):
            r = span(m * TILE, TILE)
            dm = work[r, 0:640]
            for n in range(width // TILE):
                c = slice(n * TILE, (n + 1) * TILE)
                acc[r, c] += nn(dm, picked(tt, (q01, k01, v01, q2, v2, k2, o2), c))

        vsum[1, pl.ds(4 + tt, 1), :] = nn(ones, work[...])[0:1, :]

        @pl.when(s > 0)
        def _():
            on_r1(2, s - 1)

    pair_sum(1).start()
    on_r1(2, far)
    on_r2b(1, far, True)
    on_pair(1)
    on_r4(0)
    on_r2(2, 0)
    on_r2(2, 1)
    on_r2(2, 2)
    on_plane(1)
    on_r2b(2, 0, False)
    on_r2(2, far)
    on_r3(1)
    turns = lax.rem(width - me.t * (width // n_t), width)
    vout[0:8, :] = pltpu.roll(on_line(0), turns, 1)
    vout[8:16, :] = jnp.zeros((8, width), F32)
    on_r2b(2, 1, False)
    on_r2b(2, 2, False)
    vsum[1] = on_line(1)
    mine_row = vsum[1, pl.ds(4 + me.t, 1), :]
    vout[6:7, 0:128] = mine_row[:, 0:128]
    vout[6:7, 128:256] = mine_row[:, 384:512]
    vout[7:8, 0:128] = mine_row[:, 256:384]
    vout[7:8, 128:256] = pltpu.roll(mine_row[:, 384:512], HEAD_DIM, 1)
    vout[8:9, :] = vsum[1, pl.ds(me.t, 1), :]
    on_r2b(2, far, True)
    on_r3(2)
    on_r4(1)
    on_r4(2)
    for k in range(3):
        r5(k).wait_recv()

    for s in range(far):
        bcopy(s).wait_send()
    for k in range(3):
        zends(k, lambda c: c.wait_send())
        for s in range(far):
            zpass(k, s, lambda c: c.wait_send())
            scopy(k, s).wait_send()
            for j in range(2):
                xcopy(k, s, j).wait_send()
                relay(k, s, j).wait_send()
        for s in range(n_t):
            if k > 0:
                r1(k, s).wait_send()
                for h in range(2):
                    for j in range(3):
                        r2(k, s, h, j).wait_send()
        for j in range(3):
            r4(k, j).wait_send()
        r5(k).wait_send()


def run_layer(wq, wk, wv, wo, wup, wdown, x, dy, seg, vecs, n_t):
    groups, (rows, cols) = 3, wup.shape
    length, width = x.shape
    ch, half, far = rows // PLANE, rows // 2, n_t - 1
    dma, vmem = pltpu.SemaphoreType.DMA, pltpu.VMEM
    here, there = pl.BlockSpec(memory_space=vmem), pl.BlockSpec(memory_space=pl.ANY)
    shape = jax.ShapeDtypeStruct
    pair = lambda *dims: [dma(dims), dma(dims)]
    return pl.pallas_call(
        functools.partial(layer_kernel, n_t),
        out_shape=(
            shape((length, width), BF16),
            shape((TEXTS, width), F32),
            shape((length, width), F32),
            shape((groups, rows, cols), BF16),
            shape((16, width), F32),
        ),
        in_specs=[there] * 6 + [here, there, here, here],
        out_specs=[here] * 5,
        scratch_shapes=[
            vmem((groups, n_t, rows, cols), BF16),
            vmem((2, n_t, rows, cols), BF16),
            vmem((2, n_t, half, cols), BF16),
            vmem((groups, n_t, 3, ch, cols), BF16),
            vmem((groups, far, ch, cols), BF16),
            vmem((n_t, length, 640), BF16),
            vmem((n_t, length, 256), BF16),
            vmem((length, 256), BF16),
            vmem((n_t, 3, length, 384), BF16),
            vmem((n_t, length, rows), BF16),
            vmem((n_t, length, rows), BF16),
            vmem((length, width), BF16),
            vmem((length, width), BF16),
            vmem((length, width), BF16),
            vmem((width, length), BF16),
            vmem((2, length, 384), BF16),
            vmem((length, width), F32),
            vmem((n_t, 8, width), F32),
            vmem((8, width), F32),
            vmem((length, 384), F32),
            vmem((TEXTS, length), F32),
            vmem((length, 1), F32),
            vmem((6, 8, width), F32),
            vmem((2, 8, width), F32),
            vmem((2, 8, width), F32),
            vmem((2, 3, 8, width), F32),
            vmem((2, far, 8, width), F32),
            dma((7,)),
            dma((groups, far + 2)),
            dma((groups, n_t)),
            *pair(groups, far, 2),
            *pair(groups, far, 2),
            *pair(groups, far),
            *pair(far),
            *pair(groups, n_t),
            *pair(groups, n_t, 2, 3),
            *pair(groups, far),
            *pair(groups, 3),
            *pair(groups),
            *pair(2, 4 + far),
        ],
        compiler_params=pltpu.CompilerParams(
            collective_id=1, has_side_effects=True, vmem_limit_bytes=67043328
        ),
    )(wq, wk, wv, wo, wup, wdown, x, dy, seg, vecs)


def per_device(
    n_t, n_b,
    hidden_in, segment_ids, query_weight, query_bias, key_weight, value_weight, value_bias,
    out_weight, out_bias, attn_gain, attn_shift, up_weight, up_bias, down_weight, down_bias,
    ffn_gain, ffn_shift, cotangent,
):
    inner, width = out_weight.shape
    spare = jnp.zeros((width - 2 * inner,), F32)
    vecs = jnp.concatenate(
        [
            out_bias, attn_gain, attn_shift, down_bias, ffn_gain, ffn_shift, up_bias,
            query_bias, value_bias, spare,
        ]
    ).reshape(8, width)
    final, pooled, dx, fout, vout = run_layer(
        query_weight.T, key_weight.T, value_weight.T, out_weight, up_weight, down_weight,
        hidden_in[0], cotangent[0], segment_ids, vecs, n_t,
    )
    if n_b > PLANE:
        apart = [[i + PLANE * j for j in range(n_b // PLANE)] for i in range(PLANE)]
        fout, vout = lax.psum((fout.astype(F32), vout), "batch", axis_index_groups=apart)
    own = fout[2].astype(F32)
    return (
        final[None],
        pooled[None],
        dx[None],
        own[:inner].T,
        vout[6, :inner],
        own[inner : 2 * inner].T,
        own[2 * inner : 3 * inner].T,
        vout[7, :inner],
        own[3 * inner :],
        vout[0, :inner],
        vout[1, :inner],
        vout[2, :inner],
        fout[1].astype(F32),
        vout[8],
        fout[0].astype(F32),
        vout[3, :inner],
        vout[4, :inner],
        vout[5, :inner],
    )


def solution(mesh):
    rows, tens = P(("batch", "tensor"), None, None), P("tensor")
    col, row = P(None, "tensor"), P("tensor", None)
    in_specs = (
        rows, P("batch", None), col, tens, col, col, tens, row, P(), P(), P(), col, tens, row,
        P(), P(), P(), rows,
    )
    out_specs = (
        rows, rows, rows, col, tens, col, col, tens, row, tens, tens, tens, col, tens, row, tens,
        tens, tens,
    )
    body = functools.partial(per_device, mesh.shape["tensor"], mesh.shape["batch"])
    return jax.shard_map(
        body, mesh=mesh, in_specs=in_specs, out_specs=out_specs, check_vma=False
    )
```

```python
import functools
import math

import jax
import jax.numpy as jnp
from jax import lax
from jax.experimental import pallas as pl
from jax.experimental.pallas import tpu as pltpu
from jax.sharding import PartitionSpec as P

HEAD_DIM = 64
TEXTS = 8
TEXT_MOST = 128
PLANE = 8
CHIPS = 4
LANES = 128
TILE = 256
MESH = pl.DeviceIdType.MESH
F32 = jnp.float32
BF16 = jnp.bfloat16
QKVO, UP, DOWN = 0, 1, 2
ERFC_STEP = 0.43
ERFC_POLY = (
    0.24251981500369507,
    0.24429385145717694,
    0.2054723295686731,
    0.24508130662046312,
    -0.0823056340674522,
    0.3798888788682746,
    -0.3080966384375393,
    0.07314607841870144,
)


class Place:
    def __init__(self, n_t):
        bi = lax.axis_index("batch")
        self.t = lax.axis_index("tensor")
        self.n_t = n_t
        self.r = lax.rem(bi, PLANE)
        self.base = bi - self.r
        self.c = lax.rem(self.r, 2)
        self.q = self.r // 2
        self.x = lax.rem(self.q, 2)
        self.y = self.q // 2

    def z(self, step):
        return {"batch": self.base + self.r, "tensor": lax.rem(self.t + step, self.n_t)}

    def line(self, way):
        step = 1 if way == 0 else self.n_t - 1
        return {"batch": self.base + self.r, "tensor": lax.rem(self.t + step, self.n_t)}

    def other(self, axis):
        y = self.y if axis == 0 else 1 - self.y
        x = self.x if axis == 1 else 1 - self.x
        return y * 2 + x

    def chip(self, axis):
        return {"batch": self.base + self.other(axis) * 2 + self.c, "tensor": self.t}

    def sibling(self):
        return {"batch": self.base + self.q * 2 + 1 - self.c, "tensor": self.t}

    def greet(self):
        barrier = pltpu.get_barrier_semaphore()
        peers = [self.z(s) for s in range(1, self.n_t)]
        peers += [self.chip(j) for j in range(3)] + [self.sibling()]
        for peer in peers:
            pl.semaphore_signal(barrier, inc=1, device_id=peer, device_id_type=MESH)
        return lambda: pl.semaphore_wait(barrier, len(peers))


def remote(src, dst, send, recv, dev):
    return pltpu.make_async_remote_copy(
        src_ref=src, dst_ref=dst, send_sem=send, recv_sem=recv, device_id=dev, device_id_type=MESH
    )


def span(start, size):
    return pl.ds(start if isinstance(start, int) else pl.multiple_of(start, size), size)


def rows_at(start, size):
    return pl.ds(pl.multiple_of(start, 16), size)


def nn(left, right):
    return jnp.dot(left, right, preferred_element_type=F32)


def nt(left, right):
    return lax.dot_general(left, right, (((1,), (1,)), ((), ())), preferred_element_type=F32)


def tn(left, right):
    return lax.dot_general(left, right, (((0,), (0,)), ((), ())), preferred_element_type=F32)


def gelu_both(x):
    t = 1.0 / (1.0 + (ERFC_STEP * math.sqrt(0.5)) * jnp.abs(x))
    poly = jnp.full_like(x, ERFC_POLY[-1])
    for c in ERFC_POLY[-2::-1]:
        poly = poly * t + c
    bell = jnp.exp(x * x * -0.5)
    tail = 0.5 * (poly * t) * bell
    cdf = jnp.where(x > 0, 1.0 - tail, tail)
    return x * cdf, cdf + x * (bell * (1.0 / math.sqrt(2.0 * math.pi)))


def layer_kernel(
    n_t,
    wq, wk, wv, wo, wup, wdown, x, dy, seg, vecs,
    layer_out, pooled, acc, fout, vout,
    w, g, a, b, d, qkv, ctx, dctx, prob, act, dg, h1, dlow, work, tr, dsc, n1, near, bloc, bias,
    memb, rstd, sums, vsum, va, vb, vd,
    ls, zs, zr, xs, xr, rs, rr, ss, sr, cs, cr,
    r1s, r1r, r2s, r2r, r3s, r3r, r4s, r4r, r5s, r5r, r6s, r6r, vs, vr,
):
    me = Place(n_t)
    length, width = x.shape
    rows = w.shape[2]
    heads = 3
    ch, half = rows // PLANE, rows // 2
    mine = span((me.c * CHIPS + me.q) * ch, ch)
    my_half = span(me.c * half, half)
    blocks = length // LANES
    far = n_t - 1

    order = [sorted((abs(i - j), j) for j in range(n_t) if j != i) for i in range(n_t)]

    def pick(index, values):
        out = values[-1]
        for i in range(len(values) - 2, -1, -1):
            out = jnp.where(index == i, values[i], out)
        return out

    near_first = [pick(me.t, [jnp.int32(row[e][1]) for row in order]) for e in range(far)]

    def came(s):
        return near_first[s] if isinstance(s, int) else pick(s, near_first)

    def goes(s):
        return lax.rem(me.t + 1 + s, n_t)

    inner = rows // 4

    def local(k):
        if k > 0:
            return [pltpu.make_async_copy((wup, wdown)[k - 1], w.at[k, me.t], ls.at[3 + k])]
        return [
            pltpu.make_async_copy(src, w.at[0, me.t, pl.ds(n * inner, inner)], ls.at[n])
            for n, src in enumerate((wq, wk, wv, wo))
        ]

    def chunk(q, lo=0, hi=None):
        hi = ch if hi is None else hi
        return rows_at(me.c * half + q * ch + lo, hi - lo)

    def zown(way):
        place = w.at[QKVO, me.t, mine]
        return remote(
            place, place, zs.at[QKVO, far + way], zr.at[QKVO, me.t], me.line(way)
        )

    def zfar(k, s):
        place = w.at[k, me.t, mine]
        return remote(place, place, zs.at[k, s], zr.at[k, me.t], me.z(s + 1))

    def zrecv(k, s):
        place = w.at[k, came(s), mine]
        return remote(place, place, zs.at[k, s], zr.at[k, came(s)], me.line(0))

    def zpass(s, act_on):
        src = came(s)
        place = w.at[QKVO, src, mine]
        for way in range(2):
            goes_on = (src < me.t) & (me.t < far) if way == 0 else (src > me.t) & (me.t > 0)

            @pl.when(goes_on)
            def _():
                act_on(remote(place, place, zs.at[QKVO, s], zr.at[QKVO, src], me.line(way)))

    def zends(act_on):
        for way, there in ((0, me.t < far), (1, me.t > 0)):

            @pl.when(there)
            def _():
                act_on(zown(way))

    def zstart(k):
        for s in (0, far - 1, *range(1, far - 1)):
            zfar(k, s).start()

    def xcopy(k, s, j):
        place = w.at[k, came(s), chunk(me.q)]
        return remote(place, place, xs.at[k, s, j], xr.at[k, s, j], me.chip(j))

    def relay(k, s, j):
        part = (0, ch // 2) if j == 0 else (ch // 2, None)
        place = w.at[k, came(s), chunk(me.other(j), *part)]
        return remote(place, place, rs.at[k, s, j], rr.at[k, s, j], me.chip(1 - j))

    def relayed(k, s, j):
        part = (0, ch // 2) if j == 0 else (ch // 2, None)
        place = w.at[k, came(s), chunk(me.other(2), *part)]
        return remote(place, place, rs.at[k, s, j], rr.at[k, s, j], me.chip(1 - j))

    def scopy(k, s):
        place = w.at[k, came(s), my_half]
        return remote(place, place, ss.at[k, s], sr.at[k, s], me.sibling())

    def bcopy(s):
        return remote(bloc, near.at[me.t], cs.at[s], cr.at[s], me.z(s + 1))

    def on_z(k, s):
        zrecv(k, s).wait_recv()
        if k == QKVO:
            zpass(s, lambda c: c.start())
        for j in range(2):
            xcopy(k, s, j).start()

    def on_xy(k, s):
        for j in range(2):
            xcopy(k, s, j).wait_recv()
            relay(k, s, j).start()

    def on_relay(k, s):
        for j in range(2):
            relayed(k, s, j).wait_recv()
        scopy(k, s).start()

    def slot(k):
        return 1 if k == 1 else 0

    def inbox(k):
        return act if k == 2 else a.at[k]

    def r1(k, s):
        return remote(
            g.at[slot(k), s, span((1 - me.c) * half, half)],
            inbox(k).at[s, span(0, half)], r1s.at[k, s], r1r.at[k, s], me.sibling(),
        )

    def quarter(q):
        return span(me.c * half + q * ch, ch)

    cut = ch // 2

    def sub(q, h):
        return span(me.c * half + q * ch + h * cut, cut)

    def r2(k, s, h, j):
        source = (me.other(h), me.other(2), me.other(1 - h))[j]
        return remote(
            g.at[slot(k), s, sub(source, h)], b.at[k, s, j, span(h * cut, cut)],
            r2s.at[k, s, h, j], r2r.at[k, s, h, j], me.chip(1 - h if j == 2 else h),
        )

    def r3(k, s):
        return remote(b.at[k, s, 0], d.at[k, s], r3s.at[k, s], r3r.at[k, s], me.z(s + 1))

    def r4(k, j):
        place = fout.at[k, mine]
        return remote(place, place, r4s.at[k, j], r4r.at[k, j], me.chip(j))

    def r4b(k, j, q):
        place = fout.at[k, span((me.c * CHIPS + q) * ch + j * (ch // 2), ch // 2)]
        return remote(place, place, r6s.at[k, j], r6r.at[k, j], me.chip(1 - j))

    def r5(k):
        place = fout.at[k, my_half]
        return remote(place, place, r5s.at[k], r5r.at[k], me.sibling())

    def on_r1(k, s):
        r1(k, s).wait_recv()

        @pl.loop(0, CHIPS)
        def _(m):
            src = span(me.c * half + m * ch, ch)
            g[slot(k), s, src] += inbox(k)[s, span(m * ch, ch)]

        for h in range(2):
            for j in range(2):
                r2(k, s, h, j).start()

    def on_r2(k, s):
        for h in range(2):
            rows_h = span(h * cut, cut)
            r2(k, s, h, 1).wait_recv()
            g[slot(k), s, sub(me.other(1 - h), h)] += b[k, s, 1, rows_h]
            r2(k, s, h, 2).start()
            r2(k, s, h, 0).wait_recv()
            g[slot(k), s, sub(me.q, h)] += b[k, s, 0, rows_h]

    def on_r2b(k, s, last):
        for h in range(2):
            r2(k, s, h, 2).wait_recv()
        b[k, s, 0] = g[slot(k), s, quarter(me.q)] + b[k, s, 2]
        if last is None:

            @pl.when(s < far)
            def _():
                r3(k, s).start()

        elif not last:
            r3(k, s).start()

    def on_r3(k):
        total = b[k, far, 0].astype(F32)
        for s in range(far):
            r3(k, s).wait_recv()
            total = total + d[k, s].astype(F32)
        for s in range(far):
            r3(k, s).wait_send()
        fout[k, mine] = total.astype(BF16)
        for j in range(2):
            r4(k, j).start()

    def on_r4(k):
        for j in range(2):
            r4(k, j).wait_recv()
            r4b(k, j, me.other(j)).start()

    def on_r4b(k):
        for j in range(2):
            r4b(k, j, me.other(2)).wait_recv()
        r5(k).start()

    def pair_sum(n):
        return remote(vsum.at[n], va.at[n], vs.at[n, 0], vr.at[n, 0], me.sibling())

    def plane_sum(n, j):
        return remote(vsum.at[n], vb.at[n, j], vs.at[n, 1 + j], vr.at[n, 1 + j], me.chip(j))

    def line_sum(n, s):
        return remote(va.at[n], vd.at[n, s], vs.at[n, 4 + s], vr.at[n, 4 + s], me.z(s + 1))

    def on_pair(n):
        pair_sum(n).wait()
        vsum[n] += va[n]
        for j in range(3):
            plane_sum(n, j).start()

    def on_plane(n):
        for j in range(3):
            plane_sum(n, j).wait()
        va[n] = vsum[n] + vb[n, 0] + vb[n, 1] + vb[n, 2]
        for s in range(far):
            line_sum(n, s).start()

    def on_line(n):
        for s in range(far):
            line_sum(n, s).wait()
        total = va[n]
        for s in range(far):
            total = total + vd[n, s]
        return total

    low_lanes = lax.broadcasted_iota(jnp.int32, (1, LANES), 1) < HEAD_DIM
    low = jnp.where(low_lanes, 1.0, 0.0).astype(BF16)
    high = jnp.where(low_lanes, 0.0, 1.0).astype(BF16)
    low32 = jnp.where(low_lanes, 1.0, 0.0)
    high32 = jnp.where(low_lanes, 0.0, 1.0)

    def band(i):
        lo = max(0, i * LANES - TEXT_MOST)
        return lo, min(length, (i + 1) * LANES + TEXT_MOST)

    q01, k01, v01, o01 = (0, 128), (192, 320), (384, 512), (576, 704)
    q2, k2, v2, o2 = (128, 192), (320, 384), (512, 576), (704, 768)

    def picked(tt, spans, cols=slice(None)):
        return jnp.concatenate([w[QKVO, tt, lo:hi, cols] for lo, hi in spans], axis=0)

    def project(tt):
        @pl.loop(0, length // TILE)
        def _(m):
            r = span(m * TILE, TILE)
            xm = x[r, :]
            for lo, hi, spans in (
                (0, 256, (q01, k01)), (256, 512, (v01, q2, v2)), (512, 640, (k2, o2)),
            ):
                piece = nt(xm, picked(tt, spans))
                qkv[tt, r, lo:hi] = (
                    (piece + near[tt, 1:2, lo:hi]) * scales[:, lo:hi]
                ).astype(BF16)

    def attend(tt, some=None):
        for i in some or range(blocks):
            lo, hi = band(i)
            r = slice(i * LANES, (i + 1) * LANES)
            heads_in = (
                (qkv[tt, r, 0:128] * low, 128, 256),
                (qkv[tt, r, 0:128] * high, 128, 256),
                (qkv[tt, r, 384:512] * low, 512, 384),
            )
            sc = [
                nt(q, qkv[tt, lo:hi, kc : kc + LANES]) + bias[r, 0 : hi - lo]
                for q, kc, _ in heads_in
            ]
            ex = [jnp.exp(z - jnp.max(z, axis=-1, keepdims=True)) for z in sc]
            ps = [(e * (1.0 / jnp.sum(e, axis=-1, keepdims=True))).astype(BF16) for e in ex]
            for h, p in enumerate(ps):
                prob[tt, h, r, 0 : hi - lo] = p
            outs = [
                nn(p, qkv[tt, lo:hi, vc : vc + LANES]) for p, (_, _, vc) in zip(ps, heads_in)
            ]
            ctx[tt, r, 0:128] = (outs[2] * high32).astype(BF16)
            ctx[tt, r, 128:256] = (outs[0] * low32 + outs[1] * high32).astype(BF16)

    def attend_back(tt):
        for group in range(2):
            if group == 0:
                qc, kc, vc, dc = 0, 128, 256, 128
                hs = ((0, low, low, low32), (1, high, high, high32))
            else:
                qc, kc, vc, dc = 384, 512, 384, 0
                hs = ((2, low, high, low32),)
            dq = [None] * blocks
            for i in range(blocks):
                lo, hi = band(i)
                r = slice(i * LANES, (i + 1) * LANES)
                for n, (h, qm, vm, out_mask) in enumerate(hs):
                    dp = nt(dctx[r, dc : dc + LANES] * vm, qkv[tt, lo:hi, vc : vc + LANES])
                    p = prob[tt, h, r, 0 : hi - lo].astype(F32)
                    pd = p * dp
                    ds = (pd - p * jnp.sum(pd, axis=-1, keepdims=True)).astype(BF16)
                    dsc[n, r, 0 : hi - lo] = ds
                    part = nn(ds, qkv[tt, lo:hi, kc : kc + LANES]) * (
                        out_mask * (1.0 / math.sqrt(HEAD_DIM))
                    )
                    dq[i] = part if dq[i] is None else dq[i] + part
                if group == 0:
                    work[r, 0:128] = dq[i].astype(BF16)
            for j in range(blocks):
                rj = slice(j * LANES, (j + 1) * LANES)
                dk = dv = None
                for i in range(blocks):
                    lo, hi = band(i)
                    if not lo <= j * LANES < hi:
                        continue
                    r = slice(i * LANES, (i + 1) * LANES)
                    at = slice(j * LANES - lo, (j + 1) * LANES - lo)
                    for n, (h, qm, vm, _) in enumerate(hs):
                        more = tn(dsc[n, r, at], qkv[tt, r, qc : qc + LANES] * qm)
                        dk = more if dk is None else dk + more
                        more = tn(prob[tt, h, r, at], dctx[r, dc : dc + LANES] * vm)
                        dv = more if dv is None else dv + more
                if group == 0:
                    work[rj, 128:256] = dk.astype(BF16)
                    work[rj, 256:384] = dv.astype(BF16)
                else:
                    work[rj, 384:512] = (dq[j] + dv).astype(BF16)
                    work[rj, 512:640] = dk.astype(BF16)

    def add_sum(k, tile):
        n = tile.shape[0] // 8
        sums[k] += jnp.sum(tile.reshape(n, 8, tile.shape[1]), axis=0)

    def by_tiles(body):
        @pl.loop(0, length // 64)
        def _(m):
            body(span(m * 64, 64))

    def transpose_to(src):
        @pl.loop(0, rows // TILE)
        def _(m):
            cols = span(m * TILE, TILE)
            tr[cols, :] = src[:, cols].T

    for k in range(3):
        for copy in local(k):
            copy.start()
    dy_in = pltpu.make_async_copy(dy, work, ls.at[6])
    dy_in.start()
    all_here = me.greet()
    own = vecs[7:8, :]
    mid, end = own[:, 128:256], own[:, 256:384]
    turned = jnp.where(low_lanes, pltpu.roll(mid, HEAD_DIM, 1), pltpu.roll(end, HEAD_DIM, 1))
    bloc[...] = jnp.zeros_like(bloc)
    bloc[0:1, :] = vecs[6:7, :]
    bloc[1:2, 0:128] = own[:, 0:128]
    bloc[1:2, 256:384] = turned
    bloc[1:2, 384:512] = jnp.where(low_lanes, mid, end)
    near[me.t] = bloc[...]
    lane = lax.broadcasted_iota(jnp.int32, (1, 640), 1)
    is_query = (lane < 128) | ((lane >= 384) & (lane < 448))
    scales = jnp.where(is_query, 1.0 / math.sqrt(HEAD_DIM), 1.0)
    sums[...] = jnp.zeros_like(sums)
    labels = lax.broadcasted_iota(jnp.int32, (TEXTS, length), 0)
    memb[...] = jnp.where(seg[pl.ds(me.t, 1), :] == labels, 1.0, 0.0)
    for i in range(blocks):
        lo, hi = band(i)
        r = slice(i * LANES, (i + 1) * LANES)
        bias[r, 0 : hi - lo] = (tn(memb[:, r], memb[:, lo:hi]) - 1.0) * 1000000000.0
    for copy in local(QKVO):
        copy.wait()
    all_here()
    zends(lambda c: c.start())
    for s in range(far):
        bcopy(s).start()
    for k in (UP, DOWN):
        for copy in local(k):
            copy.wait()
    project(me.t)
    on_z(QKVO, 0)
    on_z(QKVO, 1)
    attend(me.t, (0, 1))
    on_z(QKVO, 2)
    zstart(UP)
    attend(me.t, (2, 3))
    on_xy(QKVO, 0)
    for s in range(far):
        bcopy(s).wait_recv()
    on_xy(QKVO, 1)
    on_relay(QKVO, 0)
    on_xy(QKVO, 2)

    @pl.loop(0, far)
    def _(s):
        tt = came(s)
        scopy(QKVO, s).wait_recv()
        project(tt)

        @pl.when(s < far - 1)
        def _():
            on_relay(QKVO, s + 1)

        attend(tt)
        on_z(UP, s)

        @pl.when(s == 1)
        def _():
            zstart(DOWN)

        @pl.when(s > 0)
        def _():
            on_xy(UP, s - 1)

    @pl.loop(0, length // TILE)
    def _(m):
        r = span(m * TILE, TILE)
        for n in range(width // TILE):
            c = slice(n * TILE, (n + 1) * TILE)
            out = x[r, c].astype(F32) + vecs[0:1, c]
            for t in range(n_t):
                out = out + nn(ctx[t, r, :], picked(t, (k2, o2, o01), c))
            acc[r, c] = out

    on_relay(UP, 0)

    @by_tiles
    def _(r):
        center = acc[r, :]
        center = center - jnp.mean(center, axis=-1, keepdims=True)
        inv = lax.rsqrt(jnp.mean(center * center, axis=-1, keepdims=True) + 1e-12)
        rstd[r, :] = inv
        center = center * inv
        n1[r, :] = center
        h1[r, :] = (center * vecs[1:2, :] + vecs[2:3, :]).astype(BF16)

    def rise(tt):
        @pl.loop(0, length // TILE)
        def _(m):
            r = span(m * TILE, TILE)
            hm = h1[r, :]
            for n in range(rows // TILE):
                c = slice(n * TILE, (n + 1) * TILE)
                up, slope = gelu_both(nn(hm, w[UP, tt, :, c]) + near[tt, 0:1, c])
                act[tt, r, c] = up.astype(BF16)
                dg[tt, r, c] = slope.astype(BF16)

    def fall(tt, first):
        @pl.loop(0, length // TILE)
        def _(m):
            r = span(m * TILE, TILE)
            am = act[tt, r, :]
            for n in range(width // TILE):
                c = slice(n * TILE, (n + 1) * TILE)
                out = nn(am, w[DOWN, tt, :, c])
                acc[r, c] = out if first else acc[r, c] + out

    on_z(DOWN, 0)
    rise(me.t)
    on_xy(UP, 2)
    on_relay(UP, 1)
    on_z(DOWN, 1)

    @pl.loop(0, far)
    def _(s):
        scopy(UP, s).wait_recv()
        rise(came(s))

        @pl.when(s == 0)
        def _():
            on_relay(UP, far - 1)
            on_z(DOWN, far - 1)

        on_xy(DOWN, s)

    on_relay(DOWN, 0)
    fall(me.t, True)

    @pl.loop(0, far)
    def _(s):
        @pl.when(s < far - 1)
        def _():
            on_relay(DOWN, s + 1)

        scopy(DOWN, s).wait_recv()
        fall(came(s), False)

    dy_in.wait()

    @by_tiles
    def _(r):
        dyt = work[r, :].astype(F32)
        center = acc[r, :] + vecs[3:4, :] + (n1[r, :] * vecs[1:2, :] + vecs[2:3, :])
        center = center - jnp.mean(center, axis=-1, keepdims=True)
        inv = lax.rsqrt(jnp.mean(center * center, axis=-1, keepdims=True) + 1e-12)
        n2 = center * inv
        final = n2 * vecs[4:5, :] + vecs[5:6, :]
        out = final.astype(BF16)
        dn = dyt * vecs[4:5, :]
        dr = inv * (
            dn
            - jnp.mean(dn, axis=-1, keepdims=True)
            - n2 * jnp.mean(dn * n2, axis=-1, keepdims=True)
        )
        layer_out[r, :] = out
        g[1, 1, r, :] = (final - out.astype(F32)).astype(BF16)
        acc[r, :] = dr
        dlow[r, :] = dr.astype(BF16)
        add_sum(0, dr)
        add_sum(1, dyt * n2)
        add_sum(2, dyt)

    counts = jnp.sum(memb[...], axis=-1, keepdims=True)
    member = memb[...].astype(BF16)
    pooled[...] = (nn(member, layer_out[...]) + nn(member, g[1, 1, 0:length, :])) / counts

    ones = jnp.ones((8, length), BF16)

    def grad_to(k, s, left_t, right):
        @pl.loop(0, rows // TILE)
        def _(m):
            r = span(m * TILE, TILE)
            lt = left_t(r)
            for n in range(width // TILE):
                c = slice(n * TILE, (n + 1) * TILE)
                g[k, s, r, c] = nn(lt, right[:, c]).astype(BF16)

    @pl.loop(0, n_t)
    def _(s):
        tt = goes(s)
        grad_to(0, s, lambda r: act[tt, :, r].T, dlow)
        r1(0, s).start()

        @pl.when(s > 0)
        def _():
            on_r1(0, s - 1)

    transpose_to(h1)
    on_r1(0, far)

    @pl.loop(0, n_t)
    def _(s):
        tt = goes(s)

        @pl.loop(0, length // TILE)
        def _(m):
            r = span(m * TILE, TILE)
            dm = dlow[r, :]
            for n in range(rows // TILE):
                c = slice(n * TILE, (n + 1) * TILE)
                work[r, c] = (nt(dm, w[DOWN, tt, c, :]) * dg[tt, r, c].astype(F32)).astype(BF16)

        @pl.when(s > 0)
        def _():
            on_r1(1, s - 1)

        grad_to(1, s, lambda r: tr[r, :], work)
        r1(1, s).start()

        @pl.loop(0, length // TILE)
        def _(m):
            r = span(m * TILE, TILE)
            dm = work[r, :]
            for n in range(width // TILE):
                c = slice(n * TILE, (n + 1) * TILE)
                acc[r, c] += nt(dm, w[UP, tt, c, :])

        vsum[1, pl.ds(tt, 1), :] = nn(ones, work[...])[0:1, :]
        on_r2(0, s)

    on_r1(1, far)

    @by_tiles
    def _(r):
        dh, nt1 = acc[r, :], n1[r, :]
        dn = dh * vecs[1:2, :]
        dr = rstd[r, :] * (
            dn
            - jnp.mean(dn, axis=-1, keepdims=True)
            - nt1 * jnp.mean(dn * nt1, axis=-1, keepdims=True)
        )
        acc[r, :] = dr
        dlow[r, :] = dr.astype(BF16)
        add_sum(3, dr)
        add_sum(4, dh * nt1)
        add_sum(5, dh)

    on_r2b(0, 0, False)
    on_r2b(0, 1, False)
    vsum[0] = jnp.zeros((8, width), F32)
    for k, row in ((3, 0), (4, 1), (5, 2), (0, 3), (1, 4), (2, 5)):
        vsum[0, row : row + 1, :] = jnp.sum(sums[k], axis=0, keepdims=True)
    pair_sum(0).start()
    work[:, 640:768] = jnp.zeros((length, LANES), BF16)

    @pl.loop(0, n_t)
    def _(s):
        tt = goes(s)

        @pl.loop(0, length // TILE)
        def _(m):
            r = span(m * TILE, TILE)
            out = nt(dlow[r, :], picked(tt, (k2, o2, o01)))
            dctx[r, 0:128] = (out[:, 0:128] * high32).astype(BF16)
            dctx[r, 128:256] = out[:, 128:256].astype(BF16)

        attend_back(tt)

        @pl.when(s == 0)
        def _():
            on_pair(0)
            on_r2b(0, 2, False)
            on_r2(1, 0)
            on_r2(1, 1)

        @pl.when(s == 1)
        def _():
            on_r2b(0, 3, True)
            on_r2(1, 2)
            on_r2(1, 3)

        @pl.when(s == 2)
        def _():
            on_r3(0)
            on_plane(0)
            on_r2b(1, 0, False)

        @pl.when(s == 3)
        def _():
            on_r2b(1, 1, False)
            on_r2b(1, 2, False)

        r1(0, s).wait_send()
        for h in range(2):
            for j in range(3):
                r2(0, s, h, j).wait_send()

        for m in range(rows // TILE):
            r = slice(m * TILE, (m + 1) * TILE)
            lt = work[:, r].T
            ct = ctx[tt].T if r.start == 512 else None
            for n in range(width // TILE):
                c = slice(n * TILE, (n + 1) * TILE)
                out = nn(lt, x[:, c])
                if ct is not None:
                    out = out + nn(ct, dlow[:, c])
                out = out.astype(BF16)
                at = 0
                for lo, hi in ((q01, k01), (v01, q2, v2), (k2, o2, o01))[m]:
                    g[0, s, lo:hi, c] = out[at : at + hi - lo, :]
                    at += hi - lo

        r1(2, s).start()

        @pl.loop(0, length // TILE)
        def _(m):
            r = span(m * TILE, TILE)
            dm = work[r, 0:640]
            for n in range(width // TILE):
                c = slice(n * TILE, (n + 1) * TILE)
                acc[r, c] += nn(dm, picked(tt, (q01, k01, v01, q2, v2, k2, o2), c))

        vsum[1, pl.ds(4 + tt, 1), :] = nn(ones, work[...])[0:1, :]

        @pl.when(s > 0)
        def _():
            on_r1(2, s - 1)

    pair_sum(1).start()
    on_r1(2, far)
    on_r2b(1, far, True)
    on_pair(1)
    on_r4(0)
    on_r2(2, 0)
    on_r4b(0)
    on_r2(2, 1)
    on_r2(2, 2)
    on_plane(1)
    on_r2b(2, 0, False)
    on_r2(2, far)
    on_r3(1)
    turns = lax.rem(width - me.t * (width // n_t), width)
    vout[0:8, :] = pltpu.roll(on_line(0), turns, 1)
    vout[8:16, :] = jnp.zeros((8, width), F32)
    on_r2b(2, 1, False)
    on_r2b(2, 2, False)
    vsum[1] = on_line(1)
    mine_row = vsum[1, pl.ds(4 + me.t, 1), :]
    vout[6:7, 0:128] = mine_row[:, 0:128]
    vout[6:7, 128:256] = mine_row[:, 384:512]
    vout[7:8, 0:128] = mine_row[:, 256:384]
    vout[7:8, 128:256] = pltpu.roll(mine_row[:, 384:512], HEAD_DIM, 1)
    vout[8:9, :] = vsum[1, pl.ds(me.t, 1), :]
    on_r2b(2, far, True)
    on_r3(2)
    on_r4(1)
    on_r4(2)
    on_r4b(1)
    on_r4b(2)
    for k in range(3):
        r5(k).wait_recv()

    for s in range(far):
        bcopy(s).wait_send()
    for k in range(3):
        if k == QKVO:
            zends(lambda c: c.wait_send())
        for s in range(far):
            if k == QKVO:
                zpass(s, lambda c: c.wait_send())
            else:
                zfar(k, s).wait_send()
            scopy(k, s).wait_send()
            for j in range(2):
                xcopy(k, s, j).wait_send()
                relay(k, s, j).wait_send()
        for s in range(n_t):
            if k > 0:
                r1(k, s).wait_send()
                for h in range(2):
                    for j in range(3):
                        r2(k, s, h, j).wait_send()
        for j in range(2):
            r4(k, j).wait_send()
            r4b(k, j, me.other(j)).wait_send()
        r5(k).wait_send()


def run_layer(wq, wk, wv, wo, wup, wdown, x, dy, seg, vecs, n_t):
    groups, (rows, cols) = 3, wup.shape
    length, width = x.shape
    ch, half, far = rows // PLANE, rows // 2, n_t - 1
    dma, vmem = pltpu.SemaphoreType.DMA, pltpu.VMEM
    here, there = pl.BlockSpec(memory_space=vmem), pl.BlockSpec(memory_space=pl.ANY)
    shape = jax.ShapeDtypeStruct
    pair = lambda *dims: [dma(dims), dma(dims)]
    return pl.pallas_call(
        functools.partial(layer_kernel, n_t),
        out_shape=(
            shape((length, width), BF16),
            shape((TEXTS, width), F32),
            shape((length, width), F32),
            shape((groups, rows, cols), BF16),
            shape((16, width), F32),
        ),
        in_specs=[there] * 6 + [here, there, here, here],
        out_specs=[here] * 5,
        scratch_shapes=[
            vmem((groups, n_t, rows, cols), BF16),
            vmem((2, n_t, rows, cols), BF16),
            vmem((2, n_t, half, cols), BF16),
            vmem((groups, n_t, 3, ch, cols), BF16),
            vmem((groups, far, ch, cols), BF16),
            vmem((n_t, length, 640), BF16),
            vmem((n_t, length, 256), BF16),
            vmem((length, 256), BF16),
            vmem((n_t, 3, length, 384), BF16),
            vmem((n_t, length, rows), BF16),
            vmem((n_t, length, rows), BF16),
            vmem((length, width), BF16),
            vmem((length, width), BF16),
            vmem((length, width), BF16),
            vmem((width, length), BF16),
            vmem((2, length, 384), BF16),
            vmem((length, width), F32),
            vmem((n_t, 8, width), F32),
            vmem((8, width), F32),
            vmem((length, 384), F32),
            vmem((TEXTS, length), F32),
            vmem((length, 1), F32),
            vmem((6, 8, width), F32),
            vmem((2, 8, width), F32),
            vmem((2, 8, width), F32),
            vmem((2, 3, 8, width), F32),
            vmem((2, far, 8, width), F32),
            dma((7,)),
            dma((groups, far + 2)),
            dma((groups, n_t)),
            *pair(groups, far, 2),
            *pair(groups, far, 2),
            *pair(groups, far),
            *pair(far),
            *pair(groups, n_t),
            *pair(groups, n_t, 2, 3),
            *pair(groups, far),
            *pair(groups, 2),
            *pair(groups),
            *pair(groups, 2),
            *pair(2, 4 + far),
        ],
        compiler_params=pltpu.CompilerParams(
            collective_id=1, has_side_effects=True, vmem_limit_bytes=67043328
        ),
    )(wq, wk, wv, wo, wup, wdown, x, dy, seg, vecs)


def per_device(
    n_t, n_b,
    hidden_in, segment_ids, query_weight, query_bias, key_weight, value_weight, value_bias,
    out_weight, out_bias, attn_gain, attn_shift, up_weight, up_bias, down_weight, down_bias,
    ffn_gain, ffn_shift, cotangent,
):
    inner, width = out_weight.shape
    spare = jnp.zeros((width - 2 * inner,), F32)
    vecs = jnp.concatenate(
        [
            out_bias, attn_gain, attn_shift, down_bias, ffn_gain, ffn_shift, up_bias,
            query_bias, value_bias, spare,
        ]
    ).reshape(8, width)
    final, pooled, dx, fout, vout = run_layer(
        query_weight.T, key_weight.T, value_weight.T, out_weight, up_weight, down_weight,
        hidden_in[0], cotangent[0], segment_ids, vecs, n_t,
    )
    if n_b > PLANE:
        apart = [[i + PLANE * j for j in range(n_b // PLANE)] for i in range(PLANE)]
        fout, vout = lax.psum((fout.astype(F32), vout), "batch", axis_index_groups=apart)
    own = fout[2].astype(F32)
    return (
        final[None],
        pooled[None],
        dx[None],
        own[:inner].T,
        vout[6, :inner],
        own[inner : 2 * inner].T,
        own[2 * inner : 3 * inner].T,
        vout[7, :inner],
        own[3 * inner :],
        vout[0, :inner],
        vout[1, :inner],
        vout[2, :inner],
        fout[1].astype(F32),
        vout[8],
        fout[0].astype(F32),
        vout[3, :inner],
        vout[4, :inner],
        vout[5, :inner],
    )


def solution(mesh):
    rows, tens = P(("batch", "tensor"), None, None), P("tensor")
    col, row = P(None, "tensor"), P("tensor", None)
    in_specs = (
        rows, P("batch", None), col, tens, col, col, tens, row, P(), P(), P(), col, tens, row,
        P(), P(), P(), rows,
    )
    out_specs = (
        rows, rows, rows, col, tens, col, col, tens, row, tens, tens, tens, col, tens, row, tens,
        tens, tens,
    )
    body = functools.partial(per_device, mesh.shape["tensor"], mesh.shape["batch"])
    return jax.shard_map(
        body, mesh=mesh, in_specs=in_specs, out_specs=out_specs, check_vma=False
    )
```

```python
import functools
import math

import jax
import jax.numpy as jnp
from jax import lax
from jax.experimental import pallas as pl
from jax.experimental.pallas import tpu as pltpu
from jax.sharding import PartitionSpec as P

HEAD_DIM = 64
TEXTS = 8
TEXT_MOST = 128
PLANE = 8
CHIPS = 4
LANES = 128
TILE = 256
MESH = pl.DeviceIdType.MESH
F32 = jnp.float32
BF16 = jnp.bfloat16
QKVO, UP, DOWN = 0, 1, 2
PARTS = ((0, 48), (48, 80))
PLANE_ROWS, Z_ROWS = 80, 16
ERFC_STEP = 0.43
ERFC_POLY = (
    0.24251981500369507,
    0.24429385145717694,
    0.2054723295686731,
    0.24508130662046312,
    -0.0823056340674522,
    0.3798888788682746,
    -0.3080966384375393,
    0.07314607841870144,
)


class Place:
    def __init__(self, n_t):
        bi = lax.axis_index("batch")
        self.t = lax.axis_index("tensor")
        self.n_t = n_t
        self.r = lax.rem(bi, PLANE)
        self.base = bi - self.r
        self.c = lax.rem(self.r, 2)
        self.q = self.r // 2
        self.x = lax.rem(self.q, 2)
        self.y = self.q // 2

    def z(self, step):
        return {"batch": self.base + self.r, "tensor": lax.rem(self.t + step, self.n_t)}

    def line(self, way):
        step = 1 if way == 0 else self.n_t - 1
        return {"batch": self.base + self.r, "tensor": lax.rem(self.t + step, self.n_t)}

    def other(self, axis):
        y = self.y if axis == 0 else 1 - self.y
        x = self.x if axis == 1 else 1 - self.x
        return y * 2 + x

    def chip(self, axis):
        return {"batch": self.base + self.other(axis) * 2 + self.c, "tensor": self.t}

    def sibling(self):
        return {"batch": self.base + self.q * 2 + 1 - self.c, "tensor": self.t}

    def greet(self):
        barrier = pltpu.get_barrier_semaphore()
        peers = [self.z(s) for s in range(1, self.n_t)]
        peers += [self.chip(j) for j in range(3)] + [self.sibling()]
        for peer in peers:
            pl.semaphore_signal(barrier, inc=1, device_id=peer, device_id_type=MESH)
        return lambda: pl.semaphore_wait(barrier, len(peers))


def remote(src, dst, send, recv, dev):
    return pltpu.make_async_remote_copy(
        src_ref=src, dst_ref=dst, send_sem=send, recv_sem=recv, device_id=dev, device_id_type=MESH
    )


def span(start, size):
    return pl.ds(start if isinstance(start, int) else pl.multiple_of(start, size), size)


def rows_at(start, size):
    return pl.ds(pl.multiple_of(start, 16), size)


def nn(left, right):
    return jnp.dot(left, right, preferred_element_type=F32)


def nt(left, right):
    return lax.dot_general(left, right, (((1,), (1,)), ((), ())), preferred_element_type=F32)


def tn(left, right):
    return lax.dot_general(left, right, (((0,), (0,)), ((), ())), preferred_element_type=F32)


def gelu_both(x):
    t = 1.0 / (1.0 + (ERFC_STEP * math.sqrt(0.5)) * jnp.abs(x))
    poly = jnp.full_like(x, ERFC_POLY[-1])
    for c in ERFC_POLY[-2::-1]:
        poly = poly * t + c
    bell = jnp.exp(x * x * -0.5)
    tail = 0.5 * (poly * t) * bell
    cdf = jnp.where(x > 0, 1.0 - tail, tail)
    return x * cdf, cdf + x * (bell * (1.0 / math.sqrt(2.0 * math.pi)))


def layer_kernel(
    n_t,
    wq, wk, wv, wo, wup, wdown, x, dy, seg, vecs,
    layer_out, pooled, acc, fout, vout,
    w, g, a, b, d, e, hz, bz, qkv, ctx, dctx, prob, act, dg, h1, dlow, work, tr, dsc, n1, near, bloc, bias,
    memb, rstd, sums, vsum, va, vb, vd,
    ls, zs, zr, xs, xr, rs, rr, ss, sr, cs, cr,
    r1s, r1r, r2s, r2r, r3s, r3r, r4s, r4r, r5s, r5r, r6s, r6r, rzs, rzr, zps, zpr, vs, vr,
):
    me = Place(n_t)
    length, width = x.shape
    rows = w.shape[2]
    heads = 3
    ch, half = rows // PLANE, rows // 2
    mine = span((me.c * CHIPS + me.q) * ch, ch)
    my_half = span(me.c * half, half)
    blocks = length // LANES
    far = n_t - 1

    order = [sorted((abs(i - j), j) for j in range(n_t) if j != i) for i in range(n_t)]

    def pick(index, values):
        out = values[-1]
        for i in range(len(values) - 2, -1, -1):
            out = jnp.where(index == i, values[i], out)
        return out

    near_first = [pick(me.t, [jnp.int32(row[e][1]) for row in order]) for e in range(far)]

    def came(s):
        return near_first[s] if isinstance(s, int) else pick(s, near_first)

    def goes(s):
        return lax.rem(me.t + 1 + s, n_t)

    inner = rows // 4

    def local(k):
        if k > 0:
            return [pltpu.make_async_copy((wup, wdown)[k - 1], w.at[k, me.t], ls.at[3 + k])]
        return [
            pltpu.make_async_copy(src, w.at[0, me.t, pl.ds(n * inner, inner)], ls.at[n])
            for n, src in enumerate((wq, wk, wv, wo))
        ]

    def chunk(q, lo=0, hi=None):
        hi = ch if hi is None else hi
        return rows_at(me.c * half + q * ch + lo, hi - lo)

    def zown(way):
        place = w.at[QKVO, me.t, mine]
        return remote(
            place, place, zs.at[QKVO, far + way], zr.at[QKVO, me.t], me.line(way)
        )

    def zfar(k, s):
        place = w.at[k, me.t, mine]
        return remote(place, place, zs.at[k, s], zr.at[k, me.t], me.z(s + 1))

    def zrecv(k, s):
        place = w.at[k, came(s), mine]
        return remote(place, place, zs.at[k, s], zr.at[k, came(s)], me.line(0))

    def zpass(s, act_on):
        src = came(s)
        place = w.at[QKVO, src, mine]
        for way in range(2):
            goes_on = (src < me.t) & (me.t < far) if way == 0 else (src > me.t) & (me.t > 0)

            @pl.when(goes_on)
            def _():
                act_on(remote(place, place, zs.at[QKVO, s], zr.at[QKVO, src], me.line(way)))

    def zends(act_on):
        for way, there in ((0, me.t < far), (1, me.t > 0)):

            @pl.when(there)
            def _():
                act_on(zown(way))

    def zstart(k):
        for s in (0, far - 1, *range(1, far - 1)):
            zfar(k, s).start()

    def xcopy(k, s, j):
        place = w.at[k, came(s), chunk(me.q)]
        return remote(place, place, xs.at[k, s, j], xr.at[k, s, j], me.chip(j))

    def relay(k, s, j):
        part = (0, ch // 2) if j == 0 else (ch // 2, None)
        place = w.at[k, came(s), chunk(me.other(j), *part)]
        return remote(place, place, rs.at[k, s, j], rr.at[k, s, j], me.chip(1 - j))

    def relayed(k, s, j):
        part = (0, ch // 2) if j == 0 else (ch // 2, None)
        place = w.at[k, came(s), chunk(me.other(2), *part)]
        return remote(place, place, rs.at[k, s, j], rr.at[k, s, j], me.chip(1 - j))

    def scopy(k, s):
        place = w.at[k, came(s), my_half]
        return remote(place, place, ss.at[k, s], sr.at[k, s], me.sibling())

    def bcopy(s):
        return remote(bloc, near.at[me.t], cs.at[s], cr.at[s], me.z(s + 1))

    def on_z(k, s):
        zrecv(k, s).wait_recv()
        if k == QKVO:
            zpass(s, lambda c: c.start())
        for j in range(2):
            xcopy(k, s, j).start()

    def on_xy(k, s):
        for j in range(2):
            xcopy(k, s, j).wait_recv()
            relay(k, s, j).start()

    def on_relay(k, s):
        for j in range(2):
            relayed(k, s, j).wait_recv()
        scopy(k, s).start()

    def slot(k):
        return 1 if k == 1 else 0

    def inbox(k):
        return act if k == 2 else a.at[k]

    def r1(k, s):
        return remote(
            g.at[slot(k), s, span((1 - me.c) * half, half)],
            inbox(k).at[s, span(0, half)], r1s.at[k, s], r1r.at[k, s], me.sibling(),
        )

    def quarter(q):
        return rows_at(me.c * half + q * PLANE_ROWS, PLANE_ROWS)

    def sub(q, h):
        lo, hi = PARTS[h]
        return rows_at(me.c * half + q * PLANE_ROWS + lo, hi - lo)

    def axis(k, h):
        return (h + k) % 2

    def r2(k, s, h, j):
        ax, (lo, hi) = axis(k, h), PARTS[h]
        source = (me.other(ax), me.other(2), me.other(1 - ax))[j]
        return remote(
            g.at[slot(k), s, sub(source, h)], b.at[k, s, j, pl.ds(lo, hi - lo)],
            r2s.at[k, s, h, j], r2r.at[k, s, h, j], me.chip(1 - ax if j == 2 else ax),
        )

    def r3(k, s):
        return remote(b.at[k, s, 0], d.at[k, s], r3s.at[k, s], r3r.at[k, s], me.z(s + 1))

    zfirst = rows_at(me.c * half + CHIPS * PLANE_ROWS, CHIPS * Z_ROWS)

    def rz(k, s):
        return remote(
            g.at[slot(k), s, zfirst], e.at[k, s], rzs.at[k, s], rzr.at[k, s], me.z(s + 1)
        )

    def piece(q):
        return rows_at(q * Z_ROWS, Z_ROWS)

    def r2z(k, j):
        ax = axis(k, 1)
        source = (me.other(ax), me.other(2), me.other(1 - ax))[j]
        return remote(
            hz.at[k, piece(source)], bz.at[k, j], zps.at[k, j], zpr.at[k, j],
            me.chip(1 - ax if j == 2 else ax),
        )

    def final_rows(q, i, lo=0, hi=PLANE_ROWS):
        if i == 0:
            return rows_at(me.c * half + q * PLANE_ROWS + lo, hi - lo)
        return rows_at(me.c * half + CHIPS * PLANE_ROWS + q * Z_ROWS, Z_ROWS)

    def r4(k, j, i):
        place = fout.at[k, final_rows(me.q, i)]
        return remote(place, place, r4s.at[k, j, i], r4r.at[k, j, i], me.chip(j))

    def r4b(k, j, q):
        place = fout.at[k, final_rows(q, 0, *PARTS[j])]
        return remote(place, place, r6s.at[k, j], r6r.at[k, j], me.chip(1 - j))

    def r4c(k, q):
        place = fout.at[k, final_rows(q, 1)]
        return remote(place, place, r6s.at[k, 2], r6r.at[k, 2], me.chip(1))

    def r5(k):
        place = fout.at[k, my_half]
        return remote(place, place, r5s.at[k], r5r.at[k], me.sibling())

    def on_r1(k, s):
        r1(k, s).wait_recv()

        @pl.loop(0, CHIPS)
        def _(m):
            src = span(me.c * half + m * ch, ch)
            g[slot(k), s, src] += inbox(k)[s, span(m * ch, ch)]

        for h in range(2):
            for j in range(2):
                r2(k, s, h, j).start()
        if not isinstance(s, int) or s < far:
            rz(k, s).start()

    def on_r2(k, s):
        for h, (lo, hi) in enumerate(PARTS):
            got = slice(lo, hi)
            r2(k, s, h, 1).wait_recv()
            g[slot(k), s, sub(me.other(1 - axis(k, h)), h)] += b[k, s, 1, got]
            r2(k, s, h, 2).start()
            r2(k, s, h, 0).wait_recv()
            g[slot(k), s, sub(me.q, h)] += b[k, s, 0, got]

    def on_r2b(k, s, last):
        for h in range(2):
            r2(k, s, h, 2).wait_recv()
        b[k, s, 0] = g[slot(k), s, quarter(me.q)] + b[k, s, 2]
        if not last:
            r3(k, s).start()

    def on_r3(k):
        total = b[k, far, 0].astype(F32)
        for s in range(far):
            r3(k, s).wait_recv()
            total = total + d[k, s].astype(F32)
        for s in range(far):
            r3(k, s).wait_send()
        fout[k, final_rows(me.q, 0)] = total.astype(BF16)
        for j in range(2):
            r4(k, j, 0).start()

    def on_rz(k):
        total = g[slot(k), far, zfirst].astype(F32)
        for s in range(far):
            rz(k, s).wait_recv()
            total = total + e[k, s].astype(F32)
        hz[k] = total.astype(BF16)
        for j in range(2):
            r2z(k, j).start()

    def on_r2z(k):
        r2z(k, 1).wait_recv()
        hz[k, piece(me.other(1 - axis(k, 1)))] += bz[k, 1]
        r2z(k, 2).start()
        r2z(k, 0).wait_recv()
        hz[k, piece(me.q)] += bz[k, 0]

    def on_r2zb(k):
        r2z(k, 2).wait_recv()
        fout[k, final_rows(me.q, 1)] = hz[k, piece(me.q)] + bz[k, 2]
        for j in range(2):
            r4(k, j, 1).start()

    def on_r4(k):
        for j in range(2):
            r4(k, j, 0).wait_recv()
            r4b(k, j, me.other(j)).start()
        for j in range(2):
            r4(k, j, 1).wait_recv()
        r4c(k, me.other(0)).start()

    def on_r4b(k):
        for j in range(2):
            r4b(k, j, me.other(2)).wait_recv()
        r4c(k, me.other(2)).wait_recv()
        r5(k).start()

    def pair_sum(n):
        return remote(vsum.at[n], va.at[n], vs.at[n, 0], vr.at[n, 0], me.sibling())

    def plane_sum(n, j):
        return remote(vsum.at[n], vb.at[n, j], vs.at[n, 1 + j], vr.at[n, 1 + j], me.chip(j))

    def line_sum(n, s):
        return remote(va.at[n], vd.at[n, s], vs.at[n, 4 + s], vr.at[n, 4 + s], me.z(s + 1))

    def on_pair(n):
        pair_sum(n).wait()
        vsum[n] += va[n]
        for j in range(3):
            plane_sum(n, j).start()

    def on_plane(n):
        for j in range(3):
            plane_sum(n, j).wait()
        va[n] = vsum[n] + vb[n, 0] + vb[n, 1] + vb[n, 2]
        for s in range(far):
            line_sum(n, s).start()

    def on_line(n):
        for s in range(far):
            line_sum(n, s).wait()
        total = va[n]
        for s in range(far):
            total = total + vd[n, s]
        return total

    low_lanes = lax.broadcasted_iota(jnp.int32, (1, LANES), 1) < HEAD_DIM
    low = jnp.where(low_lanes, 1.0, 0.0).astype(BF16)
    high = jnp.where(low_lanes, 0.0, 1.0).astype(BF16)
    low32 = jnp.where(low_lanes, 1.0, 0.0)
    high32 = jnp.where(low_lanes, 0.0, 1.0)

    def band(i):
        lo = max(0, i * LANES - TEXT_MOST)
        return lo, min(length, (i + 1) * LANES + TEXT_MOST)

    q01, k01, v01, o01 = (0, 128), (192, 320), (384, 512), (576, 704)
    q2, k2, v2, o2 = (128, 192), (320, 384), (512, 576), (704, 768)

    def picked(tt, spans, cols=slice(None)):
        return jnp.concatenate([w[QKVO, tt, lo:hi, cols] for lo, hi in spans], axis=0)

    def project(tt):
        @pl.loop(0, length // TILE)
        def _(m):
            r = span(m * TILE, TILE)
            xm = x[r, :]
            for lo, hi, spans in (
                (0, 256, (q01, k01)), (256, 512, (v01, q2, v2)), (512, 640, (k2, o2)),
            ):
                piece = nt(xm, picked(tt, spans))
                qkv[tt, r, lo:hi] = (
                    (piece + near[tt, 1:2, lo:hi]) * scales[:, lo:hi]
                ).astype(BF16)

    def attend(tt, some=None):
        for i in some or range(blocks):
            lo, hi = band(i)
            r = slice(i * LANES, (i + 1) * LANES)
            heads_in = (
                (qkv[tt, r, 0:128] * low, 128, 256),
                (qkv[tt, r, 0:128] * high, 128, 256),
                (qkv[tt, r, 384:512] * low, 512, 384),
            )
            sc = [
                nt(q, qkv[tt, lo:hi, kc : kc + LANES]) + bias[r, 0 : hi - lo]
                for q, kc, _ in heads_in
            ]
            ex = [jnp.exp(z - jnp.max(z, axis=-1, keepdims=True)) for z in sc]
            ps = [(e * (1.0 / jnp.sum(e, axis=-1, keepdims=True))).astype(BF16) for e in ex]
            for h, p in enumerate(ps):
                prob[tt, h, r, 0 : hi - lo] = p
            outs = [
                nn(p, qkv[tt, lo:hi, vc : vc + LANES]) for p, (_, _, vc) in zip(ps, heads_in)
            ]
            ctx[tt, r, 0:128] = (outs[2] * high32).astype(BF16)
            ctx[tt, r, 128:256] = (outs[0] * low32 + outs[1] * high32).astype(BF16)

    def attend_back(tt):
        for group in range(2):
            if group == 0:
                qc, kc, vc, dc = 0, 128, 256, 128
                hs = ((0, low, low, low32), (1, high, high, high32))
            else:
                qc, kc, vc, dc = 384, 512, 384, 0
                hs = ((2, low, high, low32),)
            dq = [None] * blocks
            for i in range(blocks):
                lo, hi = band(i)
                r = slice(i * LANES, (i + 1) * LANES)
                for n, (h, qm, vm, out_mask) in enumerate(hs):
                    dp = nt(dctx[r, dc : dc + LANES] * vm, qkv[tt, lo:hi, vc : vc + LANES])
                    p = prob[tt, h, r, 0 : hi - lo].astype(F32)
                    pd = p * dp
                    ds = (pd - p * jnp.sum(pd, axis=-1, keepdims=True)).astype(BF16)
                    dsc[n, r, 0 : hi - lo] = ds
                    part = nn(ds, qkv[tt, lo:hi, kc : kc + LANES]) * (
                        out_mask * (1.0 / math.sqrt(HEAD_DIM))
                    )
                    dq[i] = part if dq[i] is None else dq[i] + part
                if group == 0:
                    work[r, 0:128] = dq[i].astype(BF16)
            for j in range(blocks):
                rj = slice(j * LANES, (j + 1) * LANES)
                dk = dv = None
                for i in range(blocks):
                    lo, hi = band(i)
                    if not lo <= j * LANES < hi:
                        continue
                    r = slice(i * LANES, (i + 1) * LANES)
                    at = slice(j * LANES - lo, (j + 1) * LANES - lo)
                    for n, (h, qm, vm, _) in enumerate(hs):
                        more = tn(dsc[n, r, at], qkv[tt, r, qc : qc + LANES] * qm)
                        dk = more if dk is None else dk + more
                        more = tn(prob[tt, h, r, at], dctx[r, dc : dc + LANES] * vm)
                        dv = more if dv is None else dv + more
                if group == 0:
                    work[rj, 128:256] = dk.astype(BF16)
                    work[rj, 256:384] = dv.astype(BF16)
                else:
                    work[rj, 384:512] = (dq[j] + dv).astype(BF16)
                    work[rj, 512:640] = dk.astype(BF16)

    def add_sum(k, tile):
        n = tile.shape[0] // 8
        sums[k] += jnp.sum(tile.reshape(n, 8, tile.shape[1]), axis=0)

    def by_tiles(body):
        @pl.loop(0, length // 64)
        def _(m):
            body(span(m * 64, 64))

    def transpose_to(src):
        @pl.loop(0, rows // TILE)
        def _(m):
            cols = span(m * TILE, TILE)
            tr[cols, :] = src[:, cols].T

    for k in range(3):
        for copy in local(k):
            copy.start()
    dy_in = pltpu.make_async_copy(dy, work, ls.at[6])
    dy_in.start()
    all_here = me.greet()
    own = vecs[7:8, :]
    mid, end = own[:, 128:256], own[:, 256:384]
    turned = jnp.where(low_lanes, pltpu.roll(mid, HEAD_DIM, 1), pltpu.roll(end, HEAD_DIM, 1))
    bloc[...] = jnp.zeros_like(bloc)
    bloc[0:1, :] = vecs[6:7, :]
    bloc[1:2, 0:128] = own[:, 0:128]
    bloc[1:2, 256:384] = turned
    bloc[1:2, 384:512] = jnp.where(low_lanes, mid, end)
    near[me.t] = bloc[...]
    lane = lax.broadcasted_iota(jnp.int32, (1, 640), 1)
    is_query = (lane < 128) | ((lane >= 384) & (lane < 448))
    scales = jnp.where(is_query, 1.0 / math.sqrt(HEAD_DIM), 1.0)
    sums[...] = jnp.zeros_like(sums)
    labels = lax.broadcasted_iota(jnp.int32, (TEXTS, length), 0)
    memb[...] = jnp.where(seg[pl.ds(me.t, 1), :] == labels, 1.0, 0.0)
    for i in range(blocks):
        lo, hi = band(i)
        r = slice(i * LANES, (i + 1) * LANES)
        bias[r, 0 : hi - lo] = (tn(memb[:, r], memb[:, lo:hi]) - 1.0) * 1000000000.0
    for copy in local(QKVO):
        copy.wait()
    all_here()
    zends(lambda c: c.start())
    for s in range(far):
        bcopy(s).start()
    for k in (UP, DOWN):
        for copy in local(k):
            copy.wait()
    project(me.t)
    on_z(QKVO, 0)
    on_z(QKVO, 1)
    attend(me.t, (0, 1))
    on_z(QKVO, 2)
    zstart(UP)
    attend(me.t, (2, 3))
    on_xy(QKVO, 0)
    for s in range(far):
        bcopy(s).wait_recv()
    on_xy(QKVO, 1)
    on_relay(QKVO, 0)
    on_xy(QKVO, 2)

    @pl.loop(0, far)
    def _(s):
        tt = came(s)
        scopy(QKVO, s).wait_recv()
        project(tt)

        @pl.when(s < far - 1)
        def _():
            on_relay(QKVO, s + 1)

        attend(tt)
        on_z(UP, s)

        @pl.when(s == 1)
        def _():
            zstart(DOWN)

        @pl.when(s > 0)
        def _():
            on_xy(UP, s - 1)

    @pl.loop(0, length // TILE)
    def _(m):
        r = span(m * TILE, TILE)
        for n in range(width // TILE):
            c = slice(n * TILE, (n + 1) * TILE)
            out = x[r, c].astype(F32) + vecs[0:1, c]
            for t in range(n_t):
                out = out + nn(ctx[t, r, :], picked(t, (k2, o2, o01), c))
            acc[r, c] = out

    on_relay(UP, 0)

    @by_tiles
    def _(r):
        center = acc[r, :]
        center = center - jnp.mean(center, axis=-1, keepdims=True)
        inv = lax.rsqrt(jnp.mean(center * center, axis=-1, keepdims=True) + 1e-12)
        rstd[r, :] = inv
        center = center * inv
        n1[r, :] = center
        h1[r, :] = (center * vecs[1:2, :] + vecs[2:3, :]).astype(BF16)

    def rise(tt):
        @pl.loop(0, length // TILE)
        def _(m):
            r = span(m * TILE, TILE)
            hm = h1[r, :]
            for n in range(rows // TILE):
                c = slice(n * TILE, (n + 1) * TILE)
                up, slope = gelu_both(nn(hm, w[UP, tt, :, c]) + near[tt, 0:1, c])
                act[tt, r, c] = up.astype(BF16)
                dg[tt, r, c] = slope.astype(BF16)

    def fall(tt, first):
        @pl.loop(0, length // TILE)
        def _(m):
            r = span(m * TILE, TILE)
            am = act[tt, r, :]
            for n in range(width // TILE):
                c = slice(n * TILE, (n + 1) * TILE)
                out = nn(am, w[DOWN, tt, :, c])
                acc[r, c] = out if first else acc[r, c] + out

    on_z(DOWN, 0)
    rise(me.t)
    on_xy(UP, 2)
    on_relay(UP, 1)
    on_z(DOWN, 1)

    @pl.loop(0, far)
    def _(s):
        scopy(UP, s).wait_recv()
        rise(came(s))

        @pl.when(s == 0)
        def _():
            on_relay(UP, far - 1)
            on_z(DOWN, far - 1)

        on_xy(DOWN, s)

    on_relay(DOWN, 0)
    fall(me.t, True)

    @pl.loop(0, far)
    def _(s):
        @pl.when(s < far - 1)
        def _():
            on_relay(DOWN, s + 1)

        scopy(DOWN, s).wait_recv()
        fall(came(s), False)

    dy_in.wait()

    @by_tiles
    def _(r):
        dyt = work[r, :].astype(F32)
        center = acc[r, :] + vecs[3:4, :] + (n1[r, :] * vecs[1:2, :] + vecs[2:3, :])
        center = center - jnp.mean(center, axis=-1, keepdims=True)
        inv = lax.rsqrt(jnp.mean(center * center, axis=-1, keepdims=True) + 1e-12)
        n2 = center * inv
        final = n2 * vecs[4:5, :] + vecs[5:6, :]
        out = final.astype(BF16)
        dn = dyt * vecs[4:5, :]
        dr = inv * (
            dn
            - jnp.mean(dn, axis=-1, keepdims=True)
            - n2 * jnp.mean(dn * n2, axis=-1, keepdims=True)
        )
        layer_out[r, :] = out
        g[1, 1, r, :] = (final - out.astype(F32)).astype(BF16)
        acc[r, :] = dr
        dlow[r, :] = dr.astype(BF16)
        add_sum(0, dr)
        add_sum(1, dyt * n2)
        add_sum(2, dyt)

    counts = jnp.sum(memb[...], axis=-1, keepdims=True)
    member = memb[...].astype(BF16)
    pooled[...] = (nn(member, layer_out[...]) + nn(member, g[1, 1, 0:length, :])) / counts

    ones = jnp.ones((8, length), BF16)

    def grad_to(k, s, left_t, right):
        @pl.loop(0, rows // TILE)
        def _(m):
            r = span(m * TILE, TILE)
            lt = left_t(r)
            for n in range(width // TILE):
                c = slice(n * TILE, (n + 1) * TILE)
                g[k, s, r, c] = nn(lt, right[:, c]).astype(BF16)

    @pl.loop(0, n_t)
    def _(s):
        tt = goes(s)
        grad_to(0, s, lambda r: act[tt, :, r].T, dlow)
        r1(0, s).start()

        @pl.when(s > 0)
        def _():
            on_r1(0, s - 1)

    transpose_to(h1)
    on_r1(0, far)

    @pl.loop(0, n_t)
    def _(s):
        tt = goes(s)

        @pl.loop(0, length // TILE)
        def _(m):
            r = span(m * TILE, TILE)
            dm = dlow[r, :]
            for n in range(rows // TILE):
                c = slice(n * TILE, (n + 1) * TILE)
                work[r, c] = (nt(dm, w[DOWN, tt, c, :]) * dg[tt, r, c].astype(F32)).astype(BF16)

        @pl.when(s > 0)
        def _():
            on_r1(1, s - 1)

        grad_to(1, s, lambda r: tr[r, :], work)
        r1(1, s).start()

        @pl.loop(0, length // TILE)
        def _(m):
            r = span(m * TILE, TILE)
            dm = work[r, :]
            for n in range(width // TILE):
                c = slice(n * TILE, (n + 1) * TILE)
                acc[r, c] += nt(dm, w[UP, tt, c, :])

        vsum[1, pl.ds(tt, 1), :] = nn(ones, work[...])[0:1, :]
        on_r2(0, s)

    on_r1(1, far)

    @by_tiles
    def _(r):
        dh, nt1 = acc[r, :], n1[r, :]
        dn = dh * vecs[1:2, :]
        dr = rstd[r, :] * (
            dn
            - jnp.mean(dn, axis=-1, keepdims=True)
            - nt1 * jnp.mean(dn * nt1, axis=-1, keepdims=True)
        )
        acc[r, :] = dr
        dlow[r, :] = dr.astype(BF16)
        add_sum(3, dr)
        add_sum(4, dh * nt1)
        add_sum(5, dh)

    on_r2b(0, 0, False)
    on_rz(0)
    on_r2b(0, 1, False)
    vsum[0] = jnp.zeros((8, width), F32)
    for k, row in ((3, 0), (4, 1), (5, 2), (0, 3), (1, 4), (2, 5)):
        vsum[0, row : row + 1, :] = jnp.sum(sums[k], axis=0, keepdims=True)
    pair_sum(0).start()
    work[:, 640:768] = jnp.zeros((length, LANES), BF16)

    @pl.loop(0, n_t)
    def _(s):
        tt = goes(s)

        @pl.loop(0, length // TILE)
        def _(m):
            r = span(m * TILE, TILE)
            out = nt(dlow[r, :], picked(tt, (k2, o2, o01)))
            dctx[r, 0:128] = (out[:, 0:128] * high32).astype(BF16)
            dctx[r, 128:256] = out[:, 128:256].astype(BF16)

        attend_back(tt)

        @pl.when(s == 0)
        def _():
            on_pair(0)
            on_r2b(0, 2, False)
            on_r2(1, 0)
            on_r2(1, 1)

        @pl.when(s == 1)
        def _():
            on_r2b(0, 3, True)
            on_rz(1)
            on_r2z(0)
            on_r2(1, 2)
            on_r2(1, 3)

        @pl.when(s == 2)
        def _():
            on_r2zb(0)
            on_r3(0)
            on_plane(0)
            on_r2b(1, 0, False)

        @pl.when(s == 3)
        def _():
            on_r2b(1, 1, False)
            on_r2z(1)
            on_r2b(1, 2, False)
            on_r2(2, 0)

        r1(0, s).wait_send()
        for h in range(2):
            for j in range(3):
                r2(0, s, h, j).wait_send()

        @pl.when(s < far)
        def _():
            rz(0, s).wait_send()

        for m in range(rows // TILE):
            r = slice(m * TILE, (m + 1) * TILE)
            lt = work[:, r].T
            ct = ctx[tt].T if r.start == 512 else None
            for n in range(width // TILE):
                c = slice(n * TILE, (n + 1) * TILE)
                out = nn(lt, x[:, c])
                if ct is not None:
                    out = out + nn(ct, dlow[:, c])
                out = out.astype(BF16)
                at = 0
                for lo, hi in ((q01, k01), (v01, q2, v2), (k2, o2, o01))[m]:
                    g[0, s, lo:hi, c] = out[at : at + hi - lo, :]
                    at += hi - lo

        r1(2, s).start()

        @pl.loop(0, length // TILE)
        def _(m):
            r = span(m * TILE, TILE)
            dm = work[r, 0:640]
            for n in range(width // TILE):
                c = slice(n * TILE, (n + 1) * TILE)
                acc[r, c] += nn(dm, picked(tt, (q01, k01, v01, q2, v2, k2, o2), c))

        vsum[1, pl.ds(4 + tt, 1), :] = nn(ones, work[...])[0:1, :]

        @pl.when(s > 0)
        def _():
            on_r1(2, s - 1)

    pair_sum(1).start()
    on_r1(2, far)
    on_r2(2, 1)
    on_r2b(1, far, True)
    on_pair(1)
    on_r2(2, 2)
    on_r4(0)
    on_r2b(2, 0, False)
    on_r2(2, far)
    on_r2b(2, 1, False)
    on_r2b(2, 2, False)
    on_rz(2)
    on_plane(1)
    on_r2zb(1)
    on_r3(1)
    turns = lax.rem(width - me.t * (width // n_t), width)
    vout[0:8, :] = pltpu.roll(on_line(0), turns, 1)
    vout[8:16, :] = jnp.zeros((8, width), F32)
    on_r2b(2, far, True)
    on_r2z(2)
    on_r4b(0)
    on_r3(2)
    on_r2zb(2)
    on_r4(1)
    on_r4(2)
    on_r4b(1)
    vsum[1] = on_line(1)
    mine_row = vsum[1, pl.ds(4 + me.t, 1), :]
    vout[6:7, 0:128] = mine_row[:, 0:128]
    vout[6:7, 128:256] = mine_row[:, 384:512]
    vout[7:8, 0:128] = mine_row[:, 256:384]
    vout[7:8, 128:256] = pltpu.roll(mine_row[:, 384:512], HEAD_DIM, 1)
    vout[8:9, :] = vsum[1, pl.ds(me.t, 1), :]
    on_r4b(2)
    for k in range(3):
        r5(k).wait_recv()

    for s in range(far):
        bcopy(s).wait_send()
    for k in range(3):
        if k == QKVO:
            zends(lambda c: c.wait_send())
        for s in range(far):
            if k == QKVO:
                zpass(s, lambda c: c.wait_send())
            else:
                zfar(k, s).wait_send()
            scopy(k, s).wait_send()
            for j in range(2):
                xcopy(k, s, j).wait_send()
                relay(k, s, j).wait_send()
        for s in range(n_t):
            if k > 0:
                r1(k, s).wait_send()
                for h in range(2):
                    for j in range(3):
                        r2(k, s, h, j).wait_send()
        for j in range(2):
            r4(k, j, 0).wait_send()
            r4(k, j, 1).wait_send()
            r4b(k, j, me.other(j)).wait_send()
        r4c(k, me.other(0)).wait_send()
        for j in range(3):
            r2z(k, j).wait_send()
        if k > 0:
            for s in range(far):
                rz(k, s).wait_send()
        r5(k).wait_send()


def run_layer(wq, wk, wv, wo, wup, wdown, x, dy, seg, vecs, n_t):
    groups, (rows, cols) = 3, wup.shape
    length, width = x.shape
    ch, half, far = rows // PLANE, rows // 2, n_t - 1
    dma, vmem = pltpu.SemaphoreType.DMA, pltpu.VMEM
    here, there = pl.BlockSpec(memory_space=vmem), pl.BlockSpec(memory_space=pl.ANY)
    shape = jax.ShapeDtypeStruct
    pair = lambda *dims: [dma(dims), dma(dims)]
    return pl.pallas_call(
        functools.partial(layer_kernel, n_t),
        out_shape=(
            shape((length, width), BF16),
            shape((TEXTS, width), F32),
            shape((length, width), F32),
            shape((groups, rows, cols), BF16),
            shape((16, width), F32),
        ),
        in_specs=[there] * 6 + [here, there, here, here],
        out_specs=[here] * 5,
        scratch_shapes=[
            vmem((groups, n_t, rows, cols), BF16),
            vmem((2, n_t, rows, cols), BF16),
            vmem((2, n_t, half, cols), BF16),
            vmem((groups, n_t, 3, PLANE_ROWS, cols), BF16),
            vmem((groups, far, PLANE_ROWS, cols), BF16),
            vmem((groups, far, CHIPS * Z_ROWS, cols), BF16),
            vmem((groups, CHIPS * Z_ROWS, cols), BF16),
            vmem((groups, 3, Z_ROWS, cols), BF16),
            vmem((n_t, length, 640), BF16),
            vmem((n_t, length, 256), BF16),
            vmem((length, 256), BF16),
            vmem((n_t, 3, length, 384), BF16),
            vmem((n_t, length, rows), BF16),
            vmem((n_t, length, rows), BF16),
            vmem((length, width), BF16),
            vmem((length, width), BF16),
            vmem((length, width), BF16),
            vmem((width, length), BF16),
            vmem((2, length, 384), BF16),
            vmem((length, width), F32),
            vmem((n_t, 8, width), F32),
            vmem((8, width), F32),
            vmem((length, 384), F32),
            vmem((TEXTS, length), F32),
            vmem((length, 1), F32),
            vmem((6, 8, width), F32),
            vmem((2, 8, width), F32),
            vmem((2, 8, width), F32),
            vmem((2, 3, 8, width), F32),
            vmem((2, far, 8, width), F32),
            dma((7,)),
            dma((groups, far + 2)),
            dma((groups, n_t)),
            *pair(groups, far, 2),
            *pair(groups, far, 2),
            *pair(groups, far),
            *pair(far),
            *pair(groups, n_t),
            *pair(groups, n_t, 2, 3),
            *pair(groups, far),
            *pair(groups, 2, 2),
            *pair(groups),
            *pair(groups, 3),
            *pair(groups, far),
            *pair(groups, 3),
            *pair(2, 4 + far),
        ],
        compiler_params=pltpu.CompilerParams(
            collective_id=1, has_side_effects=True, vmem_limit_bytes=67043328
        ),
    )(wq, wk, wv, wo, wup, wdown, x, dy, seg, vecs)


def per_device(
    n_t, n_b,
    hidden_in, segment_ids, query_weight, query_bias, key_weight, value_weight, value_bias,
    out_weight, out_bias, attn_gain, attn_shift, up_weight, up_bias, down_weight, down_bias,
    ffn_gain, ffn_shift, cotangent,
):
    inner, width = out_weight.shape
    spare = jnp.zeros((width - 2 * inner,), F32)
    vecs = jnp.concatenate(
        [
            out_bias, attn_gain, attn_shift, down_bias, ffn_gain, ffn_shift, up_bias,
            query_bias, value_bias, spare,
        ]
    ).reshape(8, width)
    final, pooled, dx, fout, vout = run_layer(
        query_weight.T, key_weight.T, value_weight.T, out_weight, up_weight, down_weight,
        hidden_in[0], cotangent[0], segment_ids, vecs, n_t,
    )
    if n_b > PLANE:
        apart = [[i + PLANE * j for j in range(n_b // PLANE)] for i in range(PLANE)]
        fout, vout = lax.psum((fout.astype(F32), vout), "batch", axis_index_groups=apart)
    own = fout[2].astype(F32)
    return (
        final[None],
        pooled[None],
        dx[None],
        own[:inner].T,
        vout[6, :inner],
        own[inner : 2 * inner].T,
        own[2 * inner : 3 * inner].T,
        vout[7, :inner],
        own[3 * inner :],
        vout[0, :inner],
        vout[1, :inner],
        vout[2, :inner],
        fout[1].astype(F32),
        vout[8],
        fout[0].astype(F32),
        vout[3, :inner],
        vout[4, :inner],
        vout[5, :inner],
    )


def solution(mesh):
    rows, tens = P(("batch", "tensor"), None, None), P("tensor")
    col, row = P(None, "tensor"), P("tensor", None)
    in_specs = (
        rows, P("batch", None), col, tens, col, col, tens, row, P(), P(), P(), col, tens, row,
        P(), P(), P(), rows,
    )
    out_specs = (
        rows, rows, rows, col, tens, col, col, tens, row, tens, tens, tens, col, tens, row, tens,
        tens, tens,
    )
    body = functools.partial(per_device, mesh.shape["tensor"], mesh.shape["batch"])
    return jax.shard_map(
        body, mesh=mesh, in_specs=in_specs, out_specs=out_specs, check_vma=False
    )
```
